128 devices in a mesh: seq: 32 (over y, z, core), head: 4 (over x).
Axes of the slice: x: 4, y: 4, z: 4, core: 2. Of those that a mesh axis runs over, the one named last changes fastest.
Arguments:
- queries: bfloat16 [2, 64, 64, 128], P(None, 'head'), may hold values from -9 to 9
- cache_keys: bfloat16 [2, 8, 32768, 128], P(None, 'head', 'seq'), may hold values from -10 to 10
- cache_values: bfloat16 [2, 8, 32768, 128], P(None, 'head', 'seq'), may hold values from -6 to 6
- new_keys: bfloat16 [2, 8, 64, 128], P(None, 'head'), may hold values from -20 to 20
- new_values: bfloat16 [2, 8, 64, 128], P(None, 'head'), may hold values from -6 to 6
- parents: int32 [2, 64], replicated, may hold values from 0 to 62, as said below
- path: int32 [2, 6], replicated, may hold values from 0 to 63, as said below
- lengths: int32 [2], replicated, may hold values from 8192 to 32768, as said below
- draft_tokens: int32 [2, 64], replicated, may hold values from 0 to 65535
- residual: bfloat16 [2, 64, 8192], P(None, None, 'seq'), may hold values from -8 to 8
- out_weight: bfloat16 [8192, 8192], P('head', 'seq'), may hold values from -0.0625 to 0.0625
- norm_gain: bfloat16 [8192], P('seq'), may hold values from 0.5 to 1.5
- vocab_weight: bfloat16 [8192, 65536], P(None, ('seq', 'head')), may hold values from -3 to 3
Outputs:
- path_logits: float32 [2, 6, 65536], P(None, None, ('seq', 'head'))
- draft_logprob: float32 [2, 64], replicated
The draws below stay inside these ranges and needn't reach their ends.
Inputs may be any that keep to these rules, and one draw needn't show every extreme that they name: parents[b, 0] is 0; for every other node n, parents[b, n] is a smaller node number. path[b] lists 6 different nodes: node 0 first, and each later entry is a child (by parents) of the entry before it. `lengths`: at least one sequence uses all 32768 cache positions.
All inputs are finite; a program needn't handle non-finite values.
Results may differ from the reference program's by a relative error of at most 0.006.
Values may be sent and summed in bfloat16 or wider, within the bound.
No kernel may reach another device: no remote copies, remote signals or barrier semaphores. Data moves between devices by JAX's collectives and lax.ppermute only.
A program may use at most 64 MiB of HBM per device.

```python
import jax
import jax.numpy as jnp
from jax import lax

D = 8192
HQ = 64
KVH = 8
HD = 128
VOCAB = 65536
NODES = 64
PATH = 6
BATCH = 2
CTX_DEV = 1024
CTX = 32768
N_SEQ = 32


def tree_shape(key):
    source = jax.random.fold_in(key, 101)
    node_ids = jnp.arange(NODES, dtype=jnp.int32)
    upper = jnp.maximum(node_ids, 1)
    parents = jax.random.randint(jax.random.fold_in(source, 1), (BATCH, NODES), 0, upper[None, :], dtype=jnp.int32)
    row_keys = jax.random.split(jax.random.fold_in(source, 2), BATCH)
    short_keys = jax.random.split(jax.random.fold_in(source, 3), BATCH)

    def shuffle(row_key):
        return jax.random.permutation(row_key, NODES - 1).astype(jnp.int32) + 1

    def shuffle_short(row_key):
        return jax.random.permutation(row_key, NODES - 3).astype(jnp.int32) + 1
    orders = jax.vmap(shuffle)(row_keys)
    chosen_free = jnp.sort(orders[:, :PATH - 1], axis=1)
    short_orders = jax.vmap(shuffle_short)(short_keys)
    head_part = jnp.sort(short_orders[:, :PATH - 3], axis=1)
    tail_part = jnp.broadcast_to(jnp.array([NODES - 2, NODES - 1], dtype=jnp.int32)[None, :], (BATCH, 2))
    chosen_end = jnp.concatenate([head_part, tail_part], axis=1)
    special = jax.random.randint(jax.random.fold_in(source, 4), (), 0, BATCH, dtype=jnp.int32)
    is_special = (jnp.arange(BATCH, dtype=jnp.int32) == special)[:, None]
    chosen = jnp.where(is_special, chosen_end, chosen_free)
    path = jnp.concatenate([jnp.zeros((BATCH, 1), jnp.int32), chosen], axis=1)
    hits = node_ids[None, None, :] == path[:, 1:, None]
    forced = jnp.sum(jnp.where(hits, path[:, :-1, None], 0), axis=1)
    parents = jnp.where(jnp.any(hits, axis=1), forced, parents)
    return (parents.astype(jnp.int32), path.astype(jnp.int32))


def draw_parents(key, part):
    return tree_shape(key)[0]


def draw_path(key, part):
    return tree_shape(key)[1]


def fresh_keys(key):
    source = jax.random.fold_in(key, 202)
    shape = (BATCH, KVH, NODES, HD)
    raw = 5.0 * jax.random.truncated_normal(jax.random.fold_in(source, 1), -3.8, 3.8, shape, jnp.float32)
    return raw


def draw_new_keys(key, part):
    return fresh_keys(key).astype(jnp.bfloat16)


def draw_queries(key, part):
    source = jax.random.fold_in(key, 303)
    shape = (BATCH, HQ, NODES, HD)
    raw = 1.7 * jax.random.truncated_normal(jax.random.fold_in(source, 1), -4.5, 4.5, shape, jnp.float32)
    return raw.astype(jnp.bfloat16)


def draw_cache_keys(key, part):
    source = jax.random.fold_in(key, 707)
    shape = (BATCH, KVH, CTX, HD)
    raw = 1.7 * jax.random.truncated_normal(jax.random.fold_in(source, 1), -10.0 / 1.7, 10.0 / 1.7, shape, jnp.float32)
    return raw.astype(jnp.bfloat16)


def draw_lengths(key, part):
    raw = jax.random.randint(jax.random.fold_in(key, 505), (BATCH,), CTX // 4, CTX + 1, dtype=jnp.int32)
    filled = jax.random.randint(jax.random.fold_in(key, 506), (), 0, BATCH, dtype=jnp.int32)
    return jnp.where(jnp.arange(BATCH, dtype=jnp.int32) == filled, CTX, raw).astype(jnp.int32)


def draw_residual(key, part):
    source = jax.random.fold_in(key, 606)
    columns = jnp.arange(D, dtype=jnp.float32) / D
    rising = 0.15 * jnp.exp(jnp.log(3.0) * columns)
    jitter = jnp.exp(jax.random.uniform(jax.random.fold_in(source, 1), (D,), jnp.float32, -0.69, 0.69))
    raw = jax.random.truncated_normal(jax.random.fold_in(source, 2), -5.0, 5.0, (BATCH, NODES, D), jnp.float32)
    return (raw * rising * jitter).astype(jnp.bfloat16)


def draw_vocab_weight(key, part):
    source = jax.random.fold_in(key, 404)
    spread = 3.0 / jnp.sqrt(jnp.float32(D))
    raw = spread * jax.random.truncated_normal(jax.random.fold_in(source, 1), -5.0, 5.0, (D, VOCAB), jnp.float32)
    return raw.astype(jnp.bfloat16)


def touch_ends(values, key, smallest, top_value):
    dims = values.shape
    place = [jax.random.randint(jax.random.fold_in(key, axis), (), 0, dims[axis]) for axis in range(len(dims))]
    values = values.at[tuple(place)].set(smallest)
    longest = dims.index(max(dims))
    place[longest] = (place[longest] + 1) % dims[longest]
    return values.at[tuple(place)].set(top_value)


def steps_of(stream_key, shape, pieces, smallest, top_value):
    def one(axis_at, parts):
        draws = jax.random.uniform(jax.random.fold_in(jax.random.fold_in(stream_key, 6), axis_at), (parts,), jnp.float32, smallest / len(pieces), top_value / len(pieces))
        return jnp.repeat(jnp.exp(draws), shape[axis_at] // parts).reshape((-1,) + (1,) * (len(shape) - axis_at - 1))

    factor_of = one(*pieces[0])
    for cut in pieces[1:]:
        factor_of = factor_of * one(*cut)
    return factor_of


def bell_draw(rng, dims, width, most, cuts=(), kind=jnp.bfloat16):
    factor_of = steps_of(rng, dims, cuts, -0.22, 0.18) if cuts else 1.0
    values = jax.random.normal(rng, dims, jnp.float32) * width * factor_of
    return jnp.minimum(jnp.maximum(values, -most), most).astype(kind)


def setup_inputs(seed: int = 0) -> dict:
    arg_keys = jax.random.split(jax.random.key(seed), 14)
    queries = draw_queries(jax.random.fold_in(arg_keys[13], 71), 0)
    cache_keys = draw_cache_keys(jax.random.fold_in(arg_keys[13], 71), 0)
    cache_values = bell_draw(arg_keys[2], (BATCH, KVH, CTX, HD), 1.0, 6.0, ((1, 4), (2, 32)))
    new_keys = draw_new_keys(jax.random.fold_in(arg_keys[13], 71), 0)
    new_values = bell_draw(arg_keys[4], (BATCH, KVH, NODES, HD), 1.0, 6.0, ((1, 4),))
    parents = draw_parents(jax.random.fold_in(arg_keys[13], 71), 0)
    path = draw_path(jax.random.fold_in(arg_keys[13], 71), 0)
    lengths = draw_lengths(jax.random.fold_in(arg_keys[13], 71), 0)
    draft_tokens = touch_ends(jax.random.randint(arg_keys[8], (BATCH, NODES), 0, VOCAB), jax.random.fold_in(arg_keys[8], 1), 0, VOCAB - 1).astype(jnp.int32)
    residual = draw_residual(jax.random.fold_in(arg_keys[13], 71), 0)
    out_weight = bell_draw(arg_keys[10], (HQ * HD, D), (HQ * HD) ** -0.5, 0.0625, ((0, 4), (1, 32)))
    norm_gain = jnp.clip(1.0 + 0.1 * jax.random.normal(arg_keys[11], (D,), jnp.float32), 0.5, 1.5).astype(jnp.bfloat16)
    vocab_weight = draw_vocab_weight(jax.random.fold_in(arg_keys[13], 71), 0)
    return {"queries": queries, "cache_keys": cache_keys, "cache_values": cache_values, "new_keys": new_keys, "new_values": new_values, "parents": parents, "path": path, "lengths": lengths, "draft_tokens": draft_tokens, "residual": residual, "out_weight": out_weight, "norm_gain": norm_gain, "vocab_weight": vocab_weight}


lowest = -1e+30
epsilon = 1e-05

def ancestors(parents):
    node_count = parents.shape[-1]
    node_ids = jnp.arange(node_count, dtype=jnp.int32)
    linked = (parents[..., :, None] == node_ids[None, None, :]).astype(jnp.float32)
    reached = jnp.maximum(linked, jnp.eye(node_count, dtype=jnp.float32)[None])
    for _ in range(node_count.bit_length()):
        reached = jnp.minimum(jnp.einsum('bij,bjk->bik', reached, reached), 1.0)
    return reached > 0.5

def block_state(scores, visible, values):
    masked = jnp.where(visible, scores, lowest)
    block_max = lax.optimization_barrier(jnp.max(masked, axis=-1))
    weights = jnp.where(visible, jnp.exp(masked - block_max[..., None]), 0.0).astype(jnp.bfloat16)
    block_total = lax.optimization_barrier(jnp.sum(weights.astype(jnp.float32), axis=-1))
    block_out = jnp.einsum('kqc,kcd->kqd', weights.astype(jnp.float32), values.astype(jnp.float32))
    return (block_max, block_total, block_out)

def reference(queries, cache_keys, cache_values, new_keys, new_values, parents, path, lengths, draft_tokens, residual, out_weight, norm_gain, vocab_weight):
    group_size = HQ // KVH
    score_scale = HD ** (-0.5)
    reached = ancestors(parents)
    positions = jnp.arange(CTX_DEV, dtype=jnp.int32)

    def per_sequence(entries):
        query_block, key_block, value_block, tree_keys, tree_values, reach_row, length = entries
        grouped = query_block.reshape(KVH, group_size * NODES, HD).astype(jnp.float32)
        tree_scores = jnp.einsum('kqd,kcd->kqc', grouped, tree_keys.astype(jnp.float32)) * score_scale
        tree_seen = jnp.tile(reach_row, (group_size, 1))[None]
        tree_max, tree_total, tree_out = block_state(tree_scores, tree_seen, tree_values)

        def per_block(anchor):
            block_keys = lax.dynamic_slice_in_dim(key_block, anchor, CTX_DEV, 1)
            block_values = lax.dynamic_slice_in_dim(value_block, anchor, CTX_DEV, 1)
            scores = jnp.einsum('kqd,kcd->kqc', grouped, block_keys.astype(jnp.float32)) * score_scale
            live_keys = (anchor + positions < length)[None, None, :]
            return block_state(scores, live_keys, block_values)
        anchors = jnp.arange(N_SEQ, dtype=jnp.int32) * CTX_DEV
        maxima, totals, outputs = lax.map(per_block, anchors)
        maxima = jnp.concatenate([maxima, tree_max[None]], 0)
        totals = jnp.concatenate([totals, tree_total[None]], 0)
        outputs = jnp.concatenate([outputs, tree_out[None]], 0)
        highest = lax.optimization_barrier(jnp.max(maxima, axis=0))
        factors = jnp.exp(maxima - highest[None])
        whole_total = lax.optimization_barrier(jnp.sum(totals * factors, axis=0))
        whole_out = lax.optimization_barrier(jnp.sum(outputs * factors[..., None], axis=0))
        result = (whole_out / whole_total[..., None]).astype(jnp.bfloat16)
        return result.reshape(HQ, NODES, HD)
    attention = lax.map(per_sequence, (queries, cache_keys, cache_values, new_keys, new_values, reached, lengths))
    projected = jnp.einsum('bhnd,hdc->bnc', attention.astype(jnp.float32), out_weight.reshape(HQ, HD, D).astype(jnp.float32))
    stream = residual.astype(jnp.float32) + projected
    mean_square = lax.optimization_barrier(jnp.sum(stream * stream, axis=-1)) / D
    normed = (stream * lax.rsqrt(mean_square + epsilon)[..., None] * norm_gain.astype(jnp.float32)).astype(jnp.bfloat16)
    flat_rows = normed.reshape(BATCH * NODES, D).astype(jnp.float32)
    block_width = VOCAB // 8

    def vocab_block(anchor):
        columns = lax.dynamic_slice_in_dim(vocab_weight, anchor, block_width, 1).astype(jnp.float32)
        return jnp.dot(flat_rows, columns, precision=lax.Precision.HIGHEST)
    blocks = lax.map(vocab_block, jnp.arange(8, dtype=jnp.int32) * block_width)
    logits = jnp.transpose(blocks, (1, 0, 2)).reshape(BATCH, NODES, VOCAB)
    path_logits = jnp.take_along_axis(logits, path[:, :, None], axis=1)
    vocab_top = lax.optimization_barrier(jnp.max(logits, axis=-1))
    vocab_sum = lax.optimization_barrier(jnp.sum(jnp.exp(logits - vocab_top[..., None]), axis=-1))
    picked = jnp.take_along_axis(logits, draft_tokens[:, :, None], axis=2)[..., 0]
    draft_logprob = picked - (vocab_top + jnp.log(vocab_sum))
    return (path_logits, draft_logprob)
```

```python
import functools

import jax
import jax.numpy as jnp
from jax import lax
from jax.experimental import pallas as pl
from jax.experimental.pallas import tpu as pltpu
from jax.sharding import Mesh
from jax.sharding import PartitionSpec as P

D = 8192
SEQ = ("seq_0", "seq_1", "seq_2")
CHIPS = ("seq_0", "seq_1")
SEQ_HEAD = ("seq_0", "seq_1", "seq_2", "head")

HIDDEN = -1e30
FLOOR = -1e25
EPSILON = 1e-5
LOG2E = 1.4426950408889634
ROWS = 256

f32 = jnp.float32
bf16 = jnp.bfloat16


def rows_dot(a, b):
    return lax.dot_general(a, b, (((1,), (1,)), ((), ())), preferred_element_type=f32)


def plain_dot(a, b):
    return lax.dot_general(a, b, (((1,), (0,)), ((), ())), preferred_element_type=f32)


def high_low(x):
    high = x.astype(bf16)
    return high, (x - high.astype(f32)).astype(bf16)


def attention_kernel(lengths_ref, parents_ref, q_ref, k_ref, v_ref, nk_ref, nv_ref, out_ref):
    heads, nodes, width = q_ref.shape[1:]
    span = k_ref.shape[2]
    scale = width**-0.5
    step = scale * LOG2E
    seq = lax.axis_index(SEQ)
    live = lengths_ref[pl.program_id(0)] - seq * span
    column = lax.broadcasted_iota(jnp.int32, (nodes, nodes), 1)
    row = lax.broadcasted_iota(jnp.int32, (nodes, nodes), 0)
    linked = jnp.logical_or(parents_ref[0] == column, row == column)
    reached = jnp.where(linked, 1.0, 0.0).astype(bf16)
    for _ in range((nodes - 1).bit_length()):
        reached = jnp.minimum(plain_dot(reached, reached), 1.0).astype(bf16)
    owner = jnp.where(seq == 0, 1.0, 0.0)
    tree_bias = jnp.where(reached.astype(f32) * owner > 0.5, 0.0, HIDDEN)
    keys, tree_keys = k_ref[0, 0], nk_ref[0, 0]
    ones = jnp.ones((span, width), bf16)
    values = jnp.concatenate([v_ref[0, 0], ones], axis=1)
    tree_values = jnp.concatenate([nv_ref[0, 0], ones[:nodes]], axis=1)
    dead = lax.broadcasted_iota(jnp.int32, (1, span), 1) >= live
    bias = jnp.where(dead, HIDDEN, 0.0)
    group = ROWS // nodes
    lane = lax.broadcasted_iota(jnp.int32, (ROWS, width), 1)
    tiled = jnp.concatenate([tree_bias] * group, axis=0)
    for part in range(heads // group):
        at = part * group
        query = q_ref[0, at : at + group].reshape(ROWS, width)
        scores = rows_dot(query, keys) + bias
        tree_scores = rows_dot(query, tree_keys) + tiled
        highest = jnp.maximum(
            jnp.max(scores, axis=1, keepdims=True), jnp.max(tree_scores, axis=1, keepdims=True)
        )
        top = jnp.maximum((highest * scale).astype(bf16).astype(f32), FLOOR)
        shift = top * LOG2E
        weights = jnp.exp2(scores * step - shift).astype(bf16)
        tree_weights = jnp.exp2(tree_scores * step - shift).astype(bf16)
        result = plain_dot(weights, values) + plain_dot(tree_weights, tree_values)
        out_ref[at : at + group, :nodes] = (
            result[:, :width].astype(bf16).reshape(group, nodes, width)
        )
        both = jnp.where(lane == 0, top, result[:, width:])
        turned = jnp.transpose(both)[:8]
        for h in range(group):
            section = turned[:, h * nodes : (h + 1) * nodes]
            high, low = high_low(section[1:2])
            out_ref[at + h, nodes : nodes + 1, :nodes] = section[0:1].astype(bf16)
            out_ref[at + h, nodes + 1 : nodes + 2, :nodes] = high
            out_ref[at + h, nodes + 2 : nodes + 3, :nodes] = low


def local_attention(queries, cache_keys, cache_values, new_keys, new_values, parents, lengths):
    batch, heads, nodes, width = queries.shape
    kv, span = cache_keys.shape[1:3]
    group = heads // kv
    whole = lambda b, g, *_: (b, g, 0, 0)
    return pl.pallas_call(
        attention_kernel,
        grid_spec=pltpu.PrefetchScalarGridSpec(
            num_scalar_prefetch=1,
            grid=(batch, kv),
            in_specs=[
                pl.BlockSpec((1, nodes, 1), lambda b, g, *_: (b, 0, 0)),
                pl.BlockSpec((1, group, nodes, width), whole),
                pl.BlockSpec((1, 1, span, width), whole),
                pl.BlockSpec((1, 1, span, width), whole),
                pl.BlockSpec((1, 1, nodes, width), whole),
                pl.BlockSpec((1, 1, nodes, width), whole),
            ],
            out_specs=pl.BlockSpec((group, nodes + 8, width), lambda b, g, *_: (b * kv + g, 0, 0)),
        ),
        out_shape=jax.ShapeDtypeStruct((batch * heads, nodes + 8, width), bf16),
        name="attend",
    )(lengths, parents[:, :, None], queries, cache_keys, cache_values, new_keys, new_values)


def join_kernel(parts_ref, out_ref):
    count, rows, width = parts_ref.shape
    nodes = rows - 8
    tops = parts_ref[:, nodes, :].astype(f32)
    totals = parts_ref[:, nodes + 1, :].astype(f32) + parts_ref[:, nodes + 2, :].astype(f32)
    used = lax.broadcasted_iota(jnp.int32, (count, width), 1) < nodes
    tops = jnp.where(used, tops, 0.0)
    totals = jnp.where(used, totals, 1.0)
    factors = jnp.exp(tops - jnp.max(tops, axis=0, keepdims=True))
    share = factors / jnp.sum(factors * totals, axis=0, keepdims=True)
    square = jnp.concatenate([share, jnp.zeros((width - count, width), f32)], axis=0)
    turned = jnp.transpose(square)[:nodes]
    total = parts_ref[0, :nodes].astype(f32) * turned[:, 0:1]
    for k in range(1, count):
        total = total + parts_ref[k, :nodes].astype(f32) * turned[:, k : k + 1]
    block = total.astype(bf16)
    for k in range(out_ref.shape[0]):
        out_ref[k] = block


def join_shares(parts, copies):
    rows, width = parts.shape[1:]
    return pl.pallas_call(
        join_kernel,
        out_shape=jax.ShapeDtypeStruct((copies, rows - 8, width), bf16),
        name="join",
    )(parts)


def project_kernel(mine_ref, other_ref, weight_ref, out_ref):
    chips, nodes, width = mine_ref.shape
    first = lax.axis_index("seq_2") == 0
    mine, other = mine_ref[...], other_ref[...]
    even = jnp.where(first, mine, other)
    odd = jnp.where(first, other, mine)
    half = chips // 2
    lines = []
    for b in range(2):
        blocks = []
        for k in range(half):
            blocks += [even[b * half + k], odd[b * half + k]]
        lines.append(jnp.concatenate(blocks, axis=1))
    result = plain_dot(jnp.concatenate(lines, axis=0), weight_ref[...]).astype(bf16)
    for k in range(out_ref.shape[0]):
        out_ref[k] = result


def project(mine, other, weight, copies):
    rows = 2 * mine.shape[1]
    return pl.pallas_call(
        project_kernel,
        out_shape=jax.ShapeDtypeStruct((copies, rows, weight.shape[1]), bf16),
        name="project",
    )(mine, other, weight)


def stream_kernel(parts_ref, residual_ref, gain_ref, out_ref):
    rows, columns = residual_ref.shape
    stream = residual_ref[...].astype(f32)
    for k in range(parts_ref.shape[0]):
        stream = stream + parts_ref[k].astype(f32)
    scaled = (stream * gain_ref[...].astype(f32)).astype(bf16)
    squares = stream * stream
    folded = squares[:, :128]
    for at in range(128, columns, 128):
        folded = folded + squares[:, at : at + 128]
    sums = jnp.sum(jnp.transpose(folded), axis=0, keepdims=True)
    high, low = high_low(sums)
    for k in range(out_ref.shape[0]):
        out_ref[k, :rows] = scaled
        out_ref[k, rows : rows + 1, :128] = high
        out_ref[k, rows + 1 : rows + 2, :128] = low


def make_stream(parts, residual, gain, copies):
    rows, columns = residual.shape
    return pl.pallas_call(
        stream_kernel,
        out_shape=jax.ShapeDtypeStruct((copies, rows + 8, columns), bf16),
        name="stream",
    )(parts, residual, gain)


def logits_kernel(path_ref, mine_ref, other_ref, weight_ref, tokens_ref, picked_ref, stats_ref, acc):
    chips, padded, columns = mine_ref.shape
    rows = padded - 8
    width = weight_ref.shape[1]
    group = weight_ref.shape[0] // (2 * columns)
    first = lax.axis_index("seq_2") == 0
    at = pl.program_id(0)

    def half(which):
        blocks = []
        for k in range(group):
            mine = mine_ref[at * group + k, :rows]
            other = other_ref[at * group + k, :rows]
            blocks += [jnp.where(first, mine, other), jnp.where(first, other, mine)]
        return jnp.concatenate(blocks, axis=1)

    part = plain_dot(half(0), weight_ref[...])

    @pl.when(at == 0)
    def _():
        acc[...] = part

    @pl.when(at > 0)
    def _():
        acc[...] += part

    @pl.when(at == pl.num_programs(0) - 1)
    def _():
        sums = jnp.zeros((1, 128), f32)
        for ref in (mine_ref, other_ref):
            for k in range(chips):
                sums += ref[k, rows : rows + 1, :128].astype(f32)
                sums += ref[k, rows + 1 : rows + 2, :128].astype(f32)
        scale = lax.rsqrt(sums / D + EPSILON)
        square = jnp.broadcast_to(scale, (rows, 128))
        logits = acc[...] * jnp.transpose(square)[:, 0:1]
        acc[...] = logits
        top = jnp.max(logits, axis=1, keepdims=True)
        total = jnp.sum(jnp.exp(logits - top), axis=1, keepdims=True)
        ids = lax.broadcasted_iota(jnp.int32, (rows, width), 1) + lax.axis_index(SEQ_HEAD) * width
        hit = jnp.sum(jnp.where(ids == tokens_ref[...], logits, 0.0), axis=1, keepdims=True)
        lane = lax.broadcasted_iota(jnp.int32, (rows, 128), 1)
        both = jnp.where(lane == 0, top + jnp.log(total), hit)
        pair = jnp.transpose(both)[:2]
        for k in range(stats_ref.shape[0]):
            stats_ref[k] = pair
        for b in range(picked_ref.shape[0]):
            for k in range(picked_ref.shape[1]):
                n = path_ref[b, k] + b * (rows // picked_ref.shape[0])
                picked_ref[b, k : k + 1] = acc[pl.ds(n, 1)]


def make_logits(mine, other, weight, path, tokens, copies):
    chips, padded, columns = mine.shape
    rows = padded - 8
    width = weight.shape[1]
    steps = 8
    depth = weight.shape[0] // steps
    fixed = lambda *_: (0, 0, 0)
    return pl.pallas_call(
        logits_kernel,
        grid_spec=pltpu.PrefetchScalarGridSpec(
            num_scalar_prefetch=1,
            grid=(steps,),
            in_specs=[
                pl.BlockSpec((chips, padded, columns), fixed),
                pl.BlockSpec((chips, padded, columns), fixed),
                pl.BlockSpec((depth, width), lambda k, *_: (k, 0)),
                pl.BlockSpec((rows, 1), lambda *_: (0, 0)),
            ],
            out_specs=[
                pl.BlockSpec((*path.shape, width), fixed),
                pl.BlockSpec((copies, 2, 128), fixed),
            ],
            scratch_shapes=[pltpu.VMEM((rows, width), f32)],
        ),
        out_shape=[
            jax.ShapeDtypeStruct((*path.shape, width), f32),
            jax.ShapeDtypeStruct((copies, 2, 128), f32),
        ],
        name="logits",
    )(path, mine, other, weight, tokens)


def to_each(x, axes):
    return lax.all_to_all(x, axes, 0, 0, tiled=True)


def across(x):
    return lax.ppermute(x, "seq_2", [(0, 1), (1, 0)])


def on_device(
    queries,
    cache_keys,
    cache_values,
    new_keys,
    new_values,
    parents,
    path,
    lengths,
    draft_tokens,
    residual,
    out_weight,
    norm_gain,
    vocab_weight,
):
    batch, nodes = parents.shape
    rows = batch * nodes
    chips = lax.axis_size(CHIPS)
    shares = local_attention(
        queries, cache_keys, cache_values, new_keys, new_values, parents, lengths
    )
    block = join_shares(to_each(shares, SEQ), chips)
    mine = to_each(block, CHIPS)
    partial = project(mine, across(mine), out_weight, lax.axis_size("head"))
    partial = to_each(partial, "head")
    stream = make_stream(partial, residual.reshape(rows, -1), norm_gain[None], chips)
    mine = to_each(stream, CHIPS)
    path_logits, stats = make_logits(
        mine,
        across(mine),
        vocab_weight,
        path,
        draft_tokens.reshape(rows, 1),
        lax.axis_size(SEQ_HEAD),
    )
    stats = to_each(stats, SEQ_HEAD)
    sums, hits = stats[:, 0], stats[:, 1]
    top = jnp.max(sums, axis=0)
    total = top + jnp.log(jnp.sum(jnp.exp(sums - top), axis=0))
    logprob = (jnp.sum(hits, axis=0) - total).reshape(batch, nodes)
    return (path_logits, logprob)


def solution(mesh):
    torus = Mesh(
        mesh.devices.reshape(4, 4, 2, mesh.shape["head"]), ("seq_0", "seq_1", "seq_2", "head")
    )
    in_specs = (
        P(None, "head", None, None),
        P(None, "head", SEQ, None),
        P(None, "head", SEQ, None),
        P(None, "head", None, None),
        P(None, "head", None, None),
        P(),
        P(),
        P(),
        P(),
        P(None, None, SEQ),
        P("head", SEQ),
        P(SEQ),
        P(None, SEQ_HEAD),
    )
    out_specs = (P(None, None, SEQ_HEAD), P())
    return jax.shard_map(
        on_device, mesh=torus, in_specs=in_specs, out_specs=out_specs, check_vma=False
    )
```

```python
import functools

import jax
import jax.numpy as jnp
from jax import lax
from jax.experimental import pallas as pl
from jax.experimental.pallas import tpu as pltpu
from jax.sharding import Mesh
from jax.sharding import PartitionSpec as P

D = 8192
SEQ = ("seq_0", "seq_1", "seq_2")
CHIPS = ("seq_0", "seq_1")
SEQ_HEAD = ("seq_0", "seq_1", "seq_2", "head")

HIDDEN = -1e30
FLOOR = -1e25
EPSILON = 1e-5
LOG2E = 1.4426950408889634
ROWS = 256

f32 = jnp.float32
bf16 = jnp.bfloat16


def rows_dot(a, b):
    return lax.dot_general(a, b, (((1,), (1,)), ((), ())), preferred_element_type=f32)


def plain_dot(a, b):
    return lax.dot_general(a, b, (((1,), (0,)), ((), ())), preferred_element_type=f32)


def room(mib):
    return pltpu.CompilerParams(vmem_limit_bytes=mib << 20)


def high_low(x):
    high = x.astype(bf16)
    return high, (x - high.astype(f32)).astype(bf16)


def tree_bias(parents):
    nodes = parents.shape[1]
    column = lax.broadcasted_iota(jnp.int32, (nodes, nodes), 1)
    row = lax.broadcasted_iota(jnp.int32, (nodes, nodes), 0)
    eye = row == column
    linked = jnp.where(jnp.logical_or(parents == row, eye), 1.0, 0.0).astype(bf16)
    reached = rows_dot(jnp.where(eye, 1.0, 0.0).astype(bf16), linked).astype(bf16)
    for _ in range((nodes - 1).bit_length()):
        reached = jnp.minimum(plain_dot(reached, reached), 1.0).astype(bf16)
    return jnp.where(reached.astype(f32) > 0.5, 0.0, HIDDEN)


def attention_kernel(lengths_ref, parents_ref, q_ref, k_ref, v_ref, nk_ref, nv_ref, out_ref):
    heads, nodes, width = q_ref.shape[1:]
    kv, span = k_ref.shape[1:3]
    scale = width**-0.5
    step = scale * LOG2E
    seq = lax.axis_index(SEQ)
    live = lengths_ref[pl.program_id(0)] - seq * span
    owner = seq == lax.axis_size(SEQ) - 1
    group = ROWS // nodes
    turns = range(heads // group)
    of_group = heads // group // kv
    ones = jnp.ones((span, width), bf16)

    def query(part):
        return q_ref[0, part * group : (part + 1) * group].reshape(ROWS, width)

    def write(part, out, top, total):
        at = part * group
        out_ref[at : at + group, :nodes] = out.astype(bf16).reshape(group, nodes, width)
        lane = lax.broadcasted_iota(jnp.int32, (ROWS, width), 1)
        turned = jnp.transpose(jnp.where(lane == 0, top, total))[:8]
        for h in range(group):
            section = turned[:, h * nodes : (h + 1) * nodes]
            high, low = high_low(section[1:2])
            out_ref[at + h, nodes : nodes + 1, :nodes] = section[0:1].astype(bf16)
            out_ref[at + h, nodes + 1 : nodes + 2, :nodes] = high
            out_ref[at + h, nodes + 2 : nodes + 3, :nodes] = low

    def sweep(with_cache, with_tree):
        streams = []
        if with_cache:
            dead = lax.broadcasted_iota(jnp.int32, (1, span), 1) >= live
            values = [jnp.concatenate([v_ref[0, g], ones], axis=1) for g in range(kv)]
            streams.append((k_ref, jnp.where(dead, HIDDEN, 0.0), values))
        if with_tree:
            bias = tree_bias(parents_ref[pl.ds(pl.program_id(0), 1)])
            values = [jnp.concatenate([nv_ref[0, g], ones[:nodes]], axis=1) for g in range(kv)]
            streams.append((nk_ref, jnp.concatenate([bias] * group, axis=0), values))

        def products(part):
            rows = query(part)
            return [rows_dot(rows, ref[0, part // of_group]) for ref, _, _ in streams]

        ahead = products(0)
        for part in turns:
            scores = [s + bias for s, (_, bias, _) in zip(ahead, streams)]
            if part + 1 < len(turns):
                ahead = products(part + 1)
            highest = functools.reduce(
                jnp.maximum, [jnp.max(s, axis=1, keepdims=True) for s in scores]
            )
            top = jnp.maximum((highest * scale).astype(bf16).astype(f32), FLOOR)
            shift = top * LOG2E
            result = 0.0
            for s, (_, _, values) in zip(scores, streams):
                weights = jnp.exp2(s * step - shift).astype(bf16)
                result = result + plain_dot(weights, values[part // of_group])
            write(part, result[:, :width], top, result[:, width:])

    has_cache = live > 0
    other = jnp.logical_not(owner)

    @pl.when(jnp.logical_and(has_cache, other))
    def _():
        sweep(True, False)

    @pl.when(jnp.logical_and(has_cache, owner))
    def _():
        sweep(True, True)

    @pl.when(jnp.logical_and(jnp.logical_not(has_cache), owner))
    def _():
        sweep(False, True)

    @pl.when(jnp.logical_and(jnp.logical_not(has_cache), other))
    def _():
        for part in turns:
            nothing = jnp.zeros((ROWS, width), f32)
            write(part, nothing, jnp.full((ROWS, 1), FLOOR), nothing)


def local_attention(queries, cache_keys, cache_values, new_keys, new_values, parents, lengths):
    batch, heads, nodes, width = queries.shape
    kv, span = cache_keys.shape[1:3]
    whole = lambda b, *_: (b, 0, 0, 0)
    return pl.pallas_call(
        attention_kernel,
        grid_spec=pltpu.PrefetchScalarGridSpec(
            num_scalar_prefetch=1,
            grid=(batch,),
            in_specs=[
                pl.BlockSpec(parents.shape, lambda b, *_: (0, 0)),
                pl.BlockSpec((1, heads, nodes, width), whole),
                pl.BlockSpec((1, kv, span, width), whole),
                pl.BlockSpec((1, kv, span, width), whole),
                pl.BlockSpec((1, kv, nodes, width), whole),
                pl.BlockSpec((1, kv, nodes, width), whole),
            ],
            out_specs=pl.BlockSpec((heads, nodes + 8, width), lambda b, *_: (b, 0, 0)),
        ),
        out_shape=jax.ShapeDtypeStruct((batch * heads, nodes + 8, width), bf16),
        compiler_params=room(24),
        name="attend",
    )(lengths, parents, queries, cache_keys, cache_values, new_keys, new_values)


def join_kernel(parts_ref, out_ref):
    count, rows, width = parts_ref.shape
    nodes = rows - 8
    tops = parts_ref[:, nodes, :].astype(f32)
    totals = parts_ref[:, nodes + 1, :].astype(f32) + parts_ref[:, nodes + 2, :].astype(f32)
    used = lax.broadcasted_iota(jnp.int32, (count, width), 1) < nodes
    tops = jnp.where(used, tops, 0.0)
    totals = jnp.where(used, totals, 1.0)
    factors = jnp.exp(tops - jnp.max(tops, axis=0, keepdims=True))
    share = factors / jnp.sum(factors * totals, axis=0, keepdims=True)
    square = jnp.concatenate([share, jnp.zeros((width - count, width), f32)], axis=0)
    turned = jnp.transpose(square)[:nodes]
    total = parts_ref[0, :nodes].astype(f32) * turned[:, 0:1]
    for k in range(1, count):
        total = total + parts_ref[k, :nodes].astype(f32) * turned[:, k : k + 1]
    block = total.astype(bf16)
    for k in range(out_ref.shape[0]):
        out_ref[k] = block


def join_shares(parts, copies):
    rows, width = parts.shape[1:]
    return pl.pallas_call(
        join_kernel,
        out_shape=jax.ShapeDtypeStruct((copies, rows - 8, width), bf16),
        compiler_params=room(8),
        name="join",
    )(parts)


def project_kernel(mine_ref, other_ref, weight_ref, out_ref):
    chips, nodes, width = mine_ref.shape
    first = lax.axis_index("seq_2") == 0
    mine, other = mine_ref[...], other_ref[...]
    even = jnp.where(first, mine, other)
    odd = jnp.where(first, other, mine)
    half = chips // 2
    lines = []
    for b in range(2):
        blocks = []
        for k in range(half):
            blocks += [even[b * half + k], odd[b * half + k]]
        lines.append(jnp.concatenate(blocks, axis=1))
    result = plain_dot(jnp.concatenate(lines, axis=0), weight_ref[...]).astype(bf16)
    for k in range(out_ref.shape[0]):
        out_ref[k] = result


def project(mine, other, weight, copies):
    rows = 2 * mine.shape[1]
    return pl.pallas_call(
        project_kernel,
        out_shape=jax.ShapeDtypeStruct((copies, rows, weight.shape[1]), bf16),
        compiler_params=room(8),
        name="project",
    )(mine, other, weight)


def stream_kernel(parts_ref, residual_ref, gain_ref, out_ref):
    rows, columns = residual_ref.shape
    stream = residual_ref[...].astype(f32)
    for k in range(parts_ref.shape[0]):
        stream = stream + parts_ref[k].astype(f32)
    scaled = (stream * gain_ref[...].astype(f32)[None]).astype(bf16)
    squares = stream * stream
    folded = squares[:, :128]
    for at in range(128, columns, 128):
        folded = folded + squares[:, at : at + 128]
    sums = jnp.sum(jnp.transpose(folded), axis=0, keepdims=True)
    high, low = high_low(sums)
    for k in range(out_ref.shape[0]):
        out_ref[k, :rows] = scaled
        out_ref[k, rows : rows + 1, :128] = high
        out_ref[k, rows + 1 : rows + 2, :128] = low


def make_stream(parts, residual, gain, copies):
    rows, columns = residual.shape
    return pl.pallas_call(
        stream_kernel,
        out_shape=jax.ShapeDtypeStruct((copies, rows + 8, columns), bf16),
        compiler_params=room(8),
        name="stream",
    )(parts, residual, gain)


def logits_kernel(path_ref, mine_ref, other_ref, weight_ref, tokens_ref, picked_ref, stats_ref, acc):
    chips, padded, columns = mine_ref.shape
    rows = padded - 8
    width = weight_ref.shape[1]
    group = weight_ref.shape[0] // (2 * columns)
    first = lax.axis_index("seq_2") == 0
    at = pl.program_id(0)

    def half(which):
        blocks = []
        for k in range(group):
            mine = mine_ref[at * group + k, :rows]
            other = other_ref[at * group + k, :rows]
            blocks += [jnp.where(first, mine, other), jnp.where(first, other, mine)]
        return jnp.concatenate(blocks, axis=1)

    part = plain_dot(half(0), weight_ref[...])

    @pl.when(at == 0)
    def _():
        acc[...] = part

    @pl.when(at > 0)
    def _():
        acc[...] += part

    @pl.when(at == pl.num_programs(0) - 1)
    def _():
        sums = jnp.zeros((1, 128), f32)
        for ref in (mine_ref, other_ref):
            for k in range(chips):
                sums += ref[k, rows : rows + 1, :128].astype(f32)
                sums += ref[k, rows + 1 : rows + 2, :128].astype(f32)
        scale = lax.rsqrt(sums / D + EPSILON)
        square = jnp.broadcast_to(scale, (rows, 128))
        logits = acc[...] * jnp.transpose(square)[:, 0:1]
        acc[...] = logits
        top = jnp.max(logits, axis=1, keepdims=True)
        total = jnp.sum(jnp.exp(logits - top), axis=1, keepdims=True)
        ids = lax.broadcasted_iota(jnp.int32, (rows, width), 1) + lax.axis_index(SEQ_HEAD) * width
        lines = [tokens_ref[b : b + 1].astype(f32) for b in range(tokens_ref.shape[0])]
        line = jnp.broadcast_to(jnp.concatenate(lines, axis=1), (128, rows))
        tokens = jnp.transpose(line)[:, 0:1].astype(jnp.int32)
        hit = jnp.sum(jnp.where(ids == tokens, logits, 0.0), axis=1, keepdims=True)
        lane = lax.broadcasted_iota(jnp.int32, (rows, 128), 1)
        both = jnp.where(lane == 0, top + jnp.log(total), hit)
        pair = jnp.transpose(both)[:2]
        for k in range(stats_ref.shape[0]):
            stats_ref[k] = pair
        for b in range(path_ref.shape[0]):
            for k in range(path_ref.shape[1]):
                n = path_ref[b, k] + b * (rows // path_ref.shape[0])
                picked_ref[k, b : b + 1] = acc[pl.ds(n, 1)]


def make_logits(mine, other, weight, path, tokens, copies):
    chips, padded, columns = mine.shape
    rows = padded - 8
    width = weight.shape[1]
    steps = 8
    depth = weight.shape[0] // steps
    fixed = lambda *_: (0, 0, 0)
    return pl.pallas_call(
        logits_kernel,
        grid_spec=pltpu.PrefetchScalarGridSpec(
            num_scalar_prefetch=1,
            grid=(steps,),
            in_specs=[
                pl.BlockSpec((chips, padded, columns), fixed),
                pl.BlockSpec((chips, padded, columns), fixed),
                pl.BlockSpec((depth, width), lambda k, *_: (k, 0)),
                pl.BlockSpec(tokens.shape, lambda *_: (0, 0)),
            ],
            out_specs=[
                pl.BlockSpec((*path.shape[::-1], width), fixed),
                pl.BlockSpec((copies, 2, 128), fixed),
            ],
            scratch_shapes=[pltpu.VMEM((rows, width), f32)],
        ),
        out_shape=[
            jax.ShapeDtypeStruct((*path.shape[::-1], width), f32),
            jax.ShapeDtypeStruct((copies, 2, 128), f32),
        ],
        compiler_params=room(16),
        name="logits",
    )(path, mine, other, weight, tokens)


def final_kernel(stats_ref, out_ref):
    sums, hits = stats_ref[:, 0], stats_ref[:, 1]
    top = jnp.max(sums, axis=0, keepdims=True)
    total = top + jnp.log(jnp.sum(jnp.exp(sums - top), axis=0, keepdims=True))
    result = jnp.sum(hits, axis=0, keepdims=True) - total
    nodes = out_ref.shape[1]
    for b in range(out_ref.shape[0]):
        out_ref[b : b + 1] = result[:, b * nodes : (b + 1) * nodes]


def log_probabilities(stats, batch):
    return pl.pallas_call(
        final_kernel,
        out_shape=jax.ShapeDtypeStruct((batch, stats.shape[2] // batch), f32),
        compiler_params=room(4),
        name="final",
    )(stats)


def to_each(x, axes):
    return lax.all_to_all(x, axes, 0, 0, tiled=True)


def across(x):
    return lax.ppermute(x, "seq_2", [(0, 1), (1, 0)])


def on_device(
    queries,
    cache_keys,
    cache_values,
    new_keys,
    new_values,
    parents,
    path,
    lengths,
    draft_tokens,
    residual,
    out_weight,
    norm_gain,
    vocab_weight,
):
    batch, nodes = parents.shape
    rows = batch * nodes
    chips = lax.axis_size(CHIPS)
    shares = local_attention(
        queries, cache_keys, cache_values, new_keys, new_values, parents, lengths
    )
    block = join_shares(to_each(shares, SEQ), chips)
    mine = to_each(block, CHIPS)
    partial = project(mine, across(mine), out_weight, lax.axis_size("head"))
    partial = to_each(partial, "head")
    stream = make_stream(partial, residual.reshape(rows, -1), norm_gain, chips)
    mine = to_each(stream, CHIPS)
    path_logits, stats = make_logits(
        mine,
        across(mine),
        vocab_weight,
        path,
        draft_tokens,
        lax.axis_size(SEQ_HEAD),
    )
    stats = to_each(stats, SEQ_HEAD)
    logprob = log_probabilities(stats, batch)
    return (jnp.transpose(path_logits, (1, 0, 2)), logprob)


def solution(mesh):
    torus = Mesh(
        mesh.devices.reshape(4, 4, 2, mesh.shape["head"]), ("seq_0", "seq_1", "seq_2", "head")
    )
    in_specs = (
        P(None, "head", None, None),
        P(None, "head", SEQ, None),
        P(None, "head", SEQ, None),
        P(None, "head", None, None),
        P(None, "head", None, None),
        P(),
        P(),
        P(),
        P(),
        P(None, None, SEQ),
        P("head", SEQ),
        P(SEQ),
        P(None, SEQ_HEAD),
    )
    out_specs = (P(None, None, SEQ_HEAD), P())
    return jax.shard_map(
        on_device, mesh=torus, in_specs=in_specs, out_specs=out_specs, check_vma=False
    )
```

```python
import functools

import jax
import jax.numpy as jnp
from jax import lax
from jax.experimental import pallas as pl
from jax.experimental.pallas import tpu as pltpu
from jax.sharding import Mesh
from jax.sharding import PartitionSpec as P

D = 8192
SEQ = ("seq_0", "seq_1", "seq_2")
CHIPS = ("seq_0", "seq_1")
SEQ_HEAD = ("seq_0", "seq_1", "seq_2", "head")

HIDDEN = -1e30
FLOOR = -1e25
EPSILON = 1e-5
LOG2E = 1.4426950408889634
ROWS = 256

f32 = jnp.float32
bf16 = jnp.bfloat16


def rows_dot(a, b):
    return lax.dot_general(a, b, (((1,), (1,)), ((), ())), preferred_element_type=f32)


def plain_dot(a, b):
    return lax.dot_general(a, b, (((1,), (0,)), ((), ())), preferred_element_type=f32)


def room(mib):
    return pltpu.CompilerParams(vmem_limit_bytes=mib << 20)


def rows_dot(a, b):
    return lax.dot_general(a, b, (((1,), (1,)), ((), ())), preferred_element_type=f32)


def plain_dot(a, b):
    return lax.dot_general(a, b, (((1,), (0,)), ((), ())), preferred_element_type=f32)


def room(mib):
    return pltpu.CompilerParams(vmem_limit_bytes=mib << 20)


def high_low(x):
    high = x.astype(bf16)
    return high, (x - high.astype(f32)).astype(bf16)


def tree_bias(parents):
    nodes = parents.shape[1]
    column = lax.broadcasted_iota(jnp.int32, (nodes, nodes), 1)
    row = lax.broadcasted_iota(jnp.int32, (nodes, nodes), 0)
    eye = row == column
    linked = jnp.where(jnp.logical_or(parents == row, eye), 1.0, 0.0).astype(bf16)
    reached = rows_dot(jnp.where(eye, 1.0, 0.0).astype(bf16), linked).astype(bf16)
    for _ in range((nodes - 1).bit_length()):
        reached = jnp.minimum(plain_dot(reached, reached), 1.0).astype(bf16)
    return jnp.where(reached.astype(f32) > 0.5, 0.0, HIDDEN)


def attention_kernel(
    lengths_hbm,
    parents_hbm,
    q_hbm,
    k_hbm,
    v_hbm,
    nk_hbm,
    nv_hbm,
    out_ref,
    lengths_ref,
    parents_ref,
    q_ref,
    k_ref,
    v_ref,
    nk_ref,
    nv_ref,
    block_sems,
    tree_sems,
    length_sem,
):
    batch, heads, nodes, width = q_ref.shape
    kv, span = k_ref.shape[1:3]
    scale = width**-0.5
    step = scale * LOG2E
    seq = lax.axis_index(SEQ)
    owner = seq == lax.axis_size(SEQ) - 1
    other = jnp.logical_not(owner)
    group = ROWS // nodes
    turns = range(heads // group)
    of_group = heads // group // kv
    ones = jnp.ones((span, width), bf16)

    lengths_copy = pltpu.make_async_copy(lengths_hbm, lengths_ref, length_sem)
    lengths_copy.start()

    def block_copy(b, g, n):
        own = pl.ds(g * (heads // kv), heads // kv)
        source, target, place = (
            (q_hbm, q_ref, (b, own)),
            (k_hbm, k_ref, (b, g)),
            (v_hbm, v_ref, (b, g)),
        )[n]
        return pltpu.make_async_copy(source.at[place], target.at[place], block_sems.at[b, g, n])

    for b in range(batch):
        for g in range(kv):
            for n in range(3):
                block_copy(b, g, n).start()
    trees = [
        pltpu.make_async_copy(source, target, tree_sems.at[n])
        for n, (source, target) in enumerate(
            ((parents_hbm, parents_ref), (nk_hbm, nk_ref), (nv_hbm, nv_ref))
        )
    ]

    @pl.when(owner)
    def _():
        for copy in trees:
            copy.start()
        for copy in trees:
            copy.wait()

    lengths_copy.wait()

    def write(b, part, out, top, total):
        at = b * heads + part * group
        out_ref[pl.ds(at, group), :nodes] = out.astype(bf16).reshape(group, nodes, width)
        lane = lax.broadcasted_iota(jnp.int32, (ROWS, width), 1)
        turned = jnp.transpose(jnp.where(lane == 0, top, total))[:8]
        for h in range(group):
            section = turned[:, h * nodes : (h + 1) * nodes]
            total = section[1:2]
            high = total.astype(bf16).astype(f32)
            row = lax.broadcasted_iota(jnp.int32, section.shape, 0)
            tail = jnp.where(row == 0, section[0:1], jnp.where(row == 1, high, total - high))
            out_ref[at + h, nodes:, :nodes] = tail.astype(bf16)

    def sweep(b, live, with_cache, with_tree):
        biases = []
        if with_cache:
            dead = lax.broadcasted_iota(jnp.int32, (1, span), 1) >= live
            biases.append(jnp.where(dead, HIDDEN, 0.0))
        if with_tree:
            bias = tree_bias(parents_ref[pl.ds(b, 1)])
            biases.append(jnp.concatenate([bias] * group, axis=0))

        def products(part):
            g = part // of_group
            rows = q_ref[b, part * group : (part + 1) * group].reshape(ROWS, width)
            found = [rows_dot(rows, k_ref[b, g])] if with_cache else []
            return found + ([rows_dot(rows, nk_ref[b, g])] if with_tree else [])

        ahead = products(0)
        for part in turns:
            g = part // of_group
            scores = [s + bias for s, bias in zip(ahead, biases)]
            if part + 1 < len(turns):
                ahead = products(part + 1)
            if part % of_group == 0:
                values = [jnp.concatenate([v_ref[b, g], ones], axis=1)] if with_cache else []
                if with_tree:
                    values.append(jnp.concatenate([nv_ref[b, g], ones[:nodes]], axis=1))
            highest = functools.reduce(
                jnp.maximum, [jnp.max(s, axis=1, keepdims=True) for s in scores]
            )
            top = jnp.maximum((highest * scale).astype(bf16).astype(f32), FLOOR)
            shift = top * LOG2E
            result = 0.0
            for s, value in zip(scores, values):
                weights = jnp.exp2(s * step - shift).astype(bf16)
                result = result + plain_dot(weights, value)
            write(b, part, result[:, :width], top, result[:, width:])

    def nothing(b):
        for part in turns:
            zeros = jnp.zeros((ROWS, width), f32)
            write(b, part, zeros, jnp.full((ROWS, 1), FLOOR), zeros)

    @pl.loop(0, batch)
    def _(b):
        live = lengths_ref[b] - seq * span
        for g in range(kv):
            for n in range(3):
                block_copy(b, g, n).wait()
        filled = live > 0
        empty = jnp.logical_not(filled)
        pl.when(jnp.logical_and(filled, other))(functools.partial(sweep, b, live, True, False))
        pl.when(jnp.logical_and(filled, owner))(functools.partial(sweep, b, live, True, True))
        pl.when(jnp.logical_and(empty, owner))(functools.partial(sweep, b, live, False, True))
        pl.when(jnp.logical_and(empty, other))(functools.partial(nothing, b))


def local_attention(queries, cache_keys, cache_values, new_keys, new_values, parents, lengths):
    batch, heads, nodes, width = queries.shape
    kv = cache_keys.shape[1]
    operands = (lengths, parents, queries, cache_keys, cache_values, new_keys, new_values)
    scratch = [pltpu.SMEM(lengths.shape, lengths.dtype)]
    scratch += [pltpu.VMEM(x.shape, x.dtype) for x in operands[1:]]
    scratch += [
        pltpu.SemaphoreType.DMA((batch, kv, 3)),
        pltpu.SemaphoreType.DMA((3,)),
        pltpu.SemaphoreType.DMA,
    ]
    return pl.pallas_call(
        attention_kernel,
        in_specs=[pl.BlockSpec(memory_space=pltpu.HBM)] * len(operands),
        out_specs=pl.BlockSpec(memory_space=pltpu.VMEM),
        out_shape=jax.ShapeDtypeStruct((batch * heads, nodes + 8, width), bf16),
        scratch_shapes=scratch,
        compiler_params=room(62),
        name="attend",
    )(*operands)


def join_kernel(parts_ref, gain_ref, out_ref):
    count, rows, width = parts_ref.shape
    nodes = rows - 8
    tops = parts_ref[:, nodes, :].astype(f32)
    totals = parts_ref[:, nodes + 1, :].astype(f32) + parts_ref[:, nodes + 2, :].astype(f32)
    used = lax.broadcasted_iota(jnp.int32, (count, width), 1) < nodes
    tops = jnp.where(used, tops, 0.0)
    totals = jnp.where(used, totals, 1.0)
    factors = jnp.exp(tops - jnp.max(tops, axis=0, keepdims=True))
    share = factors / jnp.sum(factors * totals, axis=0, keepdims=True)
    square = jnp.concatenate([share, jnp.zeros((width - count, width), f32)], axis=0)
    turned = jnp.transpose(square)[:nodes]
    total = parts_ref[0, :nodes].astype(f32) * turned[:, 0:1]
    for k in range(1, count):
        total = total + parts_ref[k, :nodes].astype(f32) * turned[:, k : k + 1]
    block = total.astype(bf16)
    gain = gain_ref[...].astype(f32)[None]
    lines = [gain[:, :width], gain[:, width:], jnp.ones((6, width), f32)]
    tail = jnp.concatenate(lines, axis=0).astype(bf16)
    for k in range(out_ref.shape[0]):
        out_ref[k, :nodes] = block
        out_ref[k, nodes:] = tail


def join_shares(parts, gain, copies):
    rows, width = parts.shape[1:]
    return pl.pallas_call(
        join_kernel,
        out_shape=jax.ShapeDtypeStruct((copies, rows, width), bf16),
        compiler_params=room(8),
        name="join",
    )(parts, gain)


def project_kernel(mine_ref, other_ref, weight_ref, out_ref):
    chips, padded, width = mine_ref.shape
    nodes = padded - 8
    first = lax.axis_index("seq_2") == 0
    mine, other = mine_ref[:, :nodes], other_ref[:, :nodes]
    even = jnp.where(first, mine, other)
    odd = jnp.where(first, other, mine)
    half = chips // 2
    lines = []
    for b in range(2):
        blocks = []
        for k in range(half):
            blocks += [even[b * half + k], odd[b * half + k]]
        lines.append(jnp.concatenate(blocks, axis=1))
    result = plain_dot(jnp.concatenate(lines, axis=0), weight_ref[...]).astype(bf16)
    for k in range(out_ref.shape[0]):
        out_ref[k] = result


def project(mine, other, weight, copies):
    rows = 2 * (mine.shape[1] - 8)
    return pl.pallas_call(
        project_kernel,
        out_shape=jax.ShapeDtypeStruct((copies, rows, weight.shape[1]), bf16),
        compiler_params=room(8),
        name="project",
    )(mine, other, weight)


def stream_kernel(parts_ref, residual_ref, gain_ref, out_ref):
    stream = residual_ref[...].astype(f32)
    for k in range(parts_ref.shape[0]):
        stream = stream + parts_ref[k].astype(f32)
    scaled = (stream * gain_ref[...].astype(f32)[None]).astype(bf16)
    for k in range(out_ref.shape[0]):
        out_ref[k] = scaled


def make_stream(parts, residual, gain, copies):
    rows, columns = residual.shape
    return pl.pallas_call(
        stream_kernel,
        out_shape=jax.ShapeDtypeStruct((copies, rows, columns), bf16),
        compiler_params=room(8),
        name="stream",
    )(parts, residual, gain)


def gathered_product(blocks_ref, gains_ref, weight_ref, core):
    chips, rows, columns = blocks_ref.shape
    nodes = gains_ref.shape[1] - 8
    blocks, sections, squares = [], [], 0.0
    for k in range(chips):
        block = blocks_ref[k]
        blocks.append(block)
        start = pl.multiple_of((2 * k + core) * columns, columns)
        sections.append(weight_ref[pl.ds(start, columns)])
        inverse = 1.0 / gains_ref[k, nodes:].astype(f32)
        for n in range(2):
            plain = block[:, n * 128 : (n + 1) * 128].astype(f32) * inverse[n : n + 1]
            squares = squares + plain * plain
    product = plain_dot(jnp.concatenate(blocks, axis=1), jnp.concatenate(sections, axis=0))
    return product, squares


def first_kernel(blocks_ref, gains_ref, weight_ref, product_ref, squares_ref):
    core = lax.axis_index("seq_2")
    product_ref[...], squares_ref[...] = gathered_product(
        blocks_ref, gains_ref, weight_ref, core
    )


def first_half(blocks, gains, weight):
    chips, rows, columns = blocks.shape
    width = weight.shape[1]
    return pl.pallas_call(
        first_kernel,
        out_shape=[
            jax.ShapeDtypeStruct((rows, width), f32),
            jax.ShapeDtypeStruct((rows, 128), f32),
        ],
        cost_estimate=pl.CostEstimate(
            flops=2 * rows * chips * columns * width,
            bytes_accessed=2 * chips * columns * (rows + width),
            transcendentals=0,
        ),
        compiler_params=room(16),
        name="logits_first",
    )(blocks, gains, weight)


def second_kernel(
    path_ref,
    blocks_ref,
    gains_ref,
    weight_ref,
    product_ref,
    squares_ref,
    tokens_ref,
    picked_ref,
    stats_ref,
    acc,
):
    rows, width = product_ref.shape
    core = 1 - lax.axis_index("seq_2")
    product, squares = gathered_product(blocks_ref, gains_ref, weight_ref, core)
    total = jnp.sum(squares + squares_ref[...], axis=1, keepdims=True)
    logits = (product + product_ref[...]) * lax.rsqrt(total / D + EPSILON)
    acc[...] = logits
    top = jnp.max(logits, axis=1, keepdims=True)
    sums = jnp.sum(jnp.exp(logits - top), axis=1, keepdims=True)
    ids = lax.broadcasted_iota(jnp.int32, (rows, width), 1) + lax.axis_index(SEQ_HEAD) * width
    lines = [tokens_ref[b : b + 1].astype(f32) for b in range(tokens_ref.shape[0])]
    line = jnp.broadcast_to(jnp.concatenate(lines, axis=1), (128, rows))
    tokens = jnp.transpose(line)[:, 0:1].astype(jnp.int32)
    hit = jnp.sum(jnp.where(ids == tokens, logits, 0.0), axis=1, keepdims=True)
    lane = lax.broadcasted_iota(jnp.int32, (rows, 128), 1)
    pair = jnp.transpose(jnp.where(lane == 0, top + jnp.log(sums), hit))[:2]
    for k in range(stats_ref.shape[0]):
        stats_ref[k] = pair
    for b in range(path_ref.shape[0]):
        for k in range(path_ref.shape[1]):
            n = path_ref[b, k] + b * (rows // path_ref.shape[0])
            picked_ref[k, b : b + 1] = acc[pl.ds(n, 1)]


def second_half(blocks, gains, weight, product, squares, path, tokens, copies):
    rows, width = product.shape
    specs = [pl.BlockSpec(memory_space=pltpu.VMEM)] * 6
    return pl.pallas_call(
        second_kernel,
        in_specs=[pl.BlockSpec(memory_space=pltpu.SMEM)] + specs,
        out_shape=[
            jax.ShapeDtypeStruct((*path.shape[::-1], width), f32),
            jax.ShapeDtypeStruct((copies, 2, 128), f32),
        ],
        scratch_shapes=[pltpu.VMEM((rows, width), f32)],
        compiler_params=room(16),
        name="logits_second",
    )(path, blocks, gains, weight, product, squares, tokens)


def final_kernel(stats_ref, out_ref):
    sums, hits = stats_ref[:, 0], stats_ref[:, 1]
    top = jnp.max(sums, axis=0, keepdims=True)
    total = top + jnp.log(jnp.sum(jnp.exp(sums - top), axis=0, keepdims=True))
    result = jnp.sum(hits, axis=0, keepdims=True) - total
    nodes = out_ref.shape[1]
    for b in range(out_ref.shape[0]):
        out_ref[b : b + 1] = result[:, b * nodes : (b + 1) * nodes]


def log_probabilities(stats, batch):
    return pl.pallas_call(
        final_kernel,
        out_shape=jax.ShapeDtypeStruct((batch, stats.shape[2] // batch), f32),
        compiler_params=room(4),
        name="final",
    )(stats)


def to_each(x, axes):
    return lax.all_to_all(x, axes, 0, 0, tiled=True)


def across(x):
    return lax.ppermute(x, "seq_2", [(0, 1), (1, 0)])


def on_device(
    queries,
    cache_keys,
    cache_values,
    new_keys,
    new_values,
    parents,
    path,
    lengths,
    draft_tokens,
    residual,
    out_weight,
    norm_gain,
    vocab_weight,
):
    batch, nodes = parents.shape
    rows = batch * nodes
    chips = lax.axis_size(CHIPS)
    shares = local_attention(
        queries, cache_keys, cache_values, new_keys, new_values, parents, lengths
    )
    heads = to_each(join_shares(to_each(shares, SEQ), norm_gain, chips), CHIPS)
    other_heads = across(heads)
    partial = project(heads, other_heads, out_weight, lax.axis_size("head"))
    partial = to_each(partial, "head")
    stream = make_stream(partial, residual.reshape(rows, -1), norm_gain, chips)
    mine = to_each(stream, CHIPS)
    other = across(mine)
    product, squares = first_half(mine, heads, vocab_weight)
    path_logits, stats = second_half(
        other,
        other_heads,
        vocab_weight,
        product,
        squares,
        path,
        draft_tokens,
        lax.axis_size(SEQ_HEAD),
    )
    stats = to_each(stats, SEQ_HEAD)
    logprob = log_probabilities(stats, batch)
    return (jnp.transpose(path_logits, (1, 0, 2)), logprob)


def solution(mesh):
    torus = Mesh(
        mesh.devices.reshape(4, 4, 2, mesh.shape["head"]), ("seq_0", "seq_1", "seq_2", "head")
    )
    in_specs = (
        P(None, "head", None, None),
        P(None, "head", SEQ, None),
        P(None, "head", SEQ, None),
        P(None, "head", None, None),
        P(None, "head", None, None),
        P(),
        P(),
        P(),
        P(),
        P(None, None, SEQ),
        P("head", SEQ),
        P(SEQ),
        P(None, SEQ_HEAD),
    )
    out_specs = (P(None, None, SEQ_HEAD), P())
    return jax.shard_map(
        on_device, mesh=torus, in_specs=in_specs, out_specs=out_specs, check_vma=False
    )
```

```python
import functools

import jax
import jax.numpy as jnp
from jax import lax
from jax.experimental import pallas as pl
from jax.experimental.pallas import tpu as pltpu
from jax.sharding import Mesh
from jax.sharding import PartitionSpec as P

D = 8192
SEQ = ("seq_0", "seq_1", "seq_2")
CHIPS = ("seq_0", "seq_1")
SEQ_HEAD = ("seq_0", "seq_1", "seq_2", "head")

HIDDEN = -1e30
FLOOR = -1e25
EPSILON = 1e-5
LOG2E = 1.4426950408889634
ROWS = 256

f32 = jnp.float32
bf16 = jnp.bfloat16


def rows_dot(a, b):
    return lax.dot_general(a, b, (((1,), (1,)), ((), ())), preferred_element_type=f32)


def plain_dot(a, b):
    return lax.dot_general(a, b, (((1,), (0,)), ((), ())), preferred_element_type=f32)


def room(mib):
    return pltpu.CompilerParams(vmem_limit_bytes=mib << 20)


def rows_dot(a, b):
    return lax.dot_general(a, b, (((1,), (1,)), ((), ())), preferred_element_type=f32)


def plain_dot(a, b):
    return lax.dot_general(a, b, (((1,), (0,)), ((), ())), preferred_element_type=f32)


def room(mib):
    return pltpu.CompilerParams(vmem_limit_bytes=mib << 20)


def high_low(x):
    high = x.astype(bf16)
    return high, (x - high.astype(f32)).astype(bf16)


def tree_bias(parents):
    nodes = parents.shape[1]
    column = lax.broadcasted_iota(jnp.int32, (nodes, nodes), 1)
    row = lax.broadcasted_iota(jnp.int32, (nodes, nodes), 0)
    eye = row == column
    linked = jnp.where(jnp.logical_or(parents == row, eye), 1.0, 0.0).astype(bf16)
    reached = rows_dot(jnp.where(eye, 1.0, 0.0).astype(bf16), linked).astype(bf16)
    for _ in range((nodes - 1).bit_length()):
        reached = jnp.minimum(plain_dot(reached, reached), 1.0).astype(bf16)
    return jnp.where(reached.astype(f32) > 0.5, 0.0, HIDDEN)


def attention_kernel(
    lengths_hbm,
    parents_hbm,
    q_hbm,
    k_hbm,
    v_hbm,
    nk_hbm,
    nv_hbm,
    gain_hbm,
    out_ref,
    lengths_ref,
    parents_ref,
    q_ref,
    k_ref,
    v_ref,
    nk_ref,
    nv_ref,
    gain_ref,
    block_sems,
    tree_sems,
    small_sems,
):
    batch, heads, nodes, width = q_ref.shape
    kv, span = k_ref.shape[1:3]
    scale = width**-0.5
    step = scale * LOG2E
    seq = lax.axis_index(SEQ)
    owner = seq == lax.axis_size(SEQ) - 1
    other = jnp.logical_not(owner)
    group = ROWS // nodes
    turns = range(heads // group)
    of_group = heads // group // kv
    ones = jnp.ones((span, width), bf16)

    lengths_copy = pltpu.make_async_copy(lengths_hbm, lengths_ref, small_sems.at[0])
    lengths_copy.start()
    gain_copy = pltpu.make_async_copy(gain_hbm, gain_ref, small_sems.at[1])
    gain_copy.start()

    def block_copy(b, g, n):
        own = pl.ds(g * (heads // kv), heads // kv)
        source, target, place = (
            (q_hbm, q_ref, (b, own)),
            (k_hbm, k_ref, (b, g)),
            (v_hbm, v_ref, (b, g)),
        )[n]
        return pltpu.make_async_copy(source.at[place], target.at[place], block_sems.at[b, g, n])

    for b in range(batch):
        for g in range(kv):
            for n in range(3):
                block_copy(b, g, n).start()
    trees = [
        pltpu.make_async_copy(source, target, tree_sems.at[n])
        for n, (source, target) in enumerate(
            ((parents_hbm, parents_ref), (nk_hbm, nk_ref), (nv_hbm, nv_ref))
        )
    ]

    @pl.when(owner)
    def _():
        for copy in trees:
            copy.start()
        for copy in trees:
            copy.wait()

    lengths_copy.wait()
    gain_copy.wait()
    gain = gain_ref[...].astype(f32)[None]
    gains = gain[:, :width], gain[:, width:]
    row = lax.broadcasted_iota(jnp.int32, (8, width), 0)

    def write(b, part, out, top, total):
        at = b * heads + part * group
        out_ref[pl.ds(at, group), :nodes] = out.astype(bf16).reshape(group, nodes, width)
        lane = lax.broadcasted_iota(jnp.int32, (ROWS, width), 1)
        turned = jnp.transpose(jnp.where(lane == 0, top, total))[:8]
        for h in range(group):
            section = turned[:, h * nodes : (h + 1) * nodes]
            total = section[1:2]
            high = total.astype(bf16).astype(f32)
            lines = jnp.where(row[:, :nodes] == 1, high, total - high)
            lines = jnp.where(row[:, :nodes] == 0, section[0:1], lines)
            tail = jnp.concatenate([lines, jnp.zeros((8, width - nodes), f32)], axis=1)
            for n in range(2):
                tail = jnp.where(row == 3 + n, gains[n], tail)
            out_ref[at + h, nodes:] = tail.astype(bf16)

    def sweep(b, live, with_cache, with_tree):
        biases = []
        if with_cache:
            dead = lax.broadcasted_iota(jnp.int32, (1, span), 1) >= live
            biases.append(jnp.where(dead, HIDDEN, 0.0))
        if with_tree:
            bias = tree_bias(parents_ref[pl.ds(b, 1)])
            biases.append(jnp.concatenate([bias] * group, axis=0))

        def products(part):
            g = part // of_group
            rows = q_ref[b, part * group : (part + 1) * group].reshape(ROWS, width)
            found = [rows_dot(rows, k_ref[b, g])] if with_cache else []
            return found + ([rows_dot(rows, nk_ref[b, g])] if with_tree else [])

        ahead = products(0)
        for part in turns:
            g = part // of_group
            scores = [s + bias for s, bias in zip(ahead, biases)]
            if part + 1 < len(turns):
                ahead = products(part + 1)
            if part % of_group == 0:
                values = [jnp.concatenate([v_ref[b, g], ones], axis=1)] if with_cache else []
                if with_tree:
                    values.append(jnp.concatenate([nv_ref[b, g], ones[:nodes]], axis=1))
            highest = functools.reduce(
                jnp.maximum, [jnp.max(s, axis=1, keepdims=True) for s in scores]
            )
            top = jnp.maximum((highest * scale).astype(bf16).astype(f32), FLOOR)
            shift = top * LOG2E
            result = 0.0
            for s, value in zip(scores, values):
                weights = jnp.exp2(s * step - shift).astype(bf16)
                result = result + plain_dot(weights, value)
            write(b, part, result[:, :width], top, result[:, width:])

    def nothing(b):
        for part in turns:
            zeros = jnp.zeros((ROWS, width), f32)
            write(b, part, zeros, jnp.full((ROWS, 1), FLOOR), zeros)

    @pl.loop(0, batch)
    def _(b):
        live = lengths_ref[b] - seq * span
        for g in range(kv):
            for n in range(3):
                block_copy(b, g, n).wait()
        filled = live > 0
        empty = jnp.logical_not(filled)
        pl.when(jnp.logical_and(filled, other))(functools.partial(sweep, b, live, True, False))
        pl.when(jnp.logical_and(filled, owner))(functools.partial(sweep, b, live, True, True))
        pl.when(jnp.logical_and(empty, owner))(functools.partial(sweep, b, live, False, True))
        pl.when(jnp.logical_and(empty, other))(functools.partial(nothing, b))


def local_attention(
    queries, cache_keys, cache_values, new_keys, new_values, parents, lengths, gain
):
    batch, heads, nodes, width = queries.shape
    kv = cache_keys.shape[1]
    operands = (lengths, parents, queries, cache_keys, cache_values, new_keys, new_values, gain)
    scratch = [pltpu.SMEM(lengths.shape, lengths.dtype)]
    scratch += [pltpu.VMEM(x.shape, x.dtype) for x in operands[1:]]
    scratch += [
        pltpu.SemaphoreType.DMA((batch, kv, 3)),
        pltpu.SemaphoreType.DMA((3,)),
        pltpu.SemaphoreType.DMA((2,)),
    ]
    return pl.pallas_call(
        attention_kernel,
        in_specs=[pl.BlockSpec(memory_space=pltpu.HBM)] * len(operands),
        out_specs=pl.BlockSpec(memory_space=pltpu.VMEM),
        out_shape=jax.ShapeDtypeStruct((batch * heads, nodes + 8, width), bf16),
        scratch_shapes=scratch,
        compiler_params=room(62),
        name="attend",
    )(*operands)


def join_kernel(parts_ref, out_ref):
    count, rows, width = parts_ref.shape
    nodes = rows - 8
    tops = parts_ref[:, nodes, :].astype(f32)
    totals = parts_ref[:, nodes + 1, :].astype(f32) + parts_ref[:, nodes + 2, :].astype(f32)
    used = lax.broadcasted_iota(jnp.int32, (count, width), 1) < nodes
    tops = jnp.where(used, tops, 0.0)
    totals = jnp.where(used, totals, 1.0)
    factors = jnp.exp(tops - jnp.max(tops, axis=0, keepdims=True))
    share = factors / jnp.sum(factors * totals, axis=0, keepdims=True)
    square = jnp.concatenate([share, jnp.zeros((width - count, width), f32)], axis=0)
    turned = jnp.transpose(square)[:nodes]
    total = parts_ref[0, :nodes].astype(f32) * turned[:, 0:1]
    for k in range(1, count):
        total = total + parts_ref[k, :nodes].astype(f32) * turned[:, k : k + 1]
    block = total.astype(bf16)
    for k in range(out_ref.shape[0]):
        out_ref[k] = block


def join_shares(parts, copies):
    rows, width = parts.shape[1:]
    return pl.pallas_call(
        join_kernel,
        out_shape=jax.ShapeDtypeStruct((copies, rows - 8, width), bf16),
        compiler_params=room(8),
        name="join",
    )(parts)


def head_lines(blocks_ref):
    half = blocks_ref.shape[0] // 2
    lines = [
        jnp.concatenate([blocks_ref[b * half + k] for k in range(half)], axis=1) for b in range(2)
    ]
    return jnp.concatenate(lines, axis=0)


def project_first_kernel(blocks_ref, weight_ref, out_ref, rest_ref):
    chips, nodes, width = blocks_ref.shape
    core = lax.axis_index("seq_2")
    sections = []
    for k in range(chips // 2):
        own = pl.multiple_of((2 * k + core) * width, width)
        other = pl.multiple_of((2 * k + 1 - core) * width, width)
        sections.append(weight_ref[pl.ds(own, width)])
        rest_ref[k * width : (k + 1) * width] = weight_ref[pl.ds(other, width)]
    out_ref[...] = plain_dot(head_lines(blocks_ref), jnp.concatenate(sections, axis=0))


def project_second_kernel(blocks_ref, weight_ref, first_ref, out_ref):
    result = first_ref[...] + plain_dot(head_lines(blocks_ref), weight_ref[...])
    result = result.astype(bf16)
    for k in range(out_ref.shape[0]):
        out_ref[k] = result


def project_first(blocks, weight):
    rows = 2 * blocks.shape[1]
    depth, columns = weight.shape
    return pl.pallas_call(
        project_first_kernel,
        out_shape=[
            jax.ShapeDtypeStruct((rows, columns), f32),
            jax.ShapeDtypeStruct((depth // 2, columns), weight.dtype),
        ],
        cost_estimate=pl.CostEstimate(
            flops=rows * weight.size, bytes_accessed=3 * weight.size, transcendentals=0
        ),
        compiler_params=room(8),
        name="project_first",
    )(blocks, weight)


def project_second(blocks, weight, first, copies):
    return pl.pallas_call(
        project_second_kernel,
        out_shape=jax.ShapeDtypeStruct((copies, *first.shape), bf16),
        compiler_params=room(8),
        name="project_second",
    )(blocks, weight, first)


def stream_kernel(parts_ref, residual_ref, gain_ref, out_ref):
    stream = residual_ref[...].astype(f32)
    for k in range(parts_ref.shape[0]):
        stream = stream + parts_ref[k].astype(f32)
    scaled = (stream * gain_ref[...].astype(f32)[None]).astype(bf16)
    for k in range(out_ref.shape[0]):
        out_ref[k] = scaled


def make_stream(parts, residual, gain, copies):
    rows, columns = residual.shape
    return pl.pallas_call(
        stream_kernel,
        out_shape=jax.ShapeDtypeStruct((copies, rows, columns), bf16),
        compiler_params=room(8),
        name="stream",
    )(parts, residual, gain)


def gathered_product(blocks_ref, shares_ref, weight_ref, core):
    chips, rows, columns = blocks_ref.shape
    nodes = shares_ref.shape[1] - 8
    blocks, sections, squares = [], [], 0.0
    for k in range(chips):
        block = blocks_ref[k]
        blocks.append(block)
        source = 2 * k + core
        sections.append(weight_ref[pl.ds(pl.multiple_of(source * columns, columns), columns)])
        gains = shares_ref[source, nodes:].astype(f32)
        for n in range(2):
            inverse = 1.0 / gains[3 + n : 4 + n]
            plain = block[:, n * 128 : (n + 1) * 128].astype(f32) * inverse
            squares = squares + plain * plain
    product = plain_dot(jnp.concatenate(blocks, axis=1), jnp.concatenate(sections, axis=0))
    return product, squares


def first_kernel(blocks_ref, shares_ref, weight_ref, product_ref, squares_ref):
    core = lax.axis_index("seq_2")
    product_ref[...], squares_ref[...] = gathered_product(
        blocks_ref, shares_ref, weight_ref, core
    )


def first_half(blocks, shares, weight):
    chips, rows, columns = blocks.shape
    width = weight.shape[1]
    return pl.pallas_call(
        first_kernel,
        out_shape=[
            jax.ShapeDtypeStruct((rows, width), f32),
            jax.ShapeDtypeStruct((rows, 128), f32),
        ],
        cost_estimate=pl.CostEstimate(
            flops=2 * rows * chips * columns * width,
            bytes_accessed=2 * chips * columns * (rows + width),
            transcendentals=0,
        ),
        compiler_params=room(16),
        name="logits_first",
    )(blocks, shares, weight)


def second_kernel(
    path_ref,
    blocks_ref,
    shares_ref,
    weight_ref,
    product_ref,
    squares_ref,
    tokens_ref,
    picked_ref,
    stats_ref,
    logits_ref,
):
    rows, width = product_ref.shape
    core = 1 - lax.axis_index("seq_2")
    product, squares = gathered_product(blocks_ref, shares_ref, weight_ref, core)
    total = jnp.sum(squares + squares_ref[...], axis=1, keepdims=True)
    logits = (product + product_ref[...]) * lax.rsqrt(total / D + EPSILON)
    logits_ref[...] = logits
    top = jnp.max(logits, axis=1, keepdims=True)
    sums = jnp.sum(jnp.exp(logits - top), axis=1, keepdims=True)
    ids = lax.broadcasted_iota(jnp.int32, (rows, width), 1) + lax.axis_index(SEQ_HEAD) * width
    lines = [tokens_ref[b : b + 1].astype(f32) for b in range(tokens_ref.shape[0])]
    line = jnp.broadcast_to(jnp.concatenate(lines, axis=1), (128, rows))
    tokens = jnp.transpose(line)[:, 0:1].astype(jnp.int32)
    hit = jnp.sum(jnp.where(ids == tokens, logits, 0.0), axis=1, keepdims=True)
    lane = lax.broadcasted_iota(jnp.int32, (rows, 128), 1)
    pair = jnp.transpose(jnp.where(lane == 0, top + jnp.log(sums), hit))[:2]
    for k in range(stats_ref.shape[0]):
        stats_ref[k] = pair
    for b in range(path_ref.shape[0]):
        for k in range(path_ref.shape[1]):
            n = path_ref[b, k] + b * (rows // path_ref.shape[0])
            picked_ref[k, b : b + 1] = logits_ref[pl.ds(n, 1)]


def second_half(blocks, shares, weight, product, squares, path, tokens, copies):
    rows, width = product.shape
    return pl.pallas_call(
        second_kernel,
        in_specs=[pl.BlockSpec(memory_space=pltpu.SMEM)]
        + [pl.BlockSpec(memory_space=pltpu.VMEM)] * 6,
        out_shape=[
            jax.ShapeDtypeStruct((*path.shape[::-1], width), f32),
            jax.ShapeDtypeStruct((copies, 2, 128), f32),
        ],
        scratch_shapes=[pltpu.VMEM((rows, width), f32)],
        compiler_params=room(16),
        name="logits_second",
    )(path, blocks, shares, weight, product, squares, tokens)


def final_kernel(stats_ref, out_ref):
    stats = stats_ref[...]
    top = jnp.max(stats, axis=0)
    total = top + jnp.log(jnp.sum(jnp.exp(stats - top[None]), axis=0))
    result = jnp.sum(stats, axis=0)[1:2] - total[0:1]
    nodes = out_ref.shape[1]
    for b in range(out_ref.shape[0]):
        out_ref[b : b + 1] = result[:, b * nodes : (b + 1) * nodes]


def log_probabilities(stats, batch):
    return pl.pallas_call(
        final_kernel,
        out_shape=jax.ShapeDtypeStruct((batch, stats.shape[2] // batch), f32),
        compiler_params=room(4),
        name="final",
    )(stats)


def to_each(x, axes):
    return lax.all_to_all(x, axes, 0, 0, tiled=True)


def across(x):
    return lax.ppermute(x, "seq_2", [(0, 1), (1, 0)])


def on_device(
    queries,
    cache_keys,
    cache_values,
    new_keys,
    new_values,
    parents,
    path,
    lengths,
    draft_tokens,
    residual,
    out_weight,
    norm_gain,
    vocab_weight,
):
    batch, nodes = parents.shape
    rows = batch * nodes
    chips = lax.axis_size(CHIPS)
    shares = local_attention(
        queries, cache_keys, cache_values, new_keys, new_values, parents, lengths, norm_gain
    )
    shares = to_each(shares, SEQ)
    heads = to_each(join_shares(shares, chips), CHIPS)
    other_heads = across(heads)
    partial, rest = project_first(heads, out_weight)
    partial = project_second(other_heads, rest, partial, lax.axis_size("head"))
    partial = to_each(partial, "head")
    stream = make_stream(partial, residual.reshape(rows, -1), norm_gain, chips)
    mine = to_each(stream, CHIPS)
    other = across(mine)
    product, squares = first_half(mine, shares, vocab_weight)
    copies = lax.axis_size(SEQ_HEAD)
    path_logits, stats = second_half(
        other, shares, vocab_weight, product, squares, path, draft_tokens, copies
    )
    stats = to_each(stats, SEQ_HEAD)
    logprob = log_probabilities(stats, batch)
    return (jnp.transpose(path_logits, (1, 0, 2)), logprob)


def solution(mesh):
    torus = Mesh(
        mesh.devices.reshape(4, 4, 2, mesh.shape["head"]), ("seq_0", "seq_1", "seq_2", "head")
    )
    in_specs = (
        P(None, "head", None, None),
        P(None, "head", SEQ, None),
        P(None, "head", SEQ, None),
        P(None, "head", None, None),
        P(None, "head", None, None),
        P(),
        P(),
        P(),
        P(),
        P(None, None, SEQ),
        P("head", SEQ),
        P(SEQ),
        P(None, SEQ_HEAD),
    )
    out_specs = (P(None, None, SEQ_HEAD), P())
    return jax.shard_map(
        on_device, mesh=torus, in_specs=in_specs, out_specs=out_specs, check_vma=False
    )
```

```python
import functools

import jax
import jax.numpy as jnp
from jax import lax
from jax.experimental import pallas as pl
from jax.experimental.pallas import tpu as pltpu
from jax.sharding import Mesh
from jax.sharding import PartitionSpec as P

D = 8192
SEQ = ("seq_0", "seq_1", "seq_2")
CHIPS = ("seq_1", "seq_0")
SEQ_HEAD = ("seq_0", "seq_1", "seq_2", "head")

HIDDEN = -1e30
FLOOR = -1e25
EPSILON = 1e-5
LOG2E = 1.4426950408889634
ROWS = 256

f32 = jnp.float32
bf16 = jnp.bfloat16


def rows_dot(a, b):
    return lax.dot_general(a, b, (((1,), (1,)), ((), ())), preferred_element_type=f32)


def place_of(chip, side=4):
    return chip % side * side + chip // side


def plain_dot(a, b):
    return lax.dot_general(a, b, (((1,), (0,)), ((), ())), preferred_element_type=f32)


def room(mib):
    return pltpu.CompilerParams(vmem_limit_bytes=mib << 20)


def rows_dot(a, b):
    return lax.dot_general(a, b, (((1,), (1,)), ((), ())), preferred_element_type=f32)


def place_of(chip, side=4):
    return chip % side * side + chip // side


def plain_dot(a, b):
    return lax.dot_general(a, b, (((1,), (0,)), ((), ())), preferred_element_type=f32)


def room(mib):
    return pltpu.CompilerParams(vmem_limit_bytes=mib << 20)


def high_low(x):
    high = x.astype(bf16)
    return high, (x - high.astype(f32)).astype(bf16)


def tree_bias(parents):
    nodes = parents.shape[1]
    column = lax.broadcasted_iota(jnp.int32, (nodes, nodes), 1)
    row = lax.broadcasted_iota(jnp.int32, (nodes, nodes), 0)
    eye = row == column
    linked = jnp.where(jnp.logical_or(parents == row, eye), 1.0, 0.0).astype(bf16)
    reached = rows_dot(jnp.where(eye, 1.0, 0.0).astype(bf16), linked).astype(bf16)
    for _ in range((nodes - 1).bit_length()):
        reached = jnp.minimum(plain_dot(reached, reached), 1.0).astype(bf16)
    return jnp.where(reached.astype(f32) > 0.5, 0.0, HIDDEN)


def attention_kernel(
    lengths_hbm,
    parents_hbm,
    q_hbm,
    k_hbm,
    v_hbm,
    nk_hbm,
    nv_hbm,
    gain_hbm,
    out_ref,
    lengths_ref,
    parents_ref,
    q_ref,
    k_ref,
    v_ref,
    nk_ref,
    nv_ref,
    gain_ref,
    block_sems,
    tree_sems,
    small_sems,
):
    batch, heads, nodes, width = q_ref.shape
    kv, span = k_ref.shape[1:3]
    scale = width**-0.5
    step = scale * LOG2E
    seq = lax.axis_index(SEQ)
    owner = seq == lax.axis_size(SEQ) - 1
    other = jnp.logical_not(owner)
    group = ROWS // nodes
    turns = range(heads // group)
    of_group = heads // group // kv
    ones = jnp.ones((span, width), bf16)

    lengths_copy = pltpu.make_async_copy(lengths_hbm, lengths_ref, small_sems.at[0])
    lengths_copy.start()
    gain_copy = pltpu.make_async_copy(gain_hbm, gain_ref, small_sems.at[1])
    gain_copy.start()

    def block_copy(b, g, n):
        own = pl.ds(g * (heads // kv), heads // kv)
        source, target, place = (
            (q_hbm, q_ref, (b, own)),
            (k_hbm, k_ref, (b, g)),
            (v_hbm, v_ref, (b, g)),
        )[n]
        return pltpu.make_async_copy(source.at[place], target.at[place], block_sems.at[b, g, n])

    for b in range(batch):
        for g in range(kv):
            for n in range(3):
                block_copy(b, g, n).start()
    trees = [
        pltpu.make_async_copy(source, target, tree_sems.at[n])
        for n, (source, target) in enumerate(
            ((parents_hbm, parents_ref), (nk_hbm, nk_ref), (nv_hbm, nv_ref))
        )
    ]

    @pl.when(owner)
    def _():
        for copy in trees:
            copy.start()
        for copy in trees:
            copy.wait()

    lengths_copy.wait()
    gain_copy.wait()
    gain = gain_ref[...].astype(f32)[None]
    gains = gain[:, :width], gain[:, width:]
    row = lax.broadcasted_iota(jnp.int32, (8, width), 0)

    def write(b, part, out, top, total):
        at = b * heads + part * group
        out_ref[pl.ds(at, group), :nodes] = out.astype(bf16).reshape(group, nodes, width)
        lane = lax.broadcasted_iota(jnp.int32, (ROWS, width), 1)
        turned = jnp.transpose(jnp.where(lane == 0, top, total))[:8]
        for h in range(group):
            section = turned[:, h * nodes : (h + 1) * nodes]
            total = section[1:2]
            high = total.astype(bf16).astype(f32)
            lines = jnp.where(row[:, :nodes] == 1, high, total - high)
            lines = jnp.where(row[:, :nodes] == 0, section[0:1], lines)
            tail = jnp.concatenate([lines, jnp.zeros((8, width - nodes), f32)], axis=1)
            for n in range(2):
                tail = jnp.where(row == 3 + n, gains[n], tail)
            out_ref[at + h, nodes:] = tail.astype(bf16)

    def sweep(b, live, with_cache, with_tree):
        biases = []
        if with_cache:
            dead = lax.broadcasted_iota(jnp.int32, (1, span), 1) >= live
            biases.append(jnp.where(dead, HIDDEN, 0.0))
        if with_tree:
            bias = tree_bias(parents_ref[pl.ds(b, 1)])
            biases.append(jnp.concatenate([bias] * group, axis=0))

        def products(part):
            g = part // of_group
            rows = q_ref[b, part * group : (part + 1) * group].reshape(ROWS, width)
            found = [rows_dot(rows, k_ref[b, g])] if with_cache else []
            return found + ([rows_dot(rows, nk_ref[b, g])] if with_tree else [])

        ahead = products(0)
        for part in turns:
            g = part // of_group
            scores = [s + bias for s, bias in zip(ahead, biases)]
            if part + 1 < len(turns):
                ahead = products(part + 1)
            if part % of_group == 0:
                values = [jnp.concatenate([v_ref[b, g], ones], axis=1)] if with_cache else []
                if with_tree:
                    values.append(jnp.concatenate([nv_ref[b, g], ones[:nodes]], axis=1))
            highest = functools.reduce(
                jnp.maximum, [jnp.max(s, axis=1, keepdims=True) for s in scores]
            )
            top = jnp.maximum((highest * scale).astype(bf16).astype(f32), FLOOR)
            shift = top * LOG2E
            result = 0.0
            for s, value in zip(scores, values):
                weights = jnp.exp2(s * step - shift).astype(bf16)
                result = result + plain_dot(weights, value)
            write(b, part, result[:, :width], top, result[:, width:])

    def nothing(b):
        for part in turns:
            zeros = jnp.zeros((ROWS, width), f32)
            write(b, part, zeros, jnp.full((ROWS, 1), FLOOR), zeros)

    @pl.loop(0, batch)
    def _(b):
        live = lengths_ref[b] - seq * span
        for g in range(kv):
            for n in range(3):
                block_copy(b, g, n).wait()
        filled = live > 0
        empty = jnp.logical_not(filled)
        pl.when(jnp.logical_and(filled, other))(functools.partial(sweep, b, live, True, False))
        pl.when(jnp.logical_and(filled, owner))(functools.partial(sweep, b, live, True, True))
        pl.when(jnp.logical_and(empty, owner))(functools.partial(sweep, b, live, False, True))
        pl.when(jnp.logical_and(empty, other))(functools.partial(nothing, b))


def local_attention(
    queries, cache_keys, cache_values, new_keys, new_values, parents, lengths, gain
):
    batch, heads, nodes, width = queries.shape
    kv = cache_keys.shape[1]
    operands = (lengths, parents, queries, cache_keys, cache_values, new_keys, new_values, gain)
    scratch = [pltpu.SMEM(lengths.shape, lengths.dtype)]
    scratch += [pltpu.VMEM(x.shape, x.dtype) for x in operands[1:]]
    scratch += [
        pltpu.SemaphoreType.DMA((batch, kv, 3)),
        pltpu.SemaphoreType.DMA((3,)),
        pltpu.SemaphoreType.DMA((2,)),
    ]
    return pl.pallas_call(
        attention_kernel,
        in_specs=[pl.BlockSpec(memory_space=pltpu.HBM)] * len(operands),
        out_specs=pl.BlockSpec(memory_space=pltpu.VMEM),
        out_shape=jax.ShapeDtypeStruct((batch * heads, nodes + 8, width), bf16),
        scratch_shapes=scratch,
        compiler_params=room(62),
        name="attend",
    )(*operands)


def join_kernel(parts_ref, out_ref):
    count, rows, width = parts_ref.shape
    nodes = rows - 8
    tops = parts_ref[:, nodes, :].astype(f32)
    totals = parts_ref[:, nodes + 1, :].astype(f32) + parts_ref[:, nodes + 2, :].astype(f32)
    used = lax.broadcasted_iota(jnp.int32, (count, width), 1) < nodes
    tops = jnp.where(used, tops, 0.0)
    totals = jnp.where(used, totals, 1.0)
    factors = jnp.exp(tops - jnp.max(tops, axis=0, keepdims=True))
    share = factors / jnp.sum(factors * totals, axis=0, keepdims=True)
    square = jnp.concatenate([share, jnp.zeros((width - count, width), f32)], axis=0)
    turned = jnp.transpose(square)[:nodes]
    total = parts_ref[0, :nodes].astype(f32) * turned[:, 0:1]
    for k in range(1, count):
        total = total + parts_ref[k, :nodes].astype(f32) * turned[:, k : k + 1]
    block = total.astype(bf16)
    for k in range(out_ref.shape[0]):
        out_ref[k] = block


def join_shares(parts, copies):
    rows, width = parts.shape[1:]
    return pl.pallas_call(
        join_kernel,
        out_shape=jax.ShapeDtypeStruct((copies, rows - 8, width), bf16),
        compiler_params=room(8),
        name="join",
    )(parts)


def head_lines(blocks_ref):
    half = blocks_ref.shape[0] // 2
    lines = [
        jnp.concatenate([blocks_ref[place_of(b * half + k)] for k in range(half)], axis=1)
        for b in range(2)
    ]
    return jnp.concatenate(lines, axis=0)


def project_first_kernel(blocks_ref, weight_ref, out_ref, rest_ref):
    chips, nodes, width = blocks_ref.shape
    core = lax.axis_index("seq_2")
    sections = []
    for k in range(chips // 2):
        own = pl.multiple_of((2 * k + core) * width, width)
        other = pl.multiple_of((2 * k + 1 - core) * width, width)
        sections.append(weight_ref[pl.ds(own, width)])
        rest_ref[k * width : (k + 1) * width] = weight_ref[pl.ds(other, width)]
    out_ref[...] = plain_dot(head_lines(blocks_ref), jnp.concatenate(sections, axis=0))


def project_second_kernel(blocks_ref, weight_ref, first_ref, out_ref):
    result = first_ref[...] + plain_dot(head_lines(blocks_ref), weight_ref[...])
    result = result.astype(bf16)
    for k in range(out_ref.shape[0]):
        out_ref[k] = result


def project_first(blocks, weight):
    rows = 2 * blocks.shape[1]
    depth, columns = weight.shape
    return pl.pallas_call(
        project_first_kernel,
        out_shape=[
            jax.ShapeDtypeStruct((rows, columns), f32),
            jax.ShapeDtypeStruct((depth // 2, columns), weight.dtype),
        ],
        cost_estimate=pl.CostEstimate(
            flops=rows * weight.size, bytes_accessed=3 * weight.size, transcendentals=0
        ),
        compiler_params=room(8),
        name="project_first",
    )(blocks, weight)


def project_second(blocks, weight, first, copies):
    return pl.pallas_call(
        project_second_kernel,
        out_shape=jax.ShapeDtypeStruct((copies, *first.shape), bf16),
        compiler_params=room(8),
        name="project_second",
    )(blocks, weight, first)


def stream_kernel(parts_ref, residual_ref, gain_ref, out_ref):
    stream = residual_ref[...].astype(f32)
    for k in range(parts_ref.shape[0]):
        stream = stream + parts_ref[k].astype(f32)
    scaled = (stream * gain_ref[...].astype(f32)[None]).astype(bf16)
    for k in range(out_ref.shape[0]):
        out_ref[k] = scaled


def make_stream(parts, residual, gain, copies):
    rows, columns = residual.shape
    return pl.pallas_call(
        stream_kernel,
        out_shape=jax.ShapeDtypeStruct((copies, rows, columns), bf16),
        compiler_params=room(8),
        name="stream",
    )(parts, residual, gain)


def gathered_product(blocks_ref, shares_ref, weight_ref, core):
    chips, rows, columns = blocks_ref.shape
    nodes = shares_ref.shape[1] - 8
    blocks, sections, squares = [], [], 0.0
    for k in range(chips):
        block = blocks_ref[k]
        blocks.append(block)
        source = 2 * place_of(k) + core
        sections.append(weight_ref[pl.ds(pl.multiple_of(source * columns, columns), columns)])
        gains = shares_ref[source, nodes:].astype(f32)
        for n in range(2):
            inverse = 1.0 / gains[3 + n : 4 + n]
            plain = block[:, n * 128 : (n + 1) * 128].astype(f32) * inverse
            squares = squares + plain * plain
    product = plain_dot(jnp.concatenate(blocks, axis=1), jnp.concatenate(sections, axis=0))
    return product, squares


def first_kernel(blocks_ref, shares_ref, weight_ref, product_ref, squares_ref):
    core = lax.axis_index("seq_2")
    product_ref[...], squares_ref[...] = gathered_product(
        blocks_ref, shares_ref, weight_ref, core
    )


def first_half(blocks, shares, weight):
    chips, rows, columns = blocks.shape
    width = weight.shape[1]
    return pl.pallas_call(
        first_kernel,
        out_shape=[
            jax.ShapeDtypeStruct((rows, width), f32),
            jax.ShapeDtypeStruct((rows, 128), f32),
        ],
        cost_estimate=pl.CostEstimate(
            flops=2 * rows * chips * columns * width,
            bytes_accessed=2 * chips * columns * (rows + width),
            transcendentals=0,
        ),
        compiler_params=room(16),
        name="logits_first",
    )(blocks, shares, weight)


def second_kernel(
    path_ref,
    blocks_ref,
    shares_ref,
    weight_ref,
    product_ref,
    squares_ref,
    tokens_ref,
    picked_ref,
    stats_ref,
    logits_ref,
):
    rows, width = product_ref.shape
    core = 1 - lax.axis_index("seq_2")
    product, squares = gathered_product(blocks_ref, shares_ref, weight_ref, core)
    total = jnp.sum(squares + squares_ref[...], axis=1, keepdims=True)
    logits = (product + product_ref[...]) * lax.rsqrt(total / D + EPSILON)
    logits_ref[...] = logits
    top = jnp.max(logits, axis=1, keepdims=True)
    sums = jnp.sum(jnp.exp(logits - top), axis=1, keepdims=True)
    ids = lax.broadcasted_iota(jnp.int32, (rows, width), 1) + lax.axis_index(SEQ_HEAD) * width
    lines = [tokens_ref[b : b + 1].astype(f32) for b in range(tokens_ref.shape[0])]
    line = jnp.broadcast_to(jnp.concatenate(lines, axis=1), (128, rows))
    tokens = jnp.transpose(line)[:, 0:1].astype(jnp.int32)
    hit = jnp.sum(jnp.where(ids == tokens, logits, 0.0), axis=1, keepdims=True)
    lane = lax.broadcasted_iota(jnp.int32, (rows, 128), 1)
    pair = jnp.transpose(jnp.where(lane == 0, top + jnp.log(sums), hit))[:2]
    for k in range(stats_ref.shape[0]):
        stats_ref[k] = pair
    for b in range(path_ref.shape[0]):
        for k in range(path_ref.shape[1]):
            n = path_ref[b, k] + b * (rows // path_ref.shape[0])
            picked_ref[k, b : b + 1] = logits_ref[pl.ds(n, 1)]


def second_half(blocks, shares, weight, product, squares, path, tokens, copies):
    rows, width = product.shape
    return pl.pallas_call(
        second_kernel,
        in_specs=[pl.BlockSpec(memory_space=pltpu.SMEM)]
        + [pl.BlockSpec(memory_space=pltpu.VMEM)] * 6,
        out_shape=[
            jax.ShapeDtypeStruct((*path.shape[::-1], width), f32),
            jax.ShapeDtypeStruct((copies, 2, 128), f32),
        ],
        scratch_shapes=[pltpu.VMEM((rows, width), f32)],
        compiler_params=room(16),
        name="logits_second",
    )(path, blocks, shares, weight, product, squares, tokens)


def final_kernel(stats_ref, out_ref):
    stats = stats_ref[...]
    top = jnp.max(stats, axis=0)
    total = top + jnp.log(jnp.sum(jnp.exp(stats - top[None]), axis=0))
    result = jnp.sum(stats, axis=0)[1:2] - total[0:1]
    nodes = out_ref.shape[1]
    for b in range(out_ref.shape[0]):
        out_ref[b : b + 1] = result[:, b * nodes : (b + 1) * nodes]


def log_probabilities(stats, batch):
    return pl.pallas_call(
        final_kernel,
        out_shape=jax.ShapeDtypeStruct((batch, stats.shape[2] // batch), f32),
        compiler_params=room(4),
        name="final",
    )(stats)


def to_each(x, axes):
    return lax.all_to_all(x, axes, 0, 0, tiled=True)


def across(x):
    return lax.ppermute(x, "seq_2", [(0, 1), (1, 0)])


def on_device(
    queries,
    cache_keys,
    cache_values,
    new_keys,
    new_values,
    parents,
    path,
    lengths,
    draft_tokens,
    residual,
    out_weight,
    norm_gain,
    vocab_weight,
):
    batch, nodes = parents.shape
    rows = batch * nodes
    chips = lax.axis_size(CHIPS)
    shares = local_attention(
        queries, cache_keys, cache_values, new_keys, new_values, parents, lengths, norm_gain
    )
    shares = to_each(shares, SEQ)
    heads = to_each(join_shares(shares, chips), CHIPS)
    other_heads = across(heads)
    partial, rest = project_first(heads, out_weight)
    partial = project_second(other_heads, rest, partial, lax.axis_size("head"))
    partial = to_each(partial, "head")
    stream = make_stream(partial, residual.reshape(rows, -1), norm_gain, chips)
    mine = to_each(stream, CHIPS)
    other = across(mine)
    product, squares = first_half(mine, shares, vocab_weight)
    copies = lax.axis_size(SEQ_HEAD)
    path_logits, stats = second_half(
        other, shares, vocab_weight, product, squares, path, draft_tokens, copies
    )
    stats = to_each(stats, SEQ_HEAD)
    logprob = log_probabilities(stats, batch)
    return (jnp.transpose(path_logits, (1, 0, 2)), logprob)


def solution(mesh):
    torus = Mesh(
        mesh.devices.reshape(4, 4, 2, mesh.shape["head"]), ("seq_0", "seq_1", "seq_2", "head")
    )
    in_specs = (
        P(None, "head", None, None),
        P(None, "head", SEQ, None),
        P(None, "head", SEQ, None),
        P(None, "head", None, None),
        P(None, "head", None, None),
        P(),
        P(),
        P(),
        P(),
        P(None, None, SEQ),
        P("head", SEQ),
        P(SEQ),
        P(None, SEQ_HEAD),
    )
    out_specs = (P(None, None, SEQ_HEAD), P())
    return jax.shard_map(
        on_device, mesh=torus, in_specs=in_specs, out_specs=out_specs, check_vma=False
    )
```

```python
import functools

import jax
import jax.numpy as jnp
from jax import lax
from jax.experimental import pallas as pl
from jax.experimental.pallas import tpu as pltpu
from jax.sharding import Mesh
from jax.sharding import PartitionSpec as P

D = 8192
SEQ = ("seq_0", "seq_1", "seq_2")
CHIPS = ("seq_1", "seq_0")
SEQ_HEAD = ("seq_0", "seq_1", "seq_2", "head")

HIDDEN = -1e30
FLOOR = -1e25
EPSILON = 1e-5
LOG2E = 1.4426950408889634
ROWS = 256

f32 = jnp.float32
bf16 = jnp.bfloat16


def rows_dot(a, b):
    return lax.dot_general(a, b, (((1,), (1,)), ((), ())), preferred_element_type=f32)


def place_of(chip, side=4):
    return chip % side * side + chip // side


def plain_dot(a, b):
    return lax.dot_general(a, b, (((1,), (0,)), ((), ())), preferred_element_type=f32)


def room(mib):
    return pltpu.CompilerParams(vmem_limit_bytes=mib << 20)


def rows_dot(a, b):
    return lax.dot_general(a, b, (((1,), (1,)), ((), ())), preferred_element_type=f32)


def place_of(chip, side=4):
    return chip % side * side + chip // side


def plain_dot(a, b):
    return lax.dot_general(a, b, (((1,), (0,)), ((), ())), preferred_element_type=f32)


def room(mib):
    return pltpu.CompilerParams(vmem_limit_bytes=mib << 20)


def high_low(x):
    high = x.astype(bf16)
    return high, (x - high.astype(f32)).astype(bf16)


def tree_bias(parents):
    nodes = parents.shape[1]
    column = lax.broadcasted_iota(jnp.int32, (nodes, nodes), 1)
    row = lax.broadcasted_iota(jnp.int32, (nodes, nodes), 0)
    eye = row == column
    linked = jnp.where(jnp.logical_or(parents == row, eye), 1.0, 0.0).astype(bf16)
    reached = rows_dot(jnp.where(eye, 1.0, 0.0).astype(bf16), linked).astype(bf16)
    for _ in range((nodes - 1).bit_length()):
        reached = jnp.minimum(plain_dot(reached, reached), 1.0).astype(bf16)
    return jnp.where(reached.astype(f32) > 0.5, 0.0, HIDDEN)


def attention_kernel(
    lengths_hbm,
    parents_hbm,
    q_hbm,
    k_hbm,
    v_hbm,
    nk_hbm,
    nv_hbm,
    gain_hbm,
    out_ref,
    lengths_ref,
    parents_ref,
    q_ref,
    k_ref,
    v_ref,
    nk_ref,
    nv_ref,
    gain_ref,
    block_sems,
    tree_sems,
    small_sems,
):
    batch, heads, nodes, width = q_ref.shape
    kv, span = k_ref.shape[1:3]
    scale = width**-0.5
    step = scale * LOG2E
    seq = lax.axis_index(SEQ)
    owner = seq == lax.axis_size(SEQ) - 1
    other = jnp.logical_not(owner)
    group = ROWS // nodes
    turns = range(heads // group)
    of_group = heads // group // kv
    ones = jnp.ones((span, width), bf16)

    lengths_copy = pltpu.make_async_copy(lengths_hbm, lengths_ref, small_sems.at[0])
    lengths_copy.start()
    gain_copy = pltpu.make_async_copy(gain_hbm, gain_ref, small_sems.at[1])
    gain_copy.start()

    def block_copy(b, g, n):
        own = pl.ds(g * (heads // kv), heads // kv)
        source, target, place = (
            (q_hbm, q_ref, (b, own)),
            (k_hbm, k_ref, (b, g)),
            (v_hbm, v_ref, (b, g)),
        )[n]
        return pltpu.make_async_copy(source.at[place], target.at[place], block_sems.at[b, g, n])

    for b in range(batch):
        for g in range(kv):
            for n in range(3):
                block_copy(b, g, n).start()
    trees = [
        pltpu.make_async_copy(source, target, tree_sems.at[n])
        for n, (source, target) in enumerate(
            ((parents_hbm, parents_ref), (nk_hbm, nk_ref), (nv_hbm, nv_ref))
        )
    ]

    @pl.when(owner)
    def _():
        for copy in trees:
            copy.start()
        for copy in trees:
            copy.wait()

    lengths_copy.wait()
    gain_copy.wait()
    gain = gain_ref[...].astype(f32)[None]
    gains = gain[:, :width], gain[:, width:]
    row = lax.broadcasted_iota(jnp.int32, (8, width), 0)

    def write(b, part, out, top, total):
        at = b * heads + part * group
        out_ref[pl.ds(at, group), :nodes] = out.astype(bf16).reshape(group, nodes, width)
        lane = lax.broadcasted_iota(jnp.int32, (ROWS, width), 1)
        turned = jnp.transpose(jnp.where(lane == 0, top, total))[:8]
        for h in range(group):
            section = turned[:, h * nodes : (h + 1) * nodes]
            total = section[1:2]
            high = total.astype(bf16).astype(f32)
            lines = jnp.where(row[:, :nodes] == 1, high, total - high)
            lines = jnp.where(row[:, :nodes] == 0, section[0:1], lines)
            tail = jnp.concatenate([lines, jnp.zeros((8, width - nodes), f32)], axis=1)
            for n in range(2):
                tail = jnp.where(row == 3 + n, gains[n], tail)
            out_ref[at + h, nodes:] = tail.astype(bf16)

    def sweep(b, live, with_cache, with_tree):
        biases = []
        if with_cache:
            dead = lax.broadcasted_iota(jnp.int32, (1, span), 1) >= live
            biases.append(jnp.where(dead, HIDDEN, 0.0))
        if with_tree:
            bias = tree_bias(parents_ref[pl.ds(b, 1)])
            biases.append(jnp.concatenate([bias] * group, axis=0))

        def products(part):
            g = part // of_group
            rows = q_ref[b, part * group : (part + 1) * group].reshape(ROWS, width)
            found = [rows_dot(rows, k_ref[b, g])] if with_cache else []
            return found + ([rows_dot(rows, nk_ref[b, g])] if with_tree else [])

        ahead = products(0)
        for part in turns:
            g = part // of_group
            scores = [s + bias for s, bias in zip(ahead, biases)]
            if part + 1 < len(turns):
                ahead = products(part + 1)
            if part % of_group == 0:
                values = [jnp.concatenate([v_ref[b, g], ones], axis=1)] if with_cache else []
                if with_tree:
                    values.append(jnp.concatenate([nv_ref[b, g], ones[:nodes]], axis=1))
            highest = functools.reduce(
                jnp.maximum, [jnp.max(s, axis=1, keepdims=True) for s in scores]
            )
            top = jnp.maximum((highest * scale).astype(bf16).astype(f32), FLOOR)
            shift = top * LOG2E
            result = 0.0
            for s, value in zip(scores, values):
                weights = jnp.exp2(s * step - shift).astype(bf16)
                result = result + plain_dot(weights, value)
            write(b, part, result[:, :width], top, result[:, width:])

    def nothing(b):
        for part in turns:
            zeros = jnp.zeros((ROWS, width), f32)
            write(b, part, zeros, jnp.full((ROWS, 1), FLOOR), zeros)

    @pl.loop(0, batch)
    def _(b):
        live = lengths_ref[b] - seq * span
        for g in range(kv):
            for n in range(3):
                block_copy(b, g, n).wait()
        filled = live > 0
        empty = jnp.logical_not(filled)
        pl.when(jnp.logical_and(filled, other))(functools.partial(sweep, b, live, True, False))
        pl.when(jnp.logical_and(filled, owner))(functools.partial(sweep, b, live, True, True))
        pl.when(jnp.logical_and(empty, owner))(functools.partial(sweep, b, live, False, True))
        pl.when(jnp.logical_and(empty, other))(functools.partial(nothing, b))


def local_attention(
    queries, cache_keys, cache_values, new_keys, new_values, parents, lengths, gain
):
    batch, heads, nodes, width = queries.shape
    kv = cache_keys.shape[1]
    operands = (lengths, parents, queries, cache_keys, cache_values, new_keys, new_values, gain)
    scratch = [pltpu.SMEM(lengths.shape, lengths.dtype)]
    scratch += [pltpu.VMEM(x.shape, x.dtype) for x in operands[1:]]
    scratch += [
        pltpu.SemaphoreType.DMA((batch, kv, 3)),
        pltpu.SemaphoreType.DMA((3,)),
        pltpu.SemaphoreType.DMA((2,)),
    ]
    return pl.pallas_call(
        attention_kernel,
        in_specs=[pl.BlockSpec(memory_space=pltpu.HBM)] * len(operands),
        out_specs=pl.BlockSpec(memory_space=pltpu.VMEM),
        out_shape=jax.ShapeDtypeStruct((batch * heads, nodes + 8, width), bf16),
        scratch_shapes=scratch,
        compiler_params=room(62),
        name="attend",
    )(*operands)


def join_kernel(parts_ref, out_ref):
    count, rows, width = parts_ref.shape
    nodes = rows - 8
    tops = parts_ref[:, nodes, :].astype(f32)
    totals = parts_ref[:, nodes + 1, :].astype(f32) + parts_ref[:, nodes + 2, :].astype(f32)
    used = lax.broadcasted_iota(jnp.int32, (count, width), 1) < nodes
    tops = jnp.where(used, tops, 0.0)
    totals = jnp.where(used, totals, 1.0)
    factors = jnp.exp(tops - jnp.max(tops, axis=0, keepdims=True))
    share = factors / jnp.sum(factors * totals, axis=0, keepdims=True)
    square = jnp.concatenate([share, jnp.zeros((width - count, width), f32)], axis=0)
    turned = jnp.transpose(square)[:nodes]
    total = parts_ref[0, :nodes].astype(f32) * turned[:, 0:1]
    for k in range(1, count):
        total = total + parts_ref[k, :nodes].astype(f32) * turned[:, k : k + 1]
    block = total.astype(bf16)
    for k in range(out_ref.shape[0]):
        out_ref[k] = block


def join_shares(parts, copies):
    rows, width = parts.shape[1:]
    return pl.pallas_call(
        join_kernel,
        out_shape=jax.ShapeDtypeStruct((copies, rows - 8, width), bf16),
        compiler_params=room(8),
        name="join",
    )(parts)


def head_lines(blocks_ref):
    half = blocks_ref.shape[0] // 2
    lines = [
        jnp.concatenate([blocks_ref[place_of(b * half + k)] for k in range(half)], axis=1)
        for b in range(2)
    ]
    return jnp.concatenate(lines, axis=0)


def project_first_kernel(blocks_ref, weight_ref, out_ref, rest_ref):
    chips, nodes, width = blocks_ref.shape
    core = lax.axis_index("seq_2")
    sections = []
    for k in range(chips // 2):
        own = pl.multiple_of((2 * k + core) * width, width)
        other = pl.multiple_of((2 * k + 1 - core) * width, width)
        sections.append(weight_ref[pl.ds(own, width)])
        rest_ref[k * width : (k + 1) * width] = weight_ref[pl.ds(other, width)]
    out_ref[...] = plain_dot(head_lines(blocks_ref), jnp.concatenate(sections, axis=0))


def project_second_kernel(blocks_ref, weight_ref, first_ref, out_ref):
    result = first_ref[...] + plain_dot(head_lines(blocks_ref), weight_ref[...])
    result = result.astype(bf16)
    for k in range(out_ref.shape[0]):
        out_ref[k] = result


def project_first(blocks, weight):
    rows = 2 * blocks.shape[1]
    depth, columns = weight.shape
    return pl.pallas_call(
        project_first_kernel,
        out_shape=[
            jax.ShapeDtypeStruct((rows, columns), f32),
            jax.ShapeDtypeStruct((depth // 2, columns), weight.dtype),
        ],
        cost_estimate=pl.CostEstimate(
            flops=rows * weight.size, bytes_accessed=3 * weight.size, transcendentals=0
        ),
        compiler_params=room(8),
        name="project_first",
    )(blocks, weight)


def project_second(blocks, weight, first, copies):
    return pl.pallas_call(
        project_second_kernel,
        out_shape=jax.ShapeDtypeStruct((copies, *first.shape), bf16),
        compiler_params=room(8),
        name="project_second",
    )(blocks, weight, first)


def stream_kernel(parts_ref, residual_ref, gain_ref, out_ref):
    stream = residual_ref[...].astype(f32)
    for k in range(parts_ref.shape[0]):
        stream = stream + parts_ref[k].astype(f32)
    scaled = (stream * gain_ref[...].astype(f32)[None]).astype(bf16)
    for k in range(out_ref.shape[0]):
        out_ref[k] = scaled


def make_stream(parts, residual, gain, copies):
    rows, columns = residual.shape
    return pl.pallas_call(
        stream_kernel,
        out_shape=jax.ShapeDtypeStruct((copies, rows, columns), bf16),
        compiler_params=room(8),
        name="stream",
    )(parts, residual, gain)


def gathered_product(blocks_ref, shares_ref, weight_ref, core):
    chips, rows, columns = blocks_ref.shape
    nodes = shares_ref.shape[1] - 8
    blocks, sections, squares = [], [], 0.0
    for k in range(chips):
        block = blocks_ref[k]
        blocks.append(block)
        source = 2 * place_of(k) + core
        sections.append(weight_ref[pl.ds(pl.multiple_of(source * columns, columns), columns)])
        gains = shares_ref[source, nodes:].astype(f32)
        for n in range(2):
            inverse = 1.0 / gains[3 + n : 4 + n]
            plain = block[:, n * 128 : (n + 1) * 128].astype(f32) * inverse
            squares = squares + plain * plain
    product = plain_dot(jnp.concatenate(blocks, axis=1), jnp.concatenate(sections, axis=0))
    return product, squares


def first_kernel(blocks_ref, shares_ref, weight_ref, product_ref, squares_ref):
    core = lax.axis_index("seq_2")
    product_ref[...], squares_ref[...] = gathered_product(
        blocks_ref, shares_ref, weight_ref, core
    )


def first_half(blocks, shares, weight):
    chips, rows, columns = blocks.shape
    width = weight.shape[1]
    return pl.pallas_call(
        first_kernel,
        out_shape=[
            jax.ShapeDtypeStruct((rows, width), f32),
            jax.ShapeDtypeStruct((rows, 128), f32),
        ],
        cost_estimate=pl.CostEstimate(
            flops=2 * rows * chips * columns * width,
            bytes_accessed=2 * chips * columns * (rows + width),
            transcendentals=0,
        ),
        compiler_params=room(16),
        name="logits_first",
    )(blocks, shares, weight)


def second_kernel(
    blocks_ref, shares_ref, weight_ref, product_ref, squares_ref, tokens_ref, logits_ref, stats_ref
):
    rows, width = product_ref.shape
    core = 1 - lax.axis_index("seq_2")
    product, squares = gathered_product(blocks_ref, shares_ref, weight_ref, core)
    total = jnp.sum(squares + squares_ref[...], axis=1, keepdims=True)
    logits = (product + product_ref[...]) * lax.rsqrt(total / D + EPSILON)
    logits_ref[...] = logits
    top = jnp.max(logits, axis=1, keepdims=True)
    sums = jnp.sum(jnp.exp(logits - top), axis=1, keepdims=True)
    ids = lax.broadcasted_iota(jnp.int32, (rows, width), 1) + lax.axis_index(SEQ_HEAD) * width
    lines = [tokens_ref[b : b + 1].astype(f32) for b in range(tokens_ref.shape[0])]
    line = jnp.broadcast_to(jnp.concatenate(lines, axis=1), (128, rows))
    tokens = jnp.transpose(line)[:, 0:1].astype(jnp.int32)
    hit = jnp.sum(jnp.where(ids == tokens, logits, 0.0), axis=1, keepdims=True)
    lane = lax.broadcasted_iota(jnp.int32, (rows, 128), 1)
    turned = jnp.transpose(jnp.where(lane % 2 == 0, top + jnp.log(sums), hit))[:8]
    for k in range(stats_ref.shape[0] // 8):
        stats_ref[k * 8 : k * 8 + 8] = turned


def second_half(blocks, shares, weight, product, squares, tokens, copies):
    return pl.pallas_call(
        second_kernel,
        out_shape=[
            jax.ShapeDtypeStruct(product.shape, f32),
            jax.ShapeDtypeStruct((copies * 2, 128), f32),
        ],
        compiler_params=room(16),
        name="logits_second",
    )(blocks, shares, weight, product, squares, tokens)


def final_kernel(path_ref, stats_ref, logits_ref, picked_ref, out_ref):
    batch, nodes = out_ref.shape
    for b in range(batch):
        for k in range(path_ref.shape[1]):
            picked_ref[k, b : b + 1] = logits_ref[pl.ds(path_ref[b, k] + b * nodes, 1)]
    stats = stats_ref[...]
    is_sum = lax.broadcasted_iota(jnp.int32, stats.shape, 0) % 2 == 0
    sums = jnp.where(is_sum, stats, HIDDEN)
    top = jnp.max(sums, axis=0, keepdims=True)
    total = top + jnp.log(jnp.sum(jnp.exp(sums - top), axis=0, keepdims=True))
    result = jnp.sum(jnp.where(is_sum, 0.0, stats), axis=0, keepdims=True) - total
    for b in range(batch):
        out_ref[b : b + 1] = result[:, b * nodes : (b + 1) * nodes]


def final_join(path, stats, logits):
    batch = path.shape[0]
    rows, width = logits.shape
    return pl.pallas_call(
        final_kernel,
        in_specs=[
            pl.BlockSpec(memory_space=pltpu.SMEM),
            pl.BlockSpec(memory_space=pltpu.VMEM),
            pl.BlockSpec(memory_space=pltpu.VMEM),
        ],
        out_shape=[
            jax.ShapeDtypeStruct((*path.shape[::-1], width), f32),
            jax.ShapeDtypeStruct((batch, rows // batch), f32),
        ],
        compiler_params=room(4),
        name="final",
    )(path, stats, logits)


def to_each(x, axes):
    return lax.all_to_all(x, axes, 0, 0, tiled=True)


def across(x):
    return lax.ppermute(x, "seq_2", [(0, 1), (1, 0)])


def on_device(
    queries,
    cache_keys,
    cache_values,
    new_keys,
    new_values,
    parents,
    path,
    lengths,
    draft_tokens,
    residual,
    out_weight,
    norm_gain,
    vocab_weight,
):
    rows = parents.size
    chips = lax.axis_size(CHIPS)
    shares = local_attention(
        queries, cache_keys, cache_values, new_keys, new_values, parents, lengths, norm_gain
    )
    shares = to_each(shares, SEQ)
    heads = to_each(join_shares(shares, chips), CHIPS)
    other_heads = across(heads)
    partial, rest = project_first(heads, out_weight)
    partial = project_second(other_heads, rest, partial, lax.axis_size("head"))
    partial = to_each(partial, "head")
    stream = make_stream(partial, residual.reshape(rows, -1), norm_gain, chips)
    mine = to_each(stream, CHIPS)
    other = across(mine)
    product, squares = first_half(mine, shares, vocab_weight)
    copies = lax.axis_size(SEQ_HEAD)
    logits, stats = second_half(
        other, shares, vocab_weight, product, squares, draft_tokens, copies
    )
    stats = to_each(stats.reshape(copies, 2, 128), SEQ_HEAD).reshape(copies * 2, 128)
    path_logits, logprob = final_join(path, stats, logits)
    return (jnp.transpose(path_logits, (1, 0, 2)), logprob)


def solution(mesh):
    torus = Mesh(
        mesh.devices.reshape(4, 4, 2, mesh.shape["head"]), ("seq_0", "seq_1", "seq_2", "head")
    )
    in_specs = (
        P(None, "head", None, None),
        P(None, "head", SEQ, None),
        P(None, "head", SEQ, None),
        P(None, "head", None, None),
        P(None, "head", None, None),
        P(),
        P(),
        P(),
        P(),
        P(None, None, SEQ),
        P("head", SEQ),
        P(SEQ),
        P(None, SEQ_HEAD),
    )
    out_specs = (P(None, None, SEQ_HEAD), P())
    return jax.shard_map(
        on_device, mesh=torus, in_specs=in_specs, out_specs=out_specs, check_vma=False
    )
```

```python
import functools

import jax
import jax.numpy as jnp
from jax import lax
from jax.experimental import pallas as pl
from jax.experimental.pallas import tpu as pltpu
from jax.sharding import Mesh
from jax.sharding import PartitionSpec as P

D = 8192
SEQ = ("seq_0", "seq_1", "seq_2")
CHIPS = ("seq_1", "seq_0")
SEQ_HEAD = ("seq_0", "seq_1", "seq_2", "head")

HIDDEN = -1e30
FLOOR = -1e25
EPSILON = 1e-5
LOG2E = 1.4426950408889634
ROWS = 256

f32 = jnp.float32
bf16 = jnp.bfloat16


def rows_dot(a, b):
    return lax.dot_general(a, b, (((1,), (1,)), ((), ())), preferred_element_type=f32)


def place_of(chip, side=4):
    return chip % side * side + chip // side


def plain_dot(a, b):
    return lax.dot_general(a, b, (((1,), (0,)), ((), ())), preferred_element_type=f32)


def room(mib):
    return pltpu.CompilerParams(vmem_limit_bytes=mib << 20)


def rows_dot(a, b):
    return lax.dot_general(a, b, (((1,), (1,)), ((), ())), preferred_element_type=f32)


def place_of(chip, side=4):
    return chip % side * side + chip // side


def plain_dot(a, b):
    return lax.dot_general(a, b, (((1,), (0,)), ((), ())), preferred_element_type=f32)


def room(mib):
    return pltpu.CompilerParams(vmem_limit_bytes=mib << 20)


def high_low(x):
    high = x.astype(bf16)
    return high, (x - high.astype(f32)).astype(bf16)


def tree_bias(parents):
    nodes = parents.shape[1]
    column = lax.broadcasted_iota(jnp.int32, (nodes, nodes), 1)
    row = lax.broadcasted_iota(jnp.int32, (nodes, nodes), 0)
    eye = row == column
    linked = jnp.where(jnp.logical_or(parents == row, eye), 1.0, 0.0).astype(bf16)
    reached = rows_dot(jnp.where(eye, 1.0, 0.0).astype(bf16), linked).astype(bf16)
    for _ in range((nodes - 1).bit_length()):
        reached = jnp.minimum(plain_dot(reached, reached), 1.0).astype(bf16)
    return jnp.where(reached.astype(f32) > 0.5, 0.0, HIDDEN)


def attention_kernel(
    lengths_hbm,
    parents_hbm,
    q_hbm,
    k_hbm,
    v_hbm,
    nk_hbm,
    nv_hbm,
    gain_hbm,
    out_ref,
    lengths_ref,
    parents_ref,
    q_ref,
    k_ref,
    v_ref,
    nk_ref,
    nv_ref,
    gain_ref,
    block_sems,
    tree_sems,
    small_sems,
):
    batch, heads, nodes, width = q_ref.shape
    kv, span = k_ref.shape[1:3]
    scale = width**-0.5
    step = scale * LOG2E
    seq = lax.axis_index(SEQ)
    owner = seq == lax.axis_size(SEQ) - 1
    other = jnp.logical_not(owner)
    group = ROWS // nodes
    turns = range(heads // group)
    of_group = heads // group // kv
    ones = jnp.ones((span, width), bf16)

    lengths_copy = pltpu.make_async_copy(lengths_hbm, lengths_ref, small_sems.at[0])
    lengths_copy.start()
    gain_copy = pltpu.make_async_copy(gain_hbm, gain_ref, small_sems.at[1])
    gain_copy.start()

    def block_copy(b, g, n):
        own = pl.ds(g * (heads // kv), heads // kv)
        source, target, place = (
            (q_hbm, q_ref, (b, own)),
            (k_hbm, k_ref, (b, g)),
            (v_hbm, v_ref, (b, g)),
        )[n]
        return pltpu.make_async_copy(source.at[place], target.at[place], block_sems.at[b, g, n])

    for b in range(batch):
        for g in range(kv):
            for n in range(3):
                block_copy(b, g, n).start()
    trees = [
        pltpu.make_async_copy(source, target, tree_sems.at[n])
        for n, (source, target) in enumerate(
            ((parents_hbm, parents_ref), (nk_hbm, nk_ref), (nv_hbm, nv_ref))
        )
    ]

    @pl.when(owner)
    def _():
        for copy in trees:
            copy.start()
        for copy in trees:
            copy.wait()

    lengths_copy.wait()
    gain_copy.wait()
    gain = gain_ref[...].astype(f32)[None]
    gains = gain[:, :width], gain[:, width:]
    row = lax.broadcasted_iota(jnp.int32, (8, width), 0)

    def write(b, part, out, top, total):
        at = b * heads + part * group
        out_ref[pl.ds(at, group), :nodes] = out.astype(bf16).reshape(group, nodes, width)
        lane = lax.broadcasted_iota(jnp.int32, (ROWS, width), 1)
        turned = jnp.transpose(jnp.where(lane == 0, top, total))[:8]
        for h in range(group):
            section = turned[:, h * nodes : (h + 1) * nodes]
            total = section[1:2]
            high = total.astype(bf16).astype(f32)
            lines = jnp.where(row[:, :nodes] == 1, high, total - high)
            lines = jnp.where(row[:, :nodes] == 0, section[0:1], lines)
            tail = jnp.concatenate([lines, jnp.zeros((8, width - nodes), f32)], axis=1)
            for n in range(2):
                tail = jnp.where(row == 3 + n, gains[n], tail)
            out_ref[at + h, nodes:] = tail.astype(bf16)

    def sweep(b, live, with_cache, with_tree):
        biases = []
        if with_cache:
            dead = lax.broadcasted_iota(jnp.int32, (1, span), 1) >= live
            biases.append(jnp.where(dead, HIDDEN, 0.0))
        if with_tree:
            bias = tree_bias(parents_ref[pl.ds(b, 1)])
            biases.append(jnp.concatenate([bias] * group, axis=0))

        def products(part):
            g = part // of_group
            rows = q_ref[b, part * group : (part + 1) * group].reshape(ROWS, width)
            found = [rows_dot(rows, k_ref[b, g])] if with_cache else []
            return found + ([rows_dot(rows, nk_ref[b, g])] if with_tree else [])

        ahead = products(0)
        for part in turns:
            g = part // of_group
            scores = [s + bias for s, bias in zip(ahead, biases)]
            if part + 1 < len(turns):
                ahead = products(part + 1)
            if part % of_group == 0:
                values = [jnp.concatenate([v_ref[b, g], ones], axis=1)] if with_cache else []
                if with_tree:
                    values.append(jnp.concatenate([nv_ref[b, g], ones[:nodes]], axis=1))
            highest = functools.reduce(
                jnp.maximum, [jnp.max(s, axis=1, keepdims=True) for s in scores]
            )
            top = jnp.maximum((highest * scale).astype(bf16).astype(f32), FLOOR)
            shift = top * LOG2E
            result = 0.0
            for s, value in zip(scores, values):
                weights = jnp.exp2(s * step - shift).astype(bf16)
                result = result + plain_dot(weights, value)
            write(b, part, result[:, :width], top, result[:, width:])

    def nothing(b):
        for part in turns:
            zeros = jnp.zeros((ROWS, width), f32)
            write(b, part, zeros, jnp.full((ROWS, 1), FLOOR), zeros)

    @pl.loop(0, batch)
    def _(b):
        live = lengths_ref[b] - seq * span
        for g in range(kv):
            for n in range(3):
                block_copy(b, g, n).wait()
        filled = live > 0
        empty = jnp.logical_not(filled)
        pl.when(jnp.logical_and(filled, other))(functools.partial(sweep, b, live, True, False))
        pl.when(jnp.logical_and(filled, owner))(functools.partial(sweep, b, live, True, True))
        pl.when(jnp.logical_and(empty, owner))(functools.partial(sweep, b, live, False, True))
        pl.when(jnp.logical_and(empty, other))(functools.partial(nothing, b))


def local_attention(
    queries, cache_keys, cache_values, new_keys, new_values, parents, lengths, gain
):
    batch, heads, nodes, width = queries.shape
    kv = cache_keys.shape[1]
    operands = (lengths, parents, queries, cache_keys, cache_values, new_keys, new_values, gain)
    scratch = [pltpu.SMEM(lengths.shape, lengths.dtype)]
    scratch += [pltpu.VMEM(x.shape, x.dtype) for x in operands[1:]]
    scratch += [
        pltpu.SemaphoreType.DMA((batch, kv, 3)),
        pltpu.SemaphoreType.DMA((3,)),
        pltpu.SemaphoreType.DMA((2,)),
    ]
    return pl.pallas_call(
        attention_kernel,
        in_specs=[pl.BlockSpec(memory_space=pltpu.HBM)] * len(operands),
        out_specs=pl.BlockSpec(memory_space=pltpu.VMEM),
        out_shape=jax.ShapeDtypeStruct((batch * heads, nodes + 8, width), bf16),
        scratch_shapes=scratch,
        compiler_params=room(62),
        name="attend",
    )(*operands)


def join_kernel(parts_ref, out_ref):
    count, rows, width = parts_ref.shape
    nodes = rows - 8
    tops = parts_ref[:, nodes, :].astype(f32)
    totals = parts_ref[:, nodes + 1, :].astype(f32) + parts_ref[:, nodes + 2, :].astype(f32)
    used = lax.broadcasted_iota(jnp.int32, (count, width), 1) < nodes
    tops = jnp.where(used, tops, 0.0)
    totals = jnp.where(used, totals, 1.0)
    factors = jnp.exp(tops - jnp.max(tops, axis=0, keepdims=True))
    share = factors / jnp.sum(factors * totals, axis=0, keepdims=True)
    square = jnp.concatenate([share, jnp.zeros((width - count, width), f32)], axis=0)
    turned = jnp.transpose(square)[:nodes]
    total = parts_ref[0, :nodes].astype(f32) * turned[:, 0:1]
    for k in range(1, count):
        total = total + parts_ref[k, :nodes].astype(f32) * turned[:, k : k + 1]
    block = total.astype(bf16)
    for k in range(out_ref.shape[0]):
        out_ref[k] = block


def join_shares(parts, copies):
    rows, width = parts.shape[1:]
    return pl.pallas_call(
        join_kernel,
        out_shape=jax.ShapeDtypeStruct((copies, rows - 8, width), bf16),
        compiler_params=room(8),
        name="join",
    )(parts)


def head_lines(blocks_ref):
    half = blocks_ref.shape[0] // 2
    lines = [
        jnp.concatenate([blocks_ref[place_of(b * half + k)] for k in range(half)], axis=1)
        for b in range(2)
    ]
    return jnp.concatenate(lines, axis=0)


def project_first_kernel(blocks_ref, weight_ref, out_ref, rest_ref):
    chips, nodes, width = blocks_ref.shape
    core = lax.axis_index("seq_2")
    sections = []
    for k in range(chips // 2):
        own = pl.multiple_of((2 * k + core) * width, width)
        other = pl.multiple_of((2 * k + 1 - core) * width, width)
        sections.append(weight_ref[pl.ds(own, width)])
        rest_ref[k * width : (k + 1) * width] = weight_ref[pl.ds(other, width)]
    out_ref[...] = plain_dot(head_lines(blocks_ref), jnp.concatenate(sections, axis=0))


def project_second_kernel(blocks_ref, weight_ref, first_ref, out_ref):
    result = first_ref[...] + plain_dot(head_lines(blocks_ref), weight_ref[...])
    result = result.astype(bf16)
    for k in range(out_ref.shape[0]):
        out_ref[k] = result


def project_first(blocks, weight):
    rows = 2 * blocks.shape[1]
    depth, columns = weight.shape
    return pl.pallas_call(
        project_first_kernel,
        out_shape=[
            jax.ShapeDtypeStruct((rows, columns), f32),
            jax.ShapeDtypeStruct((depth // 2, columns), weight.dtype),
        ],
        cost_estimate=pl.CostEstimate(
            flops=rows * weight.size, bytes_accessed=3 * weight.size, transcendentals=0
        ),
        compiler_params=room(8),
        name="project_first",
    )(blocks, weight)


def project_second(blocks, weight, first, copies):
    return pl.pallas_call(
        project_second_kernel,
        out_shape=jax.ShapeDtypeStruct((copies, *first.shape), bf16),
        compiler_params=room(8),
        name="project_second",
    )(blocks, weight, first)


def stream_kernel(parts_ref, residual_ref, gain_ref, out_ref):
    stream = residual_ref[...].astype(f32)
    for k in range(parts_ref.shape[0]):
        stream = stream + parts_ref[k].astype(f32)
    scaled = (stream * gain_ref[...].astype(f32)[None]).astype(bf16)
    for k in range(out_ref.shape[0]):
        out_ref[k] = scaled


def make_stream(parts, residual, gain, copies):
    rows, columns = residual.shape
    return pl.pallas_call(
        stream_kernel,
        out_shape=jax.ShapeDtypeStruct((copies, rows, columns), bf16),
        compiler_params=room(8),
        name="stream",
    )(parts, residual, gain)


def gathered_product(blocks_ref, weight_ref):
    chips, rows, columns = blocks_ref.shape
    core = lax.axis_index("seq_2")
    blocks, sections = [], []
    for k in range(chips):
        start = pl.multiple_of((2 * place_of(k) + core) * columns, columns)
        blocks.append(blocks_ref[k])
        sections.append(weight_ref[pl.ds(start, columns)])
    return plain_dot(jnp.concatenate(blocks, axis=1), jnp.concatenate(sections, axis=0))


def sent_kernel(blocks_ref, shares_ref, weight_ref, out_ref):
    chips = blocks_ref.shape[0]
    width = weight_ref.shape[1]
    nodes = shares_ref.shape[1] - 8
    core = lax.axis_index("seq_2")
    squares = 0.0
    for k in range(chips):
        gains = shares_ref[2 * place_of(k) + core, nodes:].astype(f32)
        for n in range(2):
            inverse = 1.0 / gains[3 + n : 4 + n]
            plain = blocks_ref[k, :, n * 128 : (n + 1) * 128].astype(f32) * inverse
            squares = squares + plain * plain
    out_ref[:, :width] = gathered_product(blocks_ref, weight_ref)
    out_ref[:, width:] = squares


def kept_kernel(blocks_ref, weight_ref, out_ref):
    out_ref[...] = gathered_product(blocks_ref, weight_ref)


def product_cost(blocks, weight):
    chips, rows, columns = blocks.shape
    return pl.CostEstimate(
        flops=2 * blocks.size * weight.shape[1],
        bytes_accessed=2 * chips * columns * (rows + weight.shape[1]),
        transcendentals=0,
    )


def sent_product(blocks, shares, weight):
    return pl.pallas_call(
        sent_kernel,
        out_shape=jax.ShapeDtypeStruct((blocks.shape[1], weight.shape[1] + 128), f32),
        cost_estimate=product_cost(blocks, weight),
        compiler_params=room(16),
        name="logits_sent",
    )(blocks, shares, weight)


def kept_product(blocks, weight):
    return pl.pallas_call(
        kept_kernel,
        out_shape=jax.ShapeDtypeStruct((blocks.shape[1], weight.shape[1]), f32),
        cost_estimate=product_cost(blocks, weight),
        compiler_params=room(16),
        name="logits_kept",
    )(blocks, weight)


def statistics_kernel(kept_ref, sent_ref, received_ref, tokens_ref, logits_ref, stats_ref):
    rows, width = kept_ref.shape
    squares = sent_ref[:, width:] + received_ref[:, width:]
    total = jnp.sum(squares, axis=1, keepdims=True)
    logits = (kept_ref[...] + received_ref[:, :width]) * lax.rsqrt(total / D + EPSILON)
    logits_ref[...] = logits
    top = jnp.max(logits, axis=1, keepdims=True)
    sums = jnp.sum(jnp.exp(logits - top), axis=1, keepdims=True)
    ids = lax.broadcasted_iota(jnp.int32, (rows, width), 1) + lax.axis_index(SEQ_HEAD) * width
    lines = [tokens_ref[b : b + 1].astype(f32) for b in range(tokens_ref.shape[0])]
    line = jnp.broadcast_to(jnp.concatenate(lines, axis=1), (128, rows))
    tokens = jnp.transpose(line)[:, 0:1].astype(jnp.int32)
    hit = jnp.sum(jnp.where(ids == tokens, logits, 0.0), axis=1, keepdims=True)
    lane = lax.broadcasted_iota(jnp.int32, (rows, 128), 1)
    turned = jnp.transpose(jnp.where(lane % 2 == 0, top + jnp.log(sums), hit))[:8]
    for k in range(stats_ref.shape[0] // 8):
        stats_ref[k * 8 : k * 8 + 8] = turned


def logit_statistics(kept, sent, received, tokens, copies):
    return pl.pallas_call(
        statistics_kernel,
        out_shape=[
            jax.ShapeDtypeStruct(kept.shape, f32),
            jax.ShapeDtypeStruct((copies * 2, 128), f32),
        ],
        compiler_params=room(8),
        name="logits_statistics",
    )(kept, sent, received, tokens)


def final_kernel(path_ref, stats_ref, logits_ref, picked_ref, out_ref):
    batch, nodes = out_ref.shape
    for b in range(batch):
        for k in range(path_ref.shape[1]):
            picked_ref[k, b : b + 1] = logits_ref[pl.ds(path_ref[b, k] + b * nodes, 1)]
    stats = stats_ref[...]
    is_sum = lax.broadcasted_iota(jnp.int32, stats.shape, 0) % 2 == 0
    sums = jnp.where(is_sum, stats, HIDDEN)
    top = jnp.max(sums, axis=0, keepdims=True)
    total = top + jnp.log(jnp.sum(jnp.exp(sums - top), axis=0, keepdims=True))
    result = jnp.sum(jnp.where(is_sum, 0.0, stats), axis=0, keepdims=True) - total
    for b in range(batch):
        out_ref[b : b + 1] = result[:, b * nodes : (b + 1) * nodes]


def final_join(path, stats, logits):
    batch = path.shape[0]
    rows, width = logits.shape
    return pl.pallas_call(
        final_kernel,
        in_specs=[
            pl.BlockSpec(memory_space=pltpu.SMEM),
            pl.BlockSpec(memory_space=pltpu.VMEM),
            pl.BlockSpec(memory_space=pltpu.VMEM),
        ],
        out_shape=[
            jax.ShapeDtypeStruct((*path.shape[::-1], width), f32),
            jax.ShapeDtypeStruct((batch, rows // batch), f32),
        ],
        compiler_params=room(4),
        name="final",
    )(path, stats, logits)


def to_each(x, axes):
    return lax.all_to_all(x, axes, 0, 0, tiled=True)


def across(x):
    return lax.ppermute(x, "seq_2", [(0, 1), (1, 0)])


def on_device(
    queries,
    cache_keys,
    cache_values,
    new_keys,
    new_values,
    parents,
    path,
    lengths,
    draft_tokens,
    residual,
    out_weight,
    norm_gain,
    vocab_weight,
):
    rows = parents.size
    chips = lax.axis_size(CHIPS)
    shares = local_attention(
        queries, cache_keys, cache_values, new_keys, new_values, parents, lengths, norm_gain
    )
    shares, own_weight = lax.optimization_barrier((shares, vocab_weight))
    other_weight = across(own_weight)
    shares = to_each(shares, SEQ)
    heads = to_each(join_shares(shares, chips), CHIPS)
    other_heads = across(heads)
    partial, rest = project_first(heads, out_weight)
    partial = project_second(other_heads, rest, partial, lax.axis_size("head"))
    partial, other_weight = lax.optimization_barrier((partial, other_weight))
    partial = to_each(partial, "head")
    stream = make_stream(partial, residual.reshape(rows, -1), norm_gain, chips)
    mine = to_each(stream, CHIPS)
    sent = sent_product(mine, shares, other_weight)
    received = across(sent)
    kept = kept_product(mine, own_weight)
    copies = lax.axis_size(SEQ_HEAD)
    logits, stats = logit_statistics(kept, sent, received, draft_tokens, copies)
    stats = to_each(stats.reshape(copies, 2, 128), SEQ_HEAD).reshape(copies * 2, 128)
    path_logits, logprob = final_join(path, stats, logits)
    return (jnp.transpose(path_logits, (1, 0, 2)), logprob)


def solution(mesh):
    torus = Mesh(
        mesh.devices.reshape(4, 4, 2, mesh.shape["head"]), ("seq_0", "seq_1", "seq_2", "head")
    )
    in_specs = (
        P(None, "head", None, None),
        P(None, "head", SEQ, None),
        P(None, "head", SEQ, None),
        P(None, "head", None, None),
        P(None, "head", None, None),
        P(),
        P(),
        P(),
        P(),
        P(None, None, SEQ),
        P("head", SEQ),
        P(SEQ),
        P(None, SEQ_HEAD),
    )
    out_specs = (P(None, None, SEQ_HEAD), P())
    return jax.shard_map(
        on_device, mesh=torus, in_specs=in_specs, out_specs=out_specs, check_vma=False
    )
```

```python
import functools

import jax
import jax.numpy as jnp
from jax import lax
from jax.experimental import pallas as pl
from jax.experimental.pallas import tpu as pltpu
from jax.sharding import Mesh
from jax.sharding import PartitionSpec as P

D = 8192
SEQ = ("seq_0", "seq_1", "seq_2")
CHIPS = ("seq_1", "seq_0")
SEQ_HEAD = ("seq_0", "seq_1", "seq_2", "head")

HIDDEN = -1e30
FLOOR = -1e25
EPSILON = 1e-5
LOG2E = 1.4426950408889634
ROWS = 256

f32 = jnp.float32
bf16 = jnp.bfloat16


def rows_dot(a, b):
    return lax.dot_general(a, b, (((1,), (1,)), ((), ())), preferred_element_type=f32)


def place_of(chip, side=4):
    return chip % side * side + chip // side


def plain_dot(a, b):
    return lax.dot_general(a, b, (((1,), (0,)), ((), ())), preferred_element_type=f32)


def room(mib):
    return pltpu.CompilerParams(vmem_limit_bytes=mib << 20)


def rows_dot(a, b):
    return lax.dot_general(a, b, (((1,), (1,)), ((), ())), preferred_element_type=f32)


def place_of(chip, side=4):
    return chip % side * side + chip // side


def plain_dot(a, b):
    return lax.dot_general(a, b, (((1,), (0,)), ((), ())), preferred_element_type=f32)


def room(mib):
    return pltpu.CompilerParams(vmem_limit_bytes=mib << 20)


def high_low(x):
    high = x.astype(bf16)
    return high, (x - high.astype(f32)).astype(bf16)


def tree_bias(parents):
    nodes = parents.shape[1]
    column = lax.broadcasted_iota(jnp.int32, (nodes, nodes), 1)
    row = lax.broadcasted_iota(jnp.int32, (nodes, nodes), 0)
    eye = row == column
    linked = jnp.where(jnp.logical_or(parents == row, eye), 1.0, 0.0).astype(bf16)
    reached = rows_dot(jnp.where(eye, 1.0, 0.0).astype(bf16), linked).astype(bf16)
    for _ in range((nodes - 1).bit_length()):
        reached = jnp.minimum(plain_dot(reached, reached), 1.0).astype(bf16)
    return jnp.where(reached.astype(f32) > 0.5, 0.0, HIDDEN)


def attention_kernel(
    lengths_hbm,
    parents_hbm,
    q_hbm,
    k_hbm,
    v_hbm,
    nk_hbm,
    nv_hbm,
    gain_hbm,
    out_ref,
    lengths_ref,
    parents_ref,
    q_ref,
    k_ref,
    v_ref,
    nk_ref,
    nv_ref,
    gain_ref,
    block_sems,
    tree_sems,
    small_sems,
):
    batch, heads, nodes, width = q_ref.shape
    kv, span = k_ref.shape[1:3]
    scale = width**-0.5
    step = scale * LOG2E
    seq = lax.axis_index(SEQ)
    owner = seq == lax.axis_size(SEQ) - 1
    other = jnp.logical_not(owner)
    group = ROWS // nodes
    turns = range(heads // group)
    of_group = heads // group // kv
    ones = jnp.ones((span, width), bf16)

    lengths_copy = pltpu.make_async_copy(lengths_hbm, lengths_ref, small_sems.at[0])
    lengths_copy.start()
    gain_copy = pltpu.make_async_copy(gain_hbm, gain_ref, small_sems.at[1])
    gain_copy.start()

    def block_copy(b, g, n):
        own = pl.ds(g * (heads // kv), heads // kv)
        source, target, place = (
            (q_hbm, q_ref, (b, own)),
            (k_hbm, k_ref, (b, g)),
            (v_hbm, v_ref, (b, g)),
        )[n]
        return pltpu.make_async_copy(source.at[place], target.at[place], block_sems.at[b, g, n])

    for b in range(batch):
        for g in range(kv):
            for n in range(3):
                block_copy(b, g, n).start()
    trees = [
        pltpu.make_async_copy(source, target, tree_sems.at[n])
        for n, (source, target) in enumerate(
            ((parents_hbm, parents_ref), (nk_hbm, nk_ref), (nv_hbm, nv_ref))
        )
    ]

    @pl.when(owner)
    def _():
        for copy in trees:
            copy.start()
        for copy in trees:
            copy.wait()

    lengths_copy.wait()
    gain_copy.wait()
    gain = gain_ref[...].astype(f32)[None]
    gains = gain[:, :width], gain[:, width:]
    row = lax.broadcasted_iota(jnp.int32, (8, width), 0)

    def write(b, part, out, top, total):
        at = b * heads + part * group
        out_ref[pl.ds(at, group), :nodes] = out.astype(bf16).reshape(group, nodes, width)
        lane = lax.broadcasted_iota(jnp.int32, (ROWS, width), 1)
        turned = jnp.transpose(jnp.where(lane == 0, top, total))[:8]
        for h in range(group):
            section = turned[:, h * nodes : (h + 1) * nodes]
            total = section[1:2]
            high = total.astype(bf16).astype(f32)
            lines = jnp.where(row[:, :nodes] == 1, high, total - high)
            lines = jnp.where(row[:, :nodes] == 0, section[0:1], lines)
            tail = jnp.concatenate([lines, jnp.zeros((8, width - nodes), f32)], axis=1)
            for n in range(2):
                tail = jnp.where(row == 3 + n, gains[n], tail)
            out_ref[at + h, nodes:] = tail.astype(bf16)

    def sweep(b, live, with_cache, with_tree):
        biases = []
        if with_cache:
            dead = lax.broadcasted_iota(jnp.int32, (1, span), 1) >= live
            biases.append(jnp.where(dead, HIDDEN, 0.0))
        if with_tree:
            bias = tree_bias(parents_ref[pl.ds(b, 1)])
            biases.append(jnp.concatenate([bias] * group, axis=0))

        def products(part):
            g = part // of_group
            rows = q_ref[b, part * group : (part + 1) * group].reshape(ROWS, width)
            found = [rows_dot(rows, k_ref[b, g])] if with_cache else []
            return found + ([rows_dot(rows, nk_ref[b, g])] if with_tree else [])

        ahead = products(0)
        for part in turns:
            g = part // of_group
            scores = [s + bias for s, bias in zip(ahead, biases)]
            if part + 1 < len(turns):
                ahead = products(part + 1)
            if part % of_group == 0:
                values = [jnp.concatenate([v_ref[b, g], ones], axis=1)] if with_cache else []
                if with_tree:
                    values.append(jnp.concatenate([nv_ref[b, g], ones[:nodes]], axis=1))
            highest = functools.reduce(
                jnp.maximum, [jnp.max(s, axis=1, keepdims=True) for s in scores]
            )
            top = jnp.maximum((highest * scale).astype(bf16).astype(f32), FLOOR)
            shift = top * LOG2E
            result = 0.0
            for s, value in zip(scores, values):
                weights = jnp.exp2(s * step - shift).astype(bf16)
                result = result + plain_dot(weights, value)
            write(b, part, result[:, :width], top, result[:, width:])

    def nothing(b):
        for part in turns:
            zeros = jnp.zeros((ROWS, width), f32)
            write(b, part, zeros, jnp.full((ROWS, 1), FLOOR), zeros)

    @pl.loop(0, batch)
    def _(b):
        live = lengths_ref[b] - seq * span
        for g in range(kv):
            for n in range(3):
                block_copy(b, g, n).wait()
        filled = live > 0
        empty = jnp.logical_not(filled)
        pl.when(jnp.logical_and(filled, other))(functools.partial(sweep, b, live, True, False))
        pl.when(jnp.logical_and(filled, owner))(functools.partial(sweep, b, live, True, True))
        pl.when(jnp.logical_and(empty, owner))(functools.partial(sweep, b, live, False, True))
        pl.when(jnp.logical_and(empty, other))(functools.partial(nothing, b))


def local_attention(
    queries, cache_keys, cache_values, new_keys, new_values, parents, lengths, gain
):
    batch, heads, nodes, width = queries.shape
    kv = cache_keys.shape[1]
    operands = (lengths, parents, queries, cache_keys, cache_values, new_keys, new_values, gain)
    scratch = [pltpu.SMEM(lengths.shape, lengths.dtype)]
    scratch += [pltpu.VMEM(x.shape, x.dtype) for x in operands[1:]]
    scratch += [
        pltpu.SemaphoreType.DMA((batch, kv, 3)),
        pltpu.SemaphoreType.DMA((3,)),
        pltpu.SemaphoreType.DMA((2,)),
    ]
    return pl.pallas_call(
        attention_kernel,
        in_specs=[pl.BlockSpec(memory_space=pltpu.HBM)] * len(operands),
        out_specs=pl.BlockSpec(memory_space=pltpu.VMEM),
        out_shape=jax.ShapeDtypeStruct((batch * heads, nodes + 8, width), bf16),
        scratch_shapes=scratch,
        compiler_params=room(62),
        name="attend",
    )(*operands)


def join_kernel(parts_ref, out_ref):
    count, rows, width = parts_ref.shape
    nodes = rows - 8
    tops = parts_ref[:, nodes, :].astype(f32)
    totals = parts_ref[:, nodes + 1, :].astype(f32) + parts_ref[:, nodes + 2, :].astype(f32)
    used = lax.broadcasted_iota(jnp.int32, (count, width), 1) < nodes
    tops = jnp.where(used, tops, 0.0)
    totals = jnp.where(used, totals, 1.0)
    factors = jnp.exp(tops - jnp.max(tops, axis=0, keepdims=True))
    share = factors / jnp.sum(factors * totals, axis=0, keepdims=True)
    square = jnp.concatenate([share, jnp.zeros((width - count, width), f32)], axis=0)
    turned = jnp.transpose(square)[:nodes]
    total = parts_ref[0, :nodes].astype(f32) * turned[:, 0:1]
    for k in range(1, count):
        total = total + parts_ref[k, :nodes].astype(f32) * turned[:, k : k + 1]
    block = total.astype(bf16)
    for k in range(out_ref.shape[0]):
        out_ref[k] = block


def join_shares(parts, copies):
    rows, width = parts.shape[1:]
    return pl.pallas_call(
        join_kernel,
        out_shape=jax.ShapeDtypeStruct((copies, rows - 8, width), bf16),
        compiler_params=room(8),
        name="join",
    )(parts)


def head_lines(blocks_ref):
    half = blocks_ref.shape[0] // 2
    lines = [
        jnp.concatenate([blocks_ref[place_of(b * half + k)] for k in range(half)], axis=1)
        for b in range(2)
    ]
    return jnp.concatenate(lines, axis=0)


def project_first_kernel(blocks_ref, weight_ref, out_ref, rest_ref):
    chips, nodes, width = blocks_ref.shape
    core = lax.axis_index("seq_2")
    sections = []
    for k in range(chips // 2):
        own = pl.multiple_of((2 * k + core) * width, width)
        other = pl.multiple_of((2 * k + 1 - core) * width, width)
        sections.append(weight_ref[pl.ds(own, width)])
        rest_ref[k * width : (k + 1) * width] = weight_ref[pl.ds(other, width)]
    out_ref[...] = plain_dot(head_lines(blocks_ref), jnp.concatenate(sections, axis=0))


def project_second_kernel(blocks_ref, weight_ref, first_ref, out_ref):
    result = first_ref[...] + plain_dot(head_lines(blocks_ref), weight_ref[...])
    result = result.astype(bf16)
    for k in range(out_ref.shape[0]):
        out_ref[k] = result


def project_first(blocks, weight):
    rows = 2 * blocks.shape[1]
    depth, columns = weight.shape
    return pl.pallas_call(
        project_first_kernel,
        out_shape=[
            jax.ShapeDtypeStruct((rows, columns), f32),
            jax.ShapeDtypeStruct((depth // 2, columns), weight.dtype),
        ],
        cost_estimate=pl.CostEstimate(
            flops=rows * weight.size, bytes_accessed=3 * weight.size, transcendentals=0
        ),
        compiler_params=room(8),
        name="project_first",
    )(blocks, weight)


def project_second(blocks, weight, first, copies):
    return pl.pallas_call(
        project_second_kernel,
        out_shape=jax.ShapeDtypeStruct((copies, *first.shape), bf16),
        compiler_params=room(8),
        name="project_second",
    )(blocks, weight, first)


def stream_kernel(parts_ref, residual_ref, gain_ref, out_ref):
    stream = residual_ref[...].astype(f32)
    for k in range(parts_ref.shape[0]):
        stream = stream + parts_ref[k].astype(f32)
    scaled = (stream * gain_ref[...].astype(f32)[None]).astype(bf16)
    for k in range(out_ref.shape[0]):
        out_ref[k] = scaled


def make_stream(parts, residual, gain, copies):
    rows, columns = residual.shape
    return pl.pallas_call(
        stream_kernel,
        out_shape=jax.ShapeDtypeStruct((copies, rows, columns), bf16),
        compiler_params=room(8),
        name="stream",
    )(parts, residual, gain)


def gathered_product(blocks_ref, weight_ref):
    chips, rows, columns = blocks_ref.shape
    core = lax.axis_index("seq_2")
    blocks, sections = [], []
    for k in range(chips):
        start = pl.multiple_of((2 * place_of(k) + core) * columns, columns)
        blocks.append(blocks_ref[k])
        sections.append(weight_ref[pl.ds(start, columns)])
    return plain_dot(jnp.concatenate(blocks, axis=1), jnp.concatenate(sections, axis=0))


def sent_kernel(blocks_ref, shares_ref, weight_ref, out_ref):
    chips = blocks_ref.shape[0]
    width = weight_ref.shape[1]
    nodes = shares_ref.shape[1] - 8
    core = lax.axis_index("seq_2")
    squares = 0.0
    for k in range(chips):
        gains = shares_ref[2 * place_of(k) + core, nodes:].astype(f32)
        for n in range(2):
            inverse = 1.0 / gains[3 + n : 4 + n]
            plain = blocks_ref[k, :, n * 128 : (n + 1) * 128].astype(f32) * inverse
            squares = squares + plain * plain
    out_ref[:, :width] = gathered_product(blocks_ref, weight_ref)
    out_ref[:, width:] = squares


def kept_kernel(blocks_ref, weight_ref, out_ref):
    out_ref[...] = gathered_product(blocks_ref, weight_ref)


def product_cost(blocks, weight):
    chips, rows, columns = blocks.shape
    return pl.CostEstimate(
        flops=2 * blocks.size * weight.shape[1],
        bytes_accessed=2 * chips * columns * (rows + weight.shape[1]),
        transcendentals=0,
    )


def sent_product(blocks, shares, weight):
    return pl.pallas_call(
        sent_kernel,
        out_shape=jax.ShapeDtypeStruct((blocks.shape[1], weight.shape[1] + 128), f32),
        cost_estimate=product_cost(blocks, weight),
        compiler_params=room(16),
        name="logits_sent",
    )(blocks, shares, weight)


def kept_product(blocks, weight):
    return pl.pallas_call(
        kept_kernel,
        out_shape=jax.ShapeDtypeStruct((blocks.shape[1], weight.shape[1]), f32),
        cost_estimate=product_cost(blocks, weight),
        compiler_params=room(16),
        name="logits_kept",
    )(blocks, weight)


def statistics_kernel(kept_ref, sent_ref, received_ref, tokens_ref, logits_ref, stats_ref):
    rows, width = kept_ref.shape
    squares = sent_ref[:, width:] + received_ref[:, width:]
    total = jnp.sum(squares, axis=1, keepdims=True)
    logits = (kept_ref[...] + received_ref[:, :width]) * lax.rsqrt(total / D + EPSILON)
    logits_ref[...] = logits
    top = jnp.max(logits, axis=1, keepdims=True)
    sums = jnp.sum(jnp.exp(logits - top), axis=1, keepdims=True)
    ids = lax.broadcasted_iota(jnp.int32, (rows, width), 1) + lax.axis_index(SEQ_HEAD) * width
    lines = [tokens_ref[b : b + 1].astype(f32) for b in range(tokens_ref.shape[0])]
    line = jnp.broadcast_to(jnp.concatenate(lines, axis=1), (128, rows))
    tokens = jnp.transpose(line)[:, 0:1].astype(jnp.int32)
    hit = jnp.sum(jnp.where(ids == tokens, logits, 0.0), axis=1, keepdims=True)
    lane = lax.broadcasted_iota(jnp.int32, (rows, 128), 1)
    turned = jnp.transpose(jnp.where(lane % 2 == 0, top + jnp.log(sums), hit))[:8]
    for k in range(stats_ref.shape[0] // 8):
        stats_ref[k * 8 : k * 8 + 8] = turned


def logit_statistics(kept, sent, received, tokens, copies):
    return pl.pallas_call(
        statistics_kernel,
        out_shape=[
            jax.ShapeDtypeStruct(kept.shape, f32),
            jax.ShapeDtypeStruct((copies * 2, 128), f32),
        ],
        compiler_params=room(8),
        name="logits_statistics",
    )(kept, sent, received, tokens)


def final_kernel(path_ref, stats_ref, logits_ref, picked_ref, out_ref):
    batch, nodes = out_ref.shape
    for b in range(batch):
        for k in range(path_ref.shape[1]):
            picked_ref[k, b : b + 1] = logits_ref[pl.ds(path_ref[b, k] + b * nodes, 1)]
    stats = stats_ref[...]
    is_sum = lax.broadcasted_iota(jnp.int32, stats.shape, 0) % 2 == 0
    sums = jnp.where(is_sum, stats, HIDDEN)
    top = jnp.max(sums, axis=0, keepdims=True)
    total = top + jnp.log(jnp.sum(jnp.exp(sums - top), axis=0, keepdims=True))
    result = jnp.sum(jnp.where(is_sum, 0.0, stats), axis=0, keepdims=True) - total
    for b in range(batch):
        out_ref[b : b + 1] = result[:, b * nodes : (b + 1) * nodes]


def final_join(path, stats, logits):
    batch = path.shape[0]
    rows, width = logits.shape
    return pl.pallas_call(
        final_kernel,
        in_specs=[
            pl.BlockSpec(memory_space=pltpu.SMEM),
            pl.BlockSpec(memory_space=pltpu.VMEM),
            pl.BlockSpec(memory_space=pltpu.VMEM),
        ],
        out_shape=[
            jax.ShapeDtypeStruct((*path.shape[::-1], width), f32),
            jax.ShapeDtypeStruct((batch, rows // batch), f32),
        ],
        compiler_params=room(4),
        name="final",
    )(path, stats, logits)


def to_each(x, axes):
    return lax.all_to_all(x, axes, 0, 0, tiled=True)


def across(x):
    return lax.ppermute(x, "seq_2", [(0, 1), (1, 0)])


def on_device(
    queries,
    cache_keys,
    cache_values,
    new_keys,
    new_values,
    parents,
    path,
    lengths,
    draft_tokens,
    residual,
    out_weight,
    norm_gain,
    vocab_weight,
):
    rows = parents.size
    chips = lax.axis_size(CHIPS)
    shares = local_attention(
        queries, cache_keys, cache_values, new_keys, new_values, parents, lengths, norm_gain
    )
    shares = to_each(shares, SEQ)
    heads = to_each(join_shares(shares, chips), CHIPS)
    other_heads = across(heads)
    partial, rest = project_first(heads, out_weight)
    partial = project_second(other_heads, rest, partial, lax.axis_size("head"))
    partial, own_weight = lax.optimization_barrier((partial, vocab_weight))
    other_weight = across(own_weight)
    partial = to_each(partial, "head")
    stream = make_stream(partial, residual.reshape(rows, -1), norm_gain, chips)
    mine = to_each(stream, CHIPS)
    sent = sent_product(mine, shares, other_weight)
    received = across(sent)
    kept = kept_product(mine, own_weight)
    copies = lax.axis_size(SEQ_HEAD)
    logits, stats = logit_statistics(kept, sent, received, draft_tokens, copies)
    stats = to_each(stats.reshape(copies, 2, 128), SEQ_HEAD).reshape(copies * 2, 128)
    path_logits, logprob = final_join(path, stats, logits)
    return (jnp.transpose(path_logits, (1, 0, 2)), logprob)


def solution(mesh):
    torus = Mesh(
        mesh.devices.reshape(4, 4, 2, mesh.shape["head"]), ("seq_0", "seq_1", "seq_2", "head")
    )
    in_specs = (
        P(None, "head", None, None),
        P(None, "head", SEQ, None),
        P(None, "head", SEQ, None),
        P(None, "head", None, None),
        P(None, "head", None, None),
        P(),
        P(),
        P(),
        P(),
        P(None, None, SEQ),
        P("head", SEQ),
        P(SEQ),
        P(None, SEQ_HEAD),
    )
    out_specs = (P(None, None, SEQ_HEAD), P())
    return jax.shard_map(
        on_device, mesh=torus, in_specs=in_specs, out_specs=out_specs, check_vma=False
    )
```

```python
import functools

import jax
import jax.numpy as jnp
from jax import lax
from jax.experimental import pallas as pl
from jax.experimental.pallas import tpu as pltpu
from jax.sharding import Mesh
from jax.sharding import PartitionSpec as P

D = 8192
SEQ = ("seq_0", "seq_1", "seq_2")
CHIPS = ("seq_1", "seq_0")
SEQ_HEAD = ("seq_0", "seq_1", "seq_2", "head")

HIDDEN = -1e30
FLOOR = -1e25
EPSILON = 1e-5
LOG2E = 1.4426950408889634
ROWS = 256

f32 = jnp.float32
bf16 = jnp.bfloat16


def rows_dot(a, b):
    return lax.dot_general(a, b, (((1,), (1,)), ((), ())), preferred_element_type=f32)


def place_of(chip, side=4):
    return chip % side * side + chip // side


def plain_dot(a, b):
    return lax.dot_general(a, b, (((1,), (0,)), ((), ())), preferred_element_type=f32)


def room(mib):
    return pltpu.CompilerParams(vmem_limit_bytes=mib << 20)


def rows_dot(a, b):
    return lax.dot_general(a, b, (((1,), (1,)), ((), ())), preferred_element_type=f32)


def place_of(chip, side=4):
    return chip % side * side + chip // side


def plain_dot(a, b):
    return lax.dot_general(a, b, (((1,), (0,)), ((), ())), preferred_element_type=f32)


def room(mib):
    return pltpu.CompilerParams(vmem_limit_bytes=mib << 20)


def high_low(x):
    high = x.astype(bf16)
    return high, (x - high.astype(f32)).astype(bf16)


def tree_bias(parents):
    nodes = parents.shape[1]
    column = lax.broadcasted_iota(jnp.int32, (nodes, nodes), 1)
    row = lax.broadcasted_iota(jnp.int32, (nodes, nodes), 0)
    eye = row == column
    linked = jnp.where(jnp.logical_or(parents == row, eye), 1.0, 0.0).astype(bf16)
    reached = rows_dot(jnp.where(eye, 1.0, 0.0).astype(bf16), linked).astype(bf16)
    for _ in range((nodes - 1).bit_length()):
        reached = jnp.minimum(plain_dot(reached, reached), 1.0).astype(bf16)
    return jnp.where(reached.astype(f32) > 0.5, 0.0, HIDDEN)


def attention_kernel(
    lengths_hbm,
    parents_hbm,
    q_hbm,
    k_hbm,
    v_hbm,
    nk_hbm,
    nv_hbm,
    gain_hbm,
    out_ref,
    lengths_ref,
    parents_ref,
    q_ref,
    k_ref,
    v_ref,
    nk_ref,
    nv_ref,
    gain_ref,
    block_sems,
    tree_sems,
    small_sems,
):
    batch, heads, nodes, width = q_ref.shape
    kv, span = k_ref.shape[1:3]
    scale = width**-0.5
    step = scale * LOG2E
    seq = lax.axis_index(SEQ)
    owner = seq == lax.axis_size(SEQ) - 1
    other = jnp.logical_not(owner)
    group = ROWS // nodes
    turns = range(heads // group)
    of_group = heads // group // kv
    ones = jnp.ones((span, width), bf16)

    lengths_copy = pltpu.make_async_copy(lengths_hbm, lengths_ref, small_sems.at[0])
    lengths_copy.start()
    gain_copy = pltpu.make_async_copy(gain_hbm, gain_ref, small_sems.at[1])
    gain_copy.start()

    def block_copy(b, g, n):
        own = pl.ds(g * (heads // kv), heads // kv)
        source, target, place = (
            (q_hbm, q_ref, (b, own)),
            (k_hbm, k_ref, (b, g)),
            (v_hbm, v_ref, (b, g)),
        )[n]
        return pltpu.make_async_copy(source.at[place], target.at[place], block_sems.at[b, g, n])

    for b in range(batch):
        for g in range(kv):
            for n in range(3):
                block_copy(b, g, n).start()
    trees = [
        pltpu.make_async_copy(source, target, tree_sems.at[n])
        for n, (source, target) in enumerate(
            ((parents_hbm, parents_ref), (nk_hbm, nk_ref), (nv_hbm, nv_ref))
        )
    ]

    @pl.when(owner)
    def _():
        for copy in trees:
            copy.start()
        for copy in trees:
            copy.wait()

    lengths_copy.wait()
    gain_copy.wait()
    gain = gain_ref[...].astype(f32)[None]
    gains = gain[:, :width], gain[:, width:]
    row = lax.broadcasted_iota(jnp.int32, (8, width), 0)

    def write(b, part, out, top, total):
        at = b * heads + part * group
        out_ref[pl.ds(at, group), :nodes] = out.astype(bf16).reshape(group, nodes, width)
        lane = lax.broadcasted_iota(jnp.int32, (ROWS, width), 1)
        turned = jnp.transpose(jnp.where(lane == 0, top, total))[:8]
        for h in range(group):
            section = turned[:, h * nodes : (h + 1) * nodes]
            total = section[1:2]
            high = total.astype(bf16).astype(f32)
            lines = jnp.where(row[:, :nodes] == 1, high, total - high)
            lines = jnp.where(row[:, :nodes] == 0, section[0:1], lines)
            tail = jnp.concatenate([lines, jnp.zeros((8, width - nodes), f32)], axis=1)
            for n in range(2):
                tail = jnp.where(row == 3 + n, gains[n], tail)
            out_ref[at + h, nodes:] = tail.astype(bf16)

    def sweep(b, live, with_cache, with_tree):
        biases = []
        if with_cache:
            dead = lax.broadcasted_iota(jnp.int32, (1, span), 1) >= live
            biases.append(jnp.where(dead, HIDDEN, 0.0))
        if with_tree:
            bias = tree_bias(parents_ref[pl.ds(b, 1)])
            biases.append(jnp.concatenate([bias] * group, axis=0))

        def products(part):
            g = part // of_group
            rows = q_ref[b, part * group : (part + 1) * group].reshape(ROWS, width)
            found = [rows_dot(rows, k_ref[b, g])] if with_cache else []
            return found + ([rows_dot(rows, nk_ref[b, g])] if with_tree else [])

        ahead = products(0)
        for part in turns:
            g = part // of_group
            scores = [s + bias for s, bias in zip(ahead, biases)]
            if part + 1 < len(turns):
                ahead = products(part + 1)
            if part % of_group == 0:
                values = [jnp.concatenate([v_ref[b, g], ones], axis=1)] if with_cache else []
                if with_tree:
                    values.append(jnp.concatenate([nv_ref[b, g], ones[:nodes]], axis=1))
            highest = functools.reduce(
                jnp.maximum, [jnp.max(s, axis=1, keepdims=True) for s in scores]
            )
            top = jnp.maximum((highest * scale).astype(bf16).astype(f32), FLOOR)
            shift = top * LOG2E
            result = 0.0
            for s, value in zip(scores, values):
                weights = jnp.exp2(s * step - shift).astype(bf16)
                result = result + plain_dot(weights, value)
            write(b, part, result[:, :width], top, result[:, width:])

    def nothing(b):
        for part in turns:
            zeros = jnp.zeros((ROWS, width), f32)
            write(b, part, zeros, jnp.full((ROWS, 1), FLOOR), zeros)

    @pl.loop(0, batch)
    def _(b):
        live = lengths_ref[b] - seq * span
        for g in range(kv):
            for n in range(3):
                block_copy(b, g, n).wait()
        filled = live > 0
        empty = jnp.logical_not(filled)
        pl.when(jnp.logical_and(filled, other))(functools.partial(sweep, b, live, True, False))
        pl.when(jnp.logical_and(filled, owner))(functools.partial(sweep, b, live, True, True))
        pl.when(jnp.logical_and(empty, owner))(functools.partial(sweep, b, live, False, True))
        pl.when(jnp.logical_and(empty, other))(functools.partial(nothing, b))


def local_attention(
    queries, cache_keys, cache_values, new_keys, new_values, parents, lengths, gain
):
    batch, heads, nodes, width = queries.shape
    kv = cache_keys.shape[1]
    operands = (lengths, parents, queries, cache_keys, cache_values, new_keys, new_values, gain)
    scratch = [pltpu.SMEM(lengths.shape, lengths.dtype)]
    scratch += [pltpu.VMEM(x.shape, x.dtype) for x in operands[1:]]
    scratch += [
        pltpu.SemaphoreType.DMA((batch, kv, 3)),
        pltpu.SemaphoreType.DMA((3,)),
        pltpu.SemaphoreType.DMA((2,)),
    ]
    return pl.pallas_call(
        attention_kernel,
        in_specs=[pl.BlockSpec(memory_space=pltpu.HBM)] * len(operands),
        out_specs=pl.BlockSpec(memory_space=pltpu.VMEM),
        out_shape=jax.ShapeDtypeStruct((batch * heads, nodes + 8, width), bf16),
        scratch_shapes=scratch,
        compiler_params=room(62),
        name="attend",
    )(*operands)


def join_kernel(parts_ref, out_ref):
    count, rows, width = parts_ref.shape
    nodes = rows - 8
    tops = parts_ref[:, nodes, :].astype(f32)
    totals = parts_ref[:, nodes + 1, :].astype(f32) + parts_ref[:, nodes + 2, :].astype(f32)
    used = lax.broadcasted_iota(jnp.int32, (count, width), 1) < nodes
    tops = jnp.where(used, tops, 0.0)
    totals = jnp.where(used, totals, 1.0)
    factors = jnp.exp(tops - jnp.max(tops, axis=0, keepdims=True))
    share = factors / jnp.sum(factors * totals, axis=0, keepdims=True)
    square = jnp.concatenate([share, jnp.zeros((width - count, width), f32)], axis=0)
    turned = jnp.transpose(square)[:nodes]
    total = parts_ref[0, :nodes].astype(f32) * turned[:, 0:1]
    for k in range(1, count):
        total = total + parts_ref[k, :nodes].astype(f32) * turned[:, k : k + 1]
    block = total.astype(bf16)
    for k in range(out_ref.shape[0]):
        out_ref[k] = block


def join_shares(parts, copies):
    rows, width = parts.shape[1:]
    return pl.pallas_call(
        join_kernel,
        out_shape=jax.ShapeDtypeStruct((copies, rows - 8, width), bf16),
        compiler_params=room(8),
        name="join",
    )(parts)


def head_lines(blocks_ref):
    half = blocks_ref.shape[0] // 2
    lines = [
        jnp.concatenate([blocks_ref[place_of(b * half + k)] for k in range(half)], axis=1)
        for b in range(2)
    ]
    return jnp.concatenate(lines, axis=0)


def project_first_kernel(blocks_ref, weight_ref, out_ref, rest_ref):
    chips, nodes, width = blocks_ref.shape
    core = lax.axis_index("seq_2")
    sections = []
    for k in range(chips // 2):
        own = pl.multiple_of((2 * k + core) * width, width)
        other = pl.multiple_of((2 * k + 1 - core) * width, width)
        sections.append(weight_ref[pl.ds(own, width)])
        rest_ref[k * width : (k + 1) * width] = weight_ref[pl.ds(other, width)]
    out_ref[...] = plain_dot(head_lines(blocks_ref), jnp.concatenate(sections, axis=0))


def project_second_kernel(blocks_ref, weight_ref, first_ref, out_ref):
    result = first_ref[...] + plain_dot(head_lines(blocks_ref), weight_ref[...])
    result = result.astype(bf16)
    for k in range(out_ref.shape[0]):
        out_ref[k] = result


def project_first(blocks, weight):
    rows = 2 * blocks.shape[1]
    depth, columns = weight.shape
    return pl.pallas_call(
        project_first_kernel,
        out_shape=[
            jax.ShapeDtypeStruct((rows, columns), f32),
            jax.ShapeDtypeStruct((depth // 2, columns), weight.dtype),
        ],
        cost_estimate=pl.CostEstimate(
            flops=rows * weight.size, bytes_accessed=3 * weight.size, transcendentals=0
        ),
        compiler_params=room(8),
        name="project_first",
    )(blocks, weight)


def project_second(blocks, weight, first, copies):
    return pl.pallas_call(
        project_second_kernel,
        out_shape=jax.ShapeDtypeStruct((copies, *first.shape), bf16),
        compiler_params=room(8),
        name="project_second",
    )(blocks, weight, first)


def stream_kernel(parts_ref, residual_ref, gain_ref, out_ref):
    stream = residual_ref[...].astype(f32)
    for k in range(parts_ref.shape[0]):
        stream = stream + parts_ref[k].astype(f32)
    scaled = (stream * gain_ref[...].astype(f32)[None]).astype(bf16)
    for k in range(out_ref.shape[0]):
        out_ref[k] = scaled


def make_stream(parts, residual, gain, copies):
    rows, columns = residual.shape
    return pl.pallas_call(
        stream_kernel,
        out_shape=jax.ShapeDtypeStruct((copies, rows, columns), bf16),
        compiler_params=room(8),
        name="stream",
    )(parts, residual, gain)


def gathered_product(blocks_ref, weight_ref):
    chips, rows, columns = blocks_ref.shape
    core = lax.axis_index("seq_2")
    blocks, sections = [], []
    for k in range(chips):
        start = pl.multiple_of((2 * place_of(k) + core) * columns, columns)
        blocks.append(blocks_ref[k])
        sections.append(weight_ref[pl.ds(start, columns)])
    return plain_dot(jnp.concatenate(blocks, axis=1), jnp.concatenate(sections, axis=0))


def sent_kernel(blocks_ref, shares_ref, weight_ref, out_ref):
    chips = blocks_ref.shape[0]
    width = weight_ref.shape[1]
    nodes = shares_ref.shape[1] - 8
    core = lax.axis_index("seq_2")
    squares = 0.0
    for k in range(chips):
        gains = shares_ref[2 * place_of(k) + core, nodes:].astype(f32)
        for n in range(2):
            inverse = 1.0 / gains[3 + n : 4 + n]
            plain = blocks_ref[k, :, n * 128 : (n + 1) * 128].astype(f32) * inverse
            squares = squares + plain * plain
    out_ref[:, :width] = gathered_product(blocks_ref, weight_ref)
    out_ref[:, width:] = squares


def kept_kernel(blocks_ref, weight_ref, out_ref):
    out_ref[...] = gathered_product(blocks_ref, weight_ref)


def product_cost(blocks, weight):
    chips, rows, columns = blocks.shape
    return pl.CostEstimate(
        flops=2 * blocks.size * weight.shape[1],
        bytes_accessed=2 * chips * columns * (rows + weight.shape[1]),
        transcendentals=0,
    )


def sent_product(blocks, shares, weight):
    return pl.pallas_call(
        sent_kernel,
        out_shape=jax.ShapeDtypeStruct((blocks.shape[1], weight.shape[1] + 128), f32),
        cost_estimate=product_cost(blocks, weight),
        compiler_params=room(16),
        name="logits_sent",
    )(blocks, shares, weight)


def kept_product(blocks, weight):
    return pl.pallas_call(
        kept_kernel,
        out_shape=jax.ShapeDtypeStruct((blocks.shape[1], weight.shape[1]), f32),
        cost_estimate=product_cost(blocks, weight),
        compiler_params=room(16),
        name="logits_kept",
    )(blocks, weight)


def statistics_kernel(kept_ref, sent_ref, received_ref, tokens_ref, logits_ref, stats_ref):
    rows, width = kept_ref.shape
    squares = sent_ref[:, width:] + received_ref[:, width:]
    total = jnp.sum(squares, axis=1, keepdims=True)
    logits = (kept_ref[...] + received_ref[:, :width]) * lax.rsqrt(total / D + EPSILON)
    logits_ref[...] = logits
    top = jnp.max(logits, axis=1, keepdims=True)
    sums = jnp.sum(jnp.exp(logits - top), axis=1, keepdims=True)
    ids = lax.broadcasted_iota(jnp.int32, (rows, width), 1) + lax.axis_index(SEQ_HEAD) * width
    lines = [tokens_ref[b : b + 1].astype(f32) for b in range(tokens_ref.shape[0])]
    line = jnp.broadcast_to(jnp.concatenate(lines, axis=1), (128, rows))
    tokens = jnp.transpose(line)[:, 0:1].astype(jnp.int32)
    hit = jnp.sum(jnp.where(ids == tokens, logits, 0.0), axis=1, keepdims=True)
    lane = lax.broadcasted_iota(jnp.int32, (rows, 128), 1)
    turned = jnp.transpose(jnp.where(lane % 2 == 0, top + jnp.log(sums), hit))[:8]
    for k in range(stats_ref.shape[0] // 8):
        stats_ref[k * 8 : k * 8 + 8] = turned


def logit_statistics(kept, sent, received, tokens, copies):
    return pl.pallas_call(
        statistics_kernel,
        out_shape=[
            jax.ShapeDtypeStruct(kept.shape, f32),
            jax.ShapeDtypeStruct((copies * 2, 128), f32),
        ],
        compiler_params=room(8),
        name="logits_statistics",
    )(kept, sent, received, tokens)


def final_kernel(path_ref, stats_ref, logits_ref, picked_hbm, out_ref, picked_ref, sem):
    batch, nodes = out_ref.shape
    for b in range(batch):
        for k in range(path_ref.shape[1]):
            picked_ref[k, b : b + 1] = logits_ref[pl.ds(path_ref[b, k] + b * nodes, 1)]
    copy = pltpu.make_async_copy(picked_ref, picked_hbm, sem)
    copy.start()
    stats = stats_ref[...]
    is_sum = lax.broadcasted_iota(jnp.int32, stats.shape, 0) % 2 == 0
    sums = jnp.where(is_sum, stats, HIDDEN)
    top = jnp.max(sums, axis=0, keepdims=True)
    total = top + jnp.log(jnp.sum(jnp.exp(sums - top), axis=0, keepdims=True))
    result = jnp.sum(jnp.where(is_sum, 0.0, stats), axis=0, keepdims=True) - total
    for b in range(batch):
        out_ref[b : b + 1] = result[:, b * nodes : (b + 1) * nodes]
    copy.wait()


def final_join(path, stats, logits):
    batch = path.shape[0]
    rows, width = logits.shape
    return pl.pallas_call(
        final_kernel,
        in_specs=[
            pl.BlockSpec(memory_space=pltpu.SMEM),
            pl.BlockSpec(memory_space=pltpu.VMEM),
            pl.BlockSpec(memory_space=pltpu.VMEM),
        ],
        out_shape=[
            jax.ShapeDtypeStruct((*path.shape[::-1], width), f32),
            jax.ShapeDtypeStruct((batch, rows // batch), f32),
        ],
        out_specs=[
            pl.BlockSpec(memory_space=pltpu.HBM),
            pl.BlockSpec(memory_space=pltpu.VMEM),
        ],
        scratch_shapes=[
            pltpu.VMEM((*path.shape[::-1], width), f32),
            pltpu.SemaphoreType.DMA,
        ],
        compiler_params=room(4),
        name="final",
    )(path, stats, logits)


def to_each(x, axes):
    return lax.all_to_all(x, axes, 0, 0, tiled=True)


def across(x):
    return lax.ppermute(x, "seq_2", [(0, 1), (1, 0)])


def on_device(
    queries,
    cache_keys,
    cache_values,
    new_keys,
    new_values,
    parents,
    path,
    lengths,
    draft_tokens,
    residual,
    out_weight,
    norm_gain,
    vocab_weight,
):
    rows = parents.size
    chips = lax.axis_size(CHIPS)
    shares = local_attention(
        queries, cache_keys, cache_values, new_keys, new_values, parents, lengths, norm_gain
    )
    shares = to_each(shares, SEQ)
    heads = to_each(join_shares(shares, chips), CHIPS)
    other_heads = across(heads)
    partial, rest = project_first(heads, out_weight)
    partial = project_second(other_heads, rest, partial, lax.axis_size("head"))
    partial, own_weight = lax.optimization_barrier((partial, vocab_weight))
    other_weight = across(own_weight)
    partial = to_each(partial, "head")
    stream = make_stream(partial, residual.reshape(rows, -1), norm_gain, chips)
    mine = to_each(stream, CHIPS)
    sent = sent_product(mine, shares, other_weight)
    received = across(sent)
    kept = kept_product(mine, own_weight)
    copies = lax.axis_size(SEQ_HEAD)
    logits, stats = logit_statistics(kept, sent, received, draft_tokens, copies)
    stats = to_each(stats.reshape(copies, 2, 128), SEQ_HEAD).reshape(copies * 2, 128)
    path_logits, logprob = final_join(path, stats, logits)
    return (jnp.transpose(path_logits, (1, 0, 2)), logprob)


def solution(mesh):
    torus = Mesh(
        mesh.devices.reshape(4, 4, 2, mesh.shape["head"]), ("seq_0", "seq_1", "seq_2", "head")
    )
    in_specs = (
        P(None, "head", None, None),
        P(None, "head", SEQ, None),
        P(None, "head", SEQ, None),
        P(None, "head", None, None),
        P(None, "head", None, None),
        P(),
        P(),
        P(),
        P(),
        P(None, None, SEQ),
        P("head", SEQ),
        P(SEQ),
        P(None, SEQ_HEAD),
    )
    out_specs = (P(None, None, SEQ_HEAD), P())
    return jax.shard_map(
        on_device, mesh=torus, in_specs=in_specs, out_specs=out_specs, check_vma=False
    )
```

```python
import functools

import jax
import jax.numpy as jnp
from jax import lax
from jax.experimental import pallas as pl
from jax.experimental.pallas import tpu as pltpu
from jax.sharding import Mesh
from jax.sharding import PartitionSpec as P

D = 8192
SEQ = ("seq_0", "seq_1", "seq_2")
CHIPS = ("seq_1", "seq_0")
SEQ_HEAD = ("seq_0", "seq_1", "seq_2", "head")

HIDDEN = -1e30
FLOOR = -1e25
EPSILON = 1e-5
LOG2E = 1.4426950408889634
ROWS = 128

f32 = jnp.float32
bf16 = jnp.bfloat16


def rows_dot(a, b):
    return lax.dot_general(a, b, (((1,), (1,)), ((), ())), preferred_element_type=f32)


def place_of(chip, side=4):
    return chip % side * side + chip // side


def plain_dot(a, b):
    return lax.dot_general(a, b, (((1,), (0,)), ((), ())), preferred_element_type=f32)


def room(mib):
    return pltpu.CompilerParams(vmem_limit_bytes=mib << 20)


def rows_dot(a, b):
    return lax.dot_general(a, b, (((1,), (1,)), ((), ())), preferred_element_type=f32)


def place_of(chip, side=4):
    return chip % side * side + chip // side


def plain_dot(a, b):
    return lax.dot_general(a, b, (((1,), (0,)), ((), ())), preferred_element_type=f32)


def room(mib):
    return pltpu.CompilerParams(vmem_limit_bytes=mib << 20)


def high_low(x):
    high = x.astype(bf16)
    return high, (x - high.astype(f32)).astype(bf16)


def tree_bias(parents):
    nodes = parents.shape[1]
    column = lax.broadcasted_iota(jnp.int32, (nodes, nodes), 1)
    row = lax.broadcasted_iota(jnp.int32, (nodes, nodes), 0)
    eye = row == column
    linked = jnp.where(jnp.logical_or(parents == row, eye), 1.0, 0.0).astype(bf16)
    reached = rows_dot(jnp.where(eye, 1.0, 0.0).astype(bf16), linked).astype(bf16)
    for _ in range((nodes - 1).bit_length()):
        reached = jnp.minimum(plain_dot(reached, reached), 1.0).astype(bf16)
    return jnp.where(reached.astype(f32) > 0.5, 0.0, HIDDEN)


def attention_kernel(
    lengths_hbm,
    parents_hbm,
    q_hbm,
    k_hbm,
    v_hbm,
    nk_hbm,
    nv_hbm,
    gain_hbm,
    out_ref,
    lengths_ref,
    parents_ref,
    q_ref,
    k_ref,
    v_ref,
    nk_ref,
    nv_ref,
    gain_ref,
    block_sems,
    tree_sems,
    small_sems,
):
    batch, heads, nodes, width = q_ref.shape
    kv, span = k_ref.shape[1:3]
    scale = width**-0.5
    step = scale * LOG2E
    seq = lax.axis_index(SEQ)
    owner = seq == lax.axis_size(SEQ) - 1
    other = jnp.logical_not(owner)
    group = ROWS // nodes
    turns = range(heads // group)
    of_group = heads // group // kv
    ones = jnp.ones((span, width), bf16)

    lengths_copy = pltpu.make_async_copy(lengths_hbm, lengths_ref, small_sems.at[0])
    lengths_copy.start()
    gain_copy = pltpu.make_async_copy(gain_hbm, gain_ref, small_sems.at[1])
    gain_copy.start()

    def block_copy(b, g, n):
        own = pl.ds(g * (heads // kv), heads // kv)
        source, target, place = (
            (q_hbm, q_ref, (b, own)),
            (k_hbm, k_ref, (b, g)),
            (v_hbm, v_ref, (b, g)),
        )[n]
        return pltpu.make_async_copy(source.at[place], target.at[place], block_sems.at[b, g, n])

    for b in range(batch):
        for g in range(kv):
            for n in range(3):
                block_copy(b, g, n).start()
    trees = [
        pltpu.make_async_copy(source, target, tree_sems.at[n])
        for n, (source, target) in enumerate(
            ((parents_hbm, parents_ref), (nk_hbm, nk_ref), (nv_hbm, nv_ref))
        )
    ]

    @pl.when(owner)
    def _():
        for copy in trees:
            copy.start()
        for copy in trees:
            copy.wait()

    lengths_copy.wait()
    gain_copy.wait()
    gain = gain_ref[...].astype(f32)[None]
    gains = gain[:, :width], gain[:, width:]
    row = lax.broadcasted_iota(jnp.int32, (8, width), 0)

    def write(b, part, out, top, total):
        at = b * heads + part * group
        out_ref[pl.ds(at, group), :nodes] = out.astype(bf16).reshape(group, nodes, width)
        lane = lax.broadcasted_iota(jnp.int32, (ROWS, width), 1)
        turned = jnp.transpose(jnp.where(lane == 0, top, total))[:8]
        for h in range(group):
            section = turned[:, h * nodes : (h + 1) * nodes]
            total = section[1:2]
            high = total.astype(bf16).astype(f32)
            lines = jnp.where(row[:, :nodes] == 1, high, total - high)
            lines = jnp.where(row[:, :nodes] == 0, section[0:1], lines)
            tail = jnp.concatenate([lines, jnp.zeros((8, width - nodes), f32)], axis=1)
            for n in range(2):
                tail = jnp.where(row == 3 + n, gains[n], tail)
            out_ref[at + h, nodes:] = tail.astype(bf16)

    def sweep(b, live, with_cache, with_tree):
        biases = []
        if with_cache:
            dead = lax.broadcasted_iota(jnp.int32, (1, span), 1) >= live
            biases.append(jnp.where(dead, HIDDEN, 0.0))
        if with_tree:
            bias = tree_bias(parents_ref[pl.ds(b, 1)])
            biases.append(jnp.concatenate([bias] * group, axis=0))

        def products(part):
            g = part // of_group
            rows = q_ref[b, part * group : (part + 1) * group].reshape(ROWS, width)
            found = [rows_dot(rows, k_ref[b, g])] if with_cache else []
            return found + ([rows_dot(rows, nk_ref[b, g])] if with_tree else [])

        ahead = products(0)
        for part in turns:
            g = part // of_group
            scores = [s + bias for s, bias in zip(ahead, biases)]
            if part + 1 < len(turns):
                ahead = products(part + 1)
            if part % of_group == 0:
                values = [jnp.concatenate([v_ref[b, g], ones], axis=1)] if with_cache else []
                if with_tree:
                    values.append(jnp.concatenate([nv_ref[b, g], ones[:nodes]], axis=1))
            highest = functools.reduce(
                jnp.maximum, [jnp.max(s, axis=1, keepdims=True) for s in scores]
            )
            top = jnp.maximum((highest * scale).astype(bf16).astype(f32), FLOOR)
            shift = top * LOG2E
            result = 0.0
            for s, value in zip(scores, values):
                weights = jnp.exp2(s * step - shift).astype(bf16)
                result = result + plain_dot(weights, value)
            write(b, part, result[:, :width], top, result[:, width:])

    def nothing(b):
        for part in turns:
            zeros = jnp.zeros((ROWS, width), f32)
            write(b, part, zeros, jnp.full((ROWS, 1), FLOOR), zeros)

    @pl.loop(0, batch)
    def _(b):
        live = lengths_ref[b] - seq * span
        for g in range(kv):
            for n in range(3):
                block_copy(b, g, n).wait()
        filled = live > 0
        empty = jnp.logical_not(filled)
        pl.when(jnp.logical_and(filled, other))(functools.partial(sweep, b, live, True, False))
        pl.when(jnp.logical_and(filled, owner))(functools.partial(sweep, b, live, True, True))
        pl.when(jnp.logical_and(empty, owner))(functools.partial(sweep, b, live, False, True))
        pl.when(jnp.logical_and(empty, other))(functools.partial(nothing, b))


def local_attention(
    queries, cache_keys, cache_values, new_keys, new_values, parents, lengths, gain
):
    batch, heads, nodes, width = queries.shape
    kv = cache_keys.shape[1]
    operands = (lengths, parents, queries, cache_keys, cache_values, new_keys, new_values, gain)
    scratch = [pltpu.SMEM(lengths.shape, lengths.dtype)]
    scratch += [pltpu.VMEM(x.shape, x.dtype) for x in operands[1:]]
    scratch += [
        pltpu.SemaphoreType.DMA((batch, kv, 3)),
        pltpu.SemaphoreType.DMA((3,)),
        pltpu.SemaphoreType.DMA((2,)),
    ]
    return pl.pallas_call(
        attention_kernel,
        in_specs=[pl.BlockSpec(memory_space=pltpu.HBM)] * len(operands),
        out_specs=pl.BlockSpec(memory_space=pltpu.VMEM),
        out_shape=jax.ShapeDtypeStruct((batch * heads, nodes + 8, width), bf16),
        scratch_shapes=scratch,
        compiler_params=room(62),
        name="attend",
    )(*operands)


def join_kernel(parts_ref, out_ref):
    count, rows, width = parts_ref.shape
    nodes = rows - 8
    tops = parts_ref[:, nodes, :].astype(f32)
    totals = parts_ref[:, nodes + 1, :].astype(f32) + parts_ref[:, nodes + 2, :].astype(f32)
    used = lax.broadcasted_iota(jnp.int32, (count, width), 1) < nodes
    tops = jnp.where(used, tops, 0.0)
    totals = jnp.where(used, totals, 1.0)
    factors = jnp.exp(tops - jnp.max(tops, axis=0, keepdims=True))
    share = factors / jnp.sum(factors * totals, axis=0, keepdims=True)
    square = jnp.concatenate([share, jnp.zeros((width - count, width), f32)], axis=0)
    turned = jnp.transpose(square)[:nodes]
    total = parts_ref[0, :nodes].astype(f32) * turned[:, 0:1]
    for k in range(1, count):
        total = total + parts_ref[k, :nodes].astype(f32) * turned[:, k : k + 1]
    block = total.astype(bf16)
    for k in range(out_ref.shape[0]):
        out_ref[k] = block


def join_shares(parts, copies):
    rows, width = parts.shape[1:]
    return pl.pallas_call(
        join_kernel,
        out_shape=jax.ShapeDtypeStruct((copies, rows - 8, width), bf16),
        compiler_params=room(8),
        name="join",
    )(parts)


def head_lines(blocks_ref):
    half = blocks_ref.shape[0] // 2
    lines = [
        jnp.concatenate([blocks_ref[place_of(b * half + k)] for k in range(half)], axis=1)
        for b in range(2)
    ]
    return jnp.concatenate(lines, axis=0)


def project_first_kernel(blocks_ref, weight_ref, out_ref, rest_ref):
    chips, nodes, width = blocks_ref.shape
    core = lax.axis_index("seq_2")
    sections = []
    for k in range(chips // 2):
        own = pl.multiple_of((2 * k + core) * width, width)
        other = pl.multiple_of((2 * k + 1 - core) * width, width)
        sections.append(weight_ref[pl.ds(own, width)])
        rest_ref[k * width : (k + 1) * width] = weight_ref[pl.ds(other, width)]
    out_ref[...] = plain_dot(head_lines(blocks_ref), jnp.concatenate(sections, axis=0))


def project_second_kernel(blocks_ref, weight_ref, first_ref, out_ref):
    result = first_ref[...] + plain_dot(head_lines(blocks_ref), weight_ref[...])
    result = result.astype(bf16)
    for k in range(out_ref.shape[0]):
        out_ref[k] = result


def project_first(blocks, weight):
    rows = 2 * blocks.shape[1]
    depth, columns = weight.shape
    return pl.pallas_call(
        project_first_kernel,
        out_shape=[
            jax.ShapeDtypeStruct((rows, columns), f32),
            jax.ShapeDtypeStruct((depth // 2, columns), weight.dtype),
        ],
        cost_estimate=pl.CostEstimate(
            flops=rows * weight.size, bytes_accessed=3 * weight.size, transcendentals=0
        ),
        compiler_params=room(8),
        name="project_first",
    )(blocks, weight)


def project_second(blocks, weight, first, copies):
    return pl.pallas_call(
        project_second_kernel,
        out_shape=jax.ShapeDtypeStruct((copies, *first.shape), bf16),
        compiler_params=room(8),
        name="project_second",
    )(blocks, weight, first)


def stream_kernel(parts_ref, residual_ref, gain_ref, out_ref):
    stream = residual_ref[...].astype(f32)
    for k in range(parts_ref.shape[0]):
        stream = stream + parts_ref[k].astype(f32)
    scaled = (stream * gain_ref[...].astype(f32)[None]).astype(bf16)
    for k in range(out_ref.shape[0]):
        out_ref[k] = scaled


def make_stream(parts, residual, gain, copies):
    rows, columns = residual.shape
    return pl.pallas_call(
        stream_kernel,
        out_shape=jax.ShapeDtypeStruct((copies, rows, columns), bf16),
        compiler_params=room(8),
        name="stream",
    )(parts, residual, gain)


def gathered_product(blocks_ref, weight_ref):
    chips, rows, columns = blocks_ref.shape
    core = lax.axis_index("seq_2")
    blocks, sections = [], []
    for k in range(chips):
        start = pl.multiple_of((2 * place_of(k) + core) * columns, columns)
        blocks.append(blocks_ref[k])
        sections.append(weight_ref[pl.ds(start, columns)])
    return plain_dot(jnp.concatenate(blocks, axis=1), jnp.concatenate(sections, axis=0))


def sent_kernel(blocks_ref, shares_ref, weight_ref, out_ref):
    chips = blocks_ref.shape[0]
    width = weight_ref.shape[1]
    nodes = shares_ref.shape[1] - 8
    core = lax.axis_index("seq_2")
    squares = 0.0
    for k in range(chips):
        gains = shares_ref[2 * place_of(k) + core, nodes:].astype(f32)
        for n in range(2):
            inverse = 1.0 / gains[3 + n : 4 + n]
            plain = blocks_ref[k, :, n * 128 : (n + 1) * 128].astype(f32) * inverse
            squares = squares + plain * plain
    out_ref[:, :width] = gathered_product(blocks_ref, weight_ref)
    out_ref[:, width:] = squares


def kept_kernel(blocks_ref, weight_ref, out_ref):
    out_ref[...] = gathered_product(blocks_ref, weight_ref)


def product_cost(blocks, weight):
    chips, rows, columns = blocks.shape
    return pl.CostEstimate(
        flops=2 * blocks.size * weight.shape[1],
        bytes_accessed=2 * chips * columns * (rows + weight.shape[1]),
        transcendentals=0,
    )


def sent_product(blocks, shares, weight):
    return pl.pallas_call(
        sent_kernel,
        out_shape=jax.ShapeDtypeStruct((blocks.shape[1], weight.shape[1] + 128), f32),
        cost_estimate=product_cost(blocks, weight),
        compiler_params=room(16),
        name="logits_sent",
    )(blocks, shares, weight)


def kept_product(blocks, weight):
    return pl.pallas_call(
        kept_kernel,
        out_shape=jax.ShapeDtypeStruct((blocks.shape[1], weight.shape[1]), f32),
        cost_estimate=product_cost(blocks, weight),
        compiler_params=room(16),
        name="logits_kept",
    )(blocks, weight)


def statistics_kernel(kept_ref, sent_ref, received_ref, tokens_ref, logits_ref, stats_ref):
    rows, width = kept_ref.shape
    squares = sent_ref[:, width:] + received_ref[:, width:]
    total = jnp.sum(squares, axis=1, keepdims=True)
    logits = (kept_ref[...] + received_ref[:, :width]) * lax.rsqrt(total / D + EPSILON)
    logits_ref[...] = logits
    top = jnp.max(logits, axis=1, keepdims=True)
    sums = jnp.sum(jnp.exp(logits - top), axis=1, keepdims=True)
    ids = lax.broadcasted_iota(jnp.int32, (rows, width), 1) + lax.axis_index(SEQ_HEAD) * width
    lines = [tokens_ref[b : b + 1].astype(f32) for b in range(tokens_ref.shape[0])]
    line = jnp.broadcast_to(jnp.concatenate(lines, axis=1), (128, rows))
    tokens = jnp.transpose(line)[:, 0:1].astype(jnp.int32)
    hit = jnp.sum(jnp.where(ids == tokens, logits, 0.0), axis=1, keepdims=True)
    lane = lax.broadcasted_iota(jnp.int32, (rows, 128), 1)
    turned = jnp.transpose(jnp.where(lane % 2 == 0, top + jnp.log(sums), hit))[:8]
    for k in range(stats_ref.shape[0] // 8):
        stats_ref[k * 8 : k * 8 + 8] = turned


def logit_statistics(kept, sent, received, tokens, copies):
    return pl.pallas_call(
        statistics_kernel,
        out_shape=[
            jax.ShapeDtypeStruct(kept.shape, f32),
            jax.ShapeDtypeStruct((copies * 2, 128), f32),
        ],
        compiler_params=room(8),
        name="logits_statistics",
    )(kept, sent, received, tokens)


def final_kernel(path_ref, stats_ref, logits_ref, picked_ref, out_ref):
    batch, nodes = out_ref.shape
    for b in range(batch):
        for k in range(path_ref.shape[1]):
            picked_ref[k, b : b + 1] = logits_ref[pl.ds(path_ref[b, k] + b * nodes, 1)]
    stats = stats_ref[...]
    is_sum = lax.broadcasted_iota(jnp.int32, stats.shape, 0) % 2 == 0
    sums = jnp.where(is_sum, stats, HIDDEN)
    top = jnp.max(sums, axis=0, keepdims=True)
    total = top + jnp.log(jnp.sum(jnp.exp(sums - top), axis=0, keepdims=True))
    result = jnp.sum(jnp.where(is_sum, 0.0, stats), axis=0, keepdims=True) - total
    for b in range(batch):
        out_ref[b : b + 1] = result[:, b * nodes : (b + 1) * nodes]


def final_join(path, stats, logits):
    batch = path.shape[0]
    rows, width = logits.shape
    return pl.pallas_call(
        final_kernel,
        in_specs=[
            pl.BlockSpec(memory_space=pltpu.SMEM),
            pl.BlockSpec(memory_space=pltpu.VMEM),
            pl.BlockSpec(memory_space=pltpu.VMEM),
        ],
        out_shape=[
            jax.ShapeDtypeStruct((*path.shape[::-1], width), f32),
            jax.ShapeDtypeStruct((batch, rows // batch), f32),
        ],
        compiler_params=room(4),
        name="final",
    )(path, stats, logits)


def to_each(x, axes):
    return lax.all_to_all(x, axes, 0, 0, tiled=True)


def across(x):
    return lax.ppermute(x, "seq_2", [(0, 1), (1, 0)])


def on_device(
    queries,
    cache_keys,
    cache_values,
    new_keys,
    new_values,
    parents,
    path,
    lengths,
    draft_tokens,
    residual,
    out_weight,
    norm_gain,
    vocab_weight,
):
    rows = parents.size
    chips = lax.axis_size(CHIPS)
    shares = local_attention(
        queries, cache_keys, cache_values, new_keys, new_values, parents, lengths, norm_gain
    )
    shares = to_each(shares, SEQ)
    heads = to_each(join_shares(shares, chips), CHIPS)
    other_heads = across(heads)
    partial, rest = project_first(heads, out_weight)
    partial = project_second(other_heads, rest, partial, lax.axis_size("head"))
    partial, own_weight = lax.optimization_barrier((partial, vocab_weight))
    other_weight = across(own_weight)
    partial = to_each(partial, "head")
    stream = make_stream(partial, residual.reshape(rows, -1), norm_gain, chips)
    mine = to_each(stream, CHIPS)
    sent = sent_product(mine, shares, other_weight)
    received = across(sent)
    kept = kept_product(mine, own_weight)
    copies = lax.axis_size(SEQ_HEAD)
    logits, stats = logit_statistics(kept, sent, received, draft_tokens, copies)
    stats = to_each(stats.reshape(copies, 2, 128), SEQ_HEAD).reshape(copies * 2, 128)
    path_logits, logprob = final_join(path, stats, logits)
    return (jnp.transpose(path_logits, (1, 0, 2)), logprob)


def solution(mesh):
    torus = Mesh(
        mesh.devices.reshape(4, 4, 2, mesh.shape["head"]), ("seq_0", "seq_1", "seq_2", "head")
    )
    in_specs = (
        P(None, "head", None, None),
        P(None, "head", SEQ, None),
        P(None, "head", SEQ, None),
        P(None, "head", None, None),
        P(None, "head", None, None),
        P(),
        P(),
        P(),
        P(),
        P(None, None, SEQ),
        P("head", SEQ),
        P(SEQ),
        P(None, SEQ_HEAD),
    )
    out_specs = (P(None, None, SEQ_HEAD), P())
    return jax.shard_map(
        on_device, mesh=torus, in_specs=in_specs, out_specs=out_specs, check_vma=False
    )
```
